128 devices in a mesh: area: 32 (over z, y, core), local: 4 (over x).
Axes of the slice: x: 4, y: 4, z: 4, core: 2. Of those that a mesh axis runs over, the one named last changes fastest.
Arguments:
- potential: float32 [8, 524288], P(None, ('area', 'local')), may hold values from -6 to 6
- current: float32 [8, 524288], P(None, ('area', 'local')), may hold values from -4 to 4
- ext_drive: float32 [8, 524288], P(None, ('area', 'local')), may hold values from -6 to 6
- decay_syn: float32 [524288], P(('area', 'local')), may hold values from 0.3 to 0.97
- decay_mem: float32 [524288], P(('area', 'local')), may hold values from 0.4 to 0.95
- weights: bfloat16 [128, 128, 2, 128, 128], P(('area', 'local')), may hold values from -0.25 to 0.25
- tile_src: int32 [128, 128, 2], P(('area', 'local')), may hold values from 0 to 31
- tile_dst: int32 [128, 128, 2], P(('area', 'local')), may hold values from 0 to 31
- blk_pop: int32 [4096], P(('area', 'local')), may hold values from 0 to 7
- tile_route: int32 [5, 128, 128, 1], P(None, ('area', 'local')), may hold values from 0 to 1, as said below
- counts: int32 [5, 128, 128], P(None, ('area', 'local')), may hold values from 0 to 1, as said below
Outputs:
- volts_out: float32 [8, 524288], P(None, ('area', 'local'))
- current_out: float32 [8, 524288], P(None, ('area', 'local'))
- pop_rates: float32 [32, 5, 8, 8], P('area')
The draws below stay inside these ranges and needn't reach their ends.
Inputs may be any that keep to these rules, and one draw needn't show every extreme that they name: `tile_route`: the 1 entries of one list name distinct tiles; entries at and beyond counts of that list are unused. `counts`: in every step some target device gets 1 tiles from every sending device.
All inputs are finite; a program needn't handle non-finite values.
Results may differ from the reference program's by a relative error of at most 0.0029.
Values may be sent and summed in bfloat16 or wider, within the bound.
No kernel may reach another device: no remote copies, remote signals or barrier semaphores. Data moves between devices by JAX's collectives and lax.ppermute only.
A program may use at most 64 MiB of HBM per device.

```python
import math
import jax
import jax.numpy as jnp
from jax import lax

BLOCK = 128
NB_DEV = 32
TRIALS = 8
TPT = 2
CAP = 1
STEPS = 5
POPS = 8
TARGETS = 128
NEURONS = 524288
N_AREA = 32
N_LOCAL = 4


def draw_tile_route(key, part):
    dev_count = N_AREA * N_LOCAL
    scores = jax.random.randint(key, (STEPS, dev_count, dev_count, TPT), 0, 1 << 20) * TPT + jnp.arange(TPT, dtype=jnp.int32)
    order = jnp.argsort(scores, axis=-1)
    return order[..., :CAP].astype(jnp.int32)


def draw_counts(key, part):
    dev_count = N_AREA * N_LOCAL
    key_one, key_two = jax.random.split(key)
    base_load = jax.random.randint(key_one, (STEPS, dev_count, dev_count), 0, CAP + 1)
    full_target = jax.random.randint(key_two, (STEPS,), 0, dev_count)
    filled = jnp.arange(dev_count, dtype=jnp.int32)[None, None, :] == full_target[:, None, None]
    return jnp.where(filled, CAP, base_load).astype(jnp.int32)


def touch_ends(entries, stream_key, smallest, largest):
    shape = entries.shape
    spot = [jax.random.randint(jax.random.fold_in(stream_key, axis), (), 0, shape[axis]) for axis in range(len(shape))]
    entries = entries.at[tuple(spot)].set(smallest)
    longest = shape.index(max(shape))
    spot[longest] = (spot[longest] + 1) % shape[longest]
    return entries.at[tuple(spot)].set(largest)


def block_levels(stream_key, dims, pieces, smallest, largest):
    def one(dim, parts):
        steps = jax.random.uniform(jax.random.fold_in(jax.random.fold_in(stream_key, 6), dim), (parts,), jnp.float32, smallest / len(pieces), largest / len(pieces))
        return jnp.repeat(jnp.exp(steps), dims[dim] // parts).reshape((-1,) + (1,) * (len(dims) - dim - 1))

    loudness = one(*pieces[0])
    for cut in pieces[1:]:
        loudness = loudness * one(*cut)
    return loudness


def normal_values(key, extent, width, bound, cuts=(), kind=jnp.bfloat16):
    array = jax.random.normal(key, extent, jnp.float32) * width
    if len(cuts) > 0:
        array = block_levels(key, extent, cuts, -0.22, 0.18) * array
    return jnp.clip(array, min=-bound, max=bound).astype(kind)


def setup_inputs(seed: int = 0) -> dict:
    key_list = jax.random.split(jax.random.key(seed), 12)
    return {
        "potential": normal_values(key_list[0], (TRIALS, NEURONS), 1.0, 6.0, ((1, 128),), jnp.float32),
        "current": normal_values(key_list[1], (TRIALS, NEURONS), 0.5, 4.0, ((1, 128),), jnp.float32),
        "ext_drive": normal_values(key_list[2], (TRIALS, NEURONS), 1.0, 6.0, ((1, 128),), jnp.float32),
        "decay_syn": jnp.clip(jnp.exp(math.log(0.97) - 1.17351359 * jax.random.uniform(key_list[3], (NEURONS,), jnp.float32) ** block_levels(key_list[3], (NEURONS,), ((0, 128),), -0.2, 0.2)), 0.3, 0.97),
        "decay_mem": jnp.clip(jnp.exp(math.log(0.95) - 0.8649974 * jax.random.uniform(key_list[4], (NEURONS,), jnp.float32) ** block_levels(key_list[4], (NEURONS,), ((0, 128),), -0.2, 0.2)), 0.4, 0.95),
        "weights": normal_values(key_list[5], (TARGETS, TARGETS, TPT, BLOCK, BLOCK), (4 * BLOCK) ** -0.5, 0.25, ((0, 128),)),
        "tile_src": touch_ends(jax.random.randint(key_list[6], (TARGETS, TARGETS, TPT), 0, NB_DEV), jax.random.fold_in(key_list[6], 1), 0, NB_DEV - 1).astype(jnp.int32),
        "tile_dst": touch_ends(jax.random.randint(key_list[7], (TARGETS, TARGETS, TPT), 0, NB_DEV), jax.random.fold_in(key_list[7], 1), 0, NB_DEV - 1).astype(jnp.int32),
        "blk_pop": touch_ends(jax.random.randint(key_list[8], (NB_DEV * TARGETS,), 0, POPS), jax.random.fold_in(key_list[8], 1), 0, POPS - 1).astype(jnp.int32),
        "tile_route": draw_tile_route(jax.random.fold_in(key_list[11], 71), 0),
        "counts": draw_counts(jax.random.fold_in(key_list[11], 71), 0),
    }


spike_gain = 4.0
threshold = 1.0
reset_size = 0.5


def reference(potential, current, ext_drive, decay_syn, decay_mem, weights, tile_src, tile_dst, blk_pop, tile_route, counts):
    dev_count = N_AREA * N_LOCAL
    state_shape = (TRIALS, dev_count, NB_DEV, BLOCK)
    volts = potential.reshape(state_shape)
    syn_cur = current.reshape(state_shape)
    ext_field = ext_drive.reshape(state_shape)
    syn_decay = decay_syn.reshape((1, dev_count, NB_DEV, BLOCK))
    mem_decay = decay_mem.reshape((1, dev_count, NB_DEV, BLOCK))
    pop_table = (blk_pop.reshape((dev_count, NB_DEV))[:, :, None] == jnp.arange(POPS, dtype=jnp.int32)[None, None, :]).astype(jnp.float32)
    target_rows = jnp.arange(dev_count, dtype=jnp.int32)[:, None]
    rate_list = []
    for step_idx in range(STEPS):
        spikes = jax.nn.sigmoid(spike_gain * (volts - threshold))
        spike_bf = spikes.astype(jnp.bfloat16)
        spike_blocks = jnp.transpose(spike_bf, (1, 2, 0, 3))
        activity = jnp.sum(spikes, axis=3)
        per_dev = jnp.einsum('rdb,dbp->drp', activity, pop_table, precision=lax.Precision.HIGHEST)
        rate_list.append(jnp.sum(per_dev.reshape((N_AREA, N_LOCAL, TRIALS, POPS)), axis=1) / (BLOCK * NB_DEV))

        def one_sender(inflow, sender):
            chosen = tile_route[step_idx, sender]
            slot_valid = jnp.arange(CAP, dtype=jnp.int32)[None, :] < counts[step_idx, sender][:, None]
            picked = jnp.take_along_axis(weights[sender], chosen[:, :, None, None], axis=1)
            src_blocks = jnp.take_along_axis(tile_src[sender], chosen, axis=1)
            dst_blocks = jnp.take_along_axis(tile_dst[sender], chosen, axis=1)
            senders = spike_blocks[sender][src_blocks]
            tile_cur = jnp.einsum('tcrn,tcnm->tcrm', senders.astype(jnp.float32), picked.astype(jnp.float32)).astype(jnp.bfloat16)
            tile_cur = jnp.where(slot_valid[:, :, None, None], tile_cur.astype(jnp.float32), jnp.float32(0.0))
            inflow = inflow.at[target_rows, dst_blocks].add(tile_cur)
            return inflow, None

        start = jnp.zeros((dev_count, NB_DEV, TRIALS, BLOCK), jnp.float32)
        inflow, unused = lax.scan(one_sender, start, jnp.arange(dev_count, dtype=jnp.int32))
        inflow = jnp.transpose(inflow, (2, 0, 1, 3))
        syn_cur = syn_decay * syn_cur + inflow
        volts = mem_decay * volts + (1.0 - mem_decay) * (syn_cur + ext_field) - reset_size * spikes
    pop_rates = jnp.stack(rate_list, axis=1)
    return volts.reshape((TRIALS, -1)), syn_cur.reshape((TRIALS, -1)), pop_rates
```

```python
import functools

import jax
import jax.numpy as jnp
from jax import lax
from jax.experimental import pallas as pl
from jax.experimental.pallas import tpu as pltpu
from jax.sharding import PartitionSpec as P

POPS = 8
BLOCK = 128
TRIALS = 8
NO_BLOCK = 64
GROUP = 8

spike_gain = 4.0
threshold = 1.0
reset_size = 0.5

VMEM = pl.BlockSpec(memory_space=pltpu.VMEM)
SMEM = pl.BlockSpec(memory_space=pltpu.SMEM)
HBM = pl.BlockSpec(memory_space=pltpu.HBM)


def params(mib, **more):
    return pltpu.CompilerParams(vmem_limit_bytes=mib << 20, **more)


def lanes(block):
    return slice(block * BLOCK, (block + 1) * BLOCK)


def spike_of(volts):
    return jax.nn.sigmoid(spike_gain * (volts - threshold))


def send_tiles(step, devs, route_ref, src_ref, blocks_ref, table_ref, tiles_ref, sems, out_ref):
    def one_round(g, carry):
        for j in range(GROUP):
            d = g * GROUP + j
            pltpu.make_async_copy(table_ref.at[d], tiles_ref.at[d], sems.at[d]).wait()
        for j in range(GROUP):
            d = g * GROUP + j
            spikes = blocks_ref[src_ref[route_ref[step, 0, d], d]]
            current = jnp.dot(spikes, tiles_ref[d], preferred_element_type=jnp.float32)
            out_ref[d, 0:TRIALS, :] = current.astype(jnp.bfloat16)
        return carry

    lax.fori_loop(0, devs // GROUP, one_round, 0)


def fetch_tiles(step, devs, tpt, route_ref, table_ref, tiles_ref, sems):
    def one(d, carry):
        pltpu.make_async_copy(
            table_ref.at[d * tpt + route_ref[step, 0, d]], tiles_ref.at[d], sems.at[d]
        ).start()
        return carry

    lax.fori_loop(0, devs, one, 0, unroll=8)


def first_kernel(
    route_ref, src_ref, volts_ref, dst_ref, routes_ref, counts_ref, table_ref,
    out_ref, spikes_ref, tiles_ref, blocks_ref, sems,
):
    devs = out_ref.shape[0]
    tpt = dst_ref.shape[0]
    steps = routes_ref.shape[0]

    fetch_tiles(0, devs, tpt, route_ref, table_ref, tiles_ref, sems)

    for b in range(blocks_ref.shape[0]):
        spikes = spike_of(volts_ref[:, lanes(b)])
        spikes_ref[:, lanes(b)] = spikes
        blocks_ref[b] = spikes.astype(jnp.bfloat16)

    step = lax.broadcasted_iota(jnp.int32, (BLOCK, devs), 0)
    targets = jnp.zeros((BLOCK, devs), jnp.int32)
    for t in range(steps):
        target = jnp.where(routes_ref[t] == 0, dst_ref[0:1, :], dst_ref[1:2, :])
        target = jnp.where(counts_ref[t] > 0, target, NO_BLOCK)
        targets = jnp.where(step == t, target, targets)
    targets = targets.astype(jnp.float32).astype(jnp.bfloat16)
    rows = lax.broadcasted_iota(jnp.int32, (devs * TRIALS, devs), 0) // TRIALS
    cols = lax.broadcasted_iota(jnp.int32, (devs * TRIALS, devs), 1)
    spread = jnp.where(rows == cols, 1.0, 0.0).astype(jnp.bfloat16)
    tails = lax.dot_general(
        spread, targets, (((1,), (1,)), ((), ())), preferred_element_type=jnp.float32
    )
    tails = tails.astype(jnp.bfloat16)
    for d in range(devs):
        out_ref[d, TRIALS:, :] = tails[d * TRIALS : (d + 1) * TRIALS, :]

    send_tiles(0, devs, route_ref, src_ref, blocks_ref, table_ref, tiles_ref, sems, out_ref)


def codes_of(tail, first):
    pick = jnp.where(
        lax.broadcasted_iota(jnp.int32, (8, BLOCK), 0)
        == lax.broadcasted_iota(jnp.int32, (8, BLOCK), 1),
        1.0,
        0.0,
    ).astype(jnp.bfloat16)
    blocks = lax.dot_general(
        pick, tail, (((1,), (1,)), ((), ())), preferred_element_type=jnp.float32
    ).astype(jnp.int32)
    trial = lax.broadcasted_iota(jnp.int32, blocks.shape, 1) % TRIALS
    return blocks * TRIALS + trial


def inflow_of(code, arrived, rows):
    row = lax.broadcasted_iota(jnp.int32, (rows, code.shape[1]), 0)
    deliver = jnp.where(row == code, 1.0, 0.0).astype(jnp.bfloat16)
    return jnp.dot(deliver, arrived, preferred_element_type=jnp.float32)


def update(b, inflow, volts_ref, cur_ref, ext_ref, spikes_ref, dsyn_ref, dmem_ref):
    at = lanes(b)
    dsyn = dsyn_ref[b : b + 1, :]
    dmem = dmem_ref[b : b + 1, :]
    cur = dsyn * cur_ref[:, at] + inflow[b * TRIALS : (b + 1) * TRIALS, :]
    volts = (
        dmem * volts_ref[:, at]
        + (1.0 - dmem) * (cur + ext_ref[:, at])
        - reset_size * spikes_ref[:, at]
    )
    return volts, cur


def step_kernel(step, *refs):
    (route_ref, src_ref, arrived_ref, codes_ref, volts_ref, cur_ref, ext_ref,
     spikes_ref, dsyn_ref, dmem_ref, table_ref) = refs[:11]
    if step == 1:
        volts_out, cur_out, spikes_out, out_ref, codes_out, tiles_ref, blocks_ref, sems = refs[11:]
    else:
        volts_out, cur_out, spikes_out, out_ref, tiles_ref, blocks_ref, sems = refs[11:]
    devs = out_ref.shape[0]
    count = blocks_ref.shape[0]
    tpt = table_ref.shape[0] // devs
    fetch_tiles(step, devs, tpt, route_ref, table_ref, tiles_ref, sems)
    if step == 1:
        tail = arrived_ref[:, TRIALS:, :].reshape(devs * TRIALS, BLOCK)
        codes = codes_of(tail, True)
        codes_out[...] = codes
        arrived = arrived_ref[:, :TRIALS, :].reshape(devs * TRIALS, BLOCK)
    else:
        codes = codes_ref[...]
        arrived = arrived_ref[...].reshape(devs * TRIALS, BLOCK)
    inflow = inflow_of(codes[step - 1 : step, :], arrived, count * TRIALS)
    for b in range(count):
        volts, cur = update(
            b, inflow, volts_ref, cur_ref, ext_ref, spikes_ref, dsyn_ref, dmem_ref
        )
        volts_out[:, lanes(b)] = volts
        cur_out[:, lanes(b)] = cur
        spikes = spike_of(volts)
        spikes_out[:, lanes(b)] = spikes
        blocks_ref[b] = spikes.astype(jnp.bfloat16)
    send_tiles(step, devs, route_ref, src_ref, blocks_ref, table_ref, tiles_ref, sems, out_ref)


def last_kernel(step, arrived_ref, codes_ref, volts_ref, cur_ref, ext_ref, spikes_ref,
                dsyn_ref, dmem_ref, volts_out, cur_out):
    devs = arrived_ref.shape[0]
    count = dsyn_ref.shape[0]
    arrived = arrived_ref[...].reshape(devs * TRIALS, BLOCK)
    inflow = inflow_of(codes_ref[step - 1 : step, :], arrived, count * TRIALS)
    for b in range(count):
        volts, cur = update(
            b, inflow, volts_ref, cur_ref, ext_ref, spikes_ref, dsyn_ref, dmem_ref
        )
        volts_out[:, lanes(b)] = volts
        cur_out[:, lanes(b)] = cur


def shards(
    potential,
    current,
    ext_drive,
    decay_syn,
    decay_mem,
    weights,
    tile_src,
    tile_dst,
    blk_pop,
    tile_route,
    counts,
):
    devs, tpt = weights.shape[1:3]
    count = blk_pop.shape[0]
    steps = tile_route.shape[0]
    f32, bf16 = jnp.float32, jnp.bfloat16
    table = weights.reshape(devs * tpt, BLOCK, BLOCK)
    src = tile_src[0].T
    dst = tile_dst[0].T
    route = tile_route.reshape(steps, 1, devs)
    used = counts.reshape(steps, 1, devs)
    dsyn = decay_syn.reshape(count, BLOCK)
    dmem = decay_mem.reshape(count, BLOCK)
    state = jax.ShapeDtypeStruct((TRIALS, count * BLOCK), f32)
    sent = jax.ShapeDtypeStruct((devs, TRIALS, BLOCK), bf16)
    scratch = [
        pltpu.VMEM((devs, BLOCK, BLOCK), bf16),
        pltpu.VMEM((count, TRIALS, BLOCK), bf16),
        pltpu.SemaphoreType.DMA((devs,)),
    ]

    def exchange(out):
        return lax.all_to_all(out, ("area", "local"), 0, 0, tiled=True)

    out, spikes = pl.pallas_call(
        first_kernel,
        out_shape=(jax.ShapeDtypeStruct((devs, 2 * TRIALS, BLOCK), bf16), state),
        in_specs=[SMEM, SMEM, VMEM, VMEM, VMEM, VMEM, HBM],
        out_specs=(VMEM, VMEM),
        scratch_shapes=scratch,
        compiler_params=params(48),
        name="first",
    )(route, src, potential, dst, route, used, table)
    arrived = exchange(out)
    volts, cur = potential, current
    codes = jnp.zeros((8, devs * TRIALS), jnp.int32)
    history = [spikes]
    for step in range(1, steps):
        outs = [state, state, state, sent]
        if step == 1:
            outs.append(jax.ShapeDtypeStruct((8, devs * TRIALS), jnp.int32))
        results = pl.pallas_call(
            functools.partial(step_kernel, step),
            out_shape=tuple(outs),
            in_specs=[SMEM, SMEM] + [VMEM] * 8 + [HBM],
            out_specs=(VMEM,) * len(outs),
            scratch_shapes=scratch,
            compiler_params=params(48),
            name=f"step{step}",
        )(route, src, arrived, codes, volts, cur, ext_drive, spikes, dsyn, dmem, table)
        volts, cur, spikes, out = results[:4]
        if step == 1:
            codes = results[4]
        history.append(spikes)
        arrived = exchange(out)
    pop_table = (blk_pop[:, None] == jnp.arange(POPS, dtype=jnp.int32)[None, :]).astype(f32)
    activity = jnp.stack([h.reshape(TRIALS, count, BLOCK).sum(axis=2) for h in history])
    rates = jnp.einsum("trb,bp->trp", activity, pop_table, precision=lax.Precision.HIGHEST)
    n_local = lax.axis_size("local")
    parts = [rates] + [
        lax.ppermute(rates, "local", [(i, (i + shift) % n_local) for i in range(n_local)])
        for shift in range(1, n_local)
    ]
    total = (parts[0] + parts[2]) + (parts[1] + parts[3])
    total = total / (BLOCK * count)
    volts, cur = pl.pallas_call(
        functools.partial(last_kernel, steps),
        out_shape=(state, state),
        in_specs=[VMEM] * 8,
        out_specs=(VMEM, VMEM),
        compiler_params=params(48),
        name="last",
    )(arrived, codes, volts, cur, ext_drive, spikes, dsyn, dmem)
    return volts, cur, total[None]


def solution(mesh):
    both = ("area", "local")
    in_specs = (
        P(None, both),
        P(None, both),
        P(None, both),
        P(both),
        P(both),
        P(both, None, None, None, None),
        P(both, None, None),
        P(both, None, None),
        P(both),
        P(None, both, None, None),
        P(None, both, None),
    )
    out_specs = (P(None, both), P(None, both), P("area", None, None, None))
    return jax.shard_map(shards, mesh=mesh, in_specs=in_specs, out_specs=out_specs, check_vma=False)
```

```python
import functools

import jax
import jax.numpy as jnp
from jax import lax
from jax.experimental import pallas as pl
from jax.experimental.pallas import tpu as pltpu
from jax.sharding import PartitionSpec as P

POPS = 8
BLOCK = 128
TRIALS = 8
NO_BLOCK = 64
GROUP = 8
CHUNKS = 8

spike_gain = 4.0
threshold = 1.0
reset_size = 0.5

VMEM = pl.BlockSpec(memory_space=pltpu.VMEM)
HBM = pl.BlockSpec(memory_space=pltpu.HBM)


def params(mib, **more):
    return pltpu.CompilerParams(vmem_limit_bytes=mib << 20, **more)


def lanes(block):
    return slice(block * BLOCK, (block + 1) * BLOCK)


def spike_of(volts):
    return jax.nn.sigmoid(spike_gain * (volts - threshold))


def send_tiles(first, last, tpt, row, route_ref, src_ref, blocks_ref, table_ref, out_ref):
    def one_round(g, carry):
        for j in range(GROUP):
            d = g * GROUP + j
            k = route_ref[row, 0, d]
            spikes = blocks_ref[src_ref[k, d]]
            current = jnp.dot(
                spikes, table_ref[d * tpt + k], preferred_element_type=jnp.float32
            )
            out_ref[d, 0:TRIALS, :] = current.astype(jnp.bfloat16)
        return carry

    lax.fori_loop(first // GROUP, last // GROUP, one_round, 0)


def one_hot(row, col):
    return jnp.where(row == col, 1.0, 0.0).astype(jnp.bfloat16)


def population_rows(pops):
    count = pops.shape[1]
    spread = one_hot(
        lax.broadcasted_iota(jnp.int32, (count, count * TRIALS), 0),
        lax.broadcasted_iota(jnp.int32, (count, count * TRIALS), 1) // TRIALS,
    )
    pops = jnp.broadcast_to(pops.astype(jnp.float32), (TRIALS, count)).astype(jnp.bfloat16)
    pops = jnp.dot(pops, spread, preferred_element_type=jnp.float32)[0:1, :].astype(jnp.int32)
    trial = lax.broadcasted_iota(jnp.int32, pops.shape, 1) % TRIALS
    row = lax.broadcasted_iota(jnp.int32, (TRIALS * POPS, count * TRIALS), 0)
    return one_hot(row, trial * POPS + pops)


def activity_of(member, spikes):
    high = spikes.astype(jnp.bfloat16)
    low = (spikes - high.astype(jnp.float32)).astype(jnp.bfloat16)
    return jnp.dot(member, high, preferred_element_type=jnp.float32) + jnp.dot(
        member, low, preferred_element_type=jnp.float32
    )


def first_kernel(
    route_hbm, src_hbm, dst_hbm, counts_hbm, volts_hbm, pops_hbm, table_hbm,
    out_ref, spikes_ref, table_ref, act_ref,
    route_s, src_s, routes_ref, dst_ref, counts_ref, volts_ref, pops_ref,
    blocks_ref, rows_ref, sems, chunk_sems,
):
    devs = out_ref.shape[0]
    tpt = dst_ref.shape[0]
    steps = routes_ref.shape[0]
    size = table_ref.shape[0] // CHUNKS
    copies = [
        pltpu.make_async_copy(a, b, sems.at[i])
        for i, (a, b) in enumerate(
            (
                (volts_hbm, volts_ref),
                (route_hbm, routes_ref),
                (dst_hbm, dst_ref),
                (counts_hbm, counts_ref),
                (route_hbm.at[0:1], route_s),
                (src_hbm, src_s),
                (pops_hbm, pops_ref),
            )
        )
    ]
    for copy in copies:
        copy.start()
    chunks = [
        pltpu.make_async_copy(
            table_hbm.at[pl.ds(c * size, size)], table_ref.at[pl.ds(c * size, size)], chunk_sems.at[c]
        )
        for c in range(CHUNKS)
    ]
    for copy in chunks:
        copy.start()
    copies[1].wait()
    copies[2].wait()
    copies[3].wait()

    step = lax.broadcasted_iota(jnp.int32, (BLOCK, devs), 0)
    targets = jnp.zeros((BLOCK, devs), jnp.int32)
    for t in range(steps):
        target = jnp.where(routes_ref[t] == 0, dst_ref[0:1, :], dst_ref[1:2, :])
        target = jnp.where(counts_ref[t] > 0, target, NO_BLOCK)
        targets = jnp.where(step == t, target, targets)
    targets = targets.astype(jnp.float32).astype(jnp.bfloat16)
    rows = lax.broadcasted_iota(jnp.int32, (devs * TRIALS, devs), 0) // TRIALS
    cols = lax.broadcasted_iota(jnp.int32, (devs * TRIALS, devs), 1)
    tails = lax.dot_general(
        one_hot(rows, cols), targets, (((1,), (1,)), ((), ())), preferred_element_type=jnp.float32
    )
    tails = tails.astype(jnp.bfloat16)
    for d in range(devs):
        out_ref[d, TRIALS:, :] = tails[d * TRIALS : (d + 1) * TRIALS, :]

    copies[0].wait()
    for b in range(blocks_ref.shape[0]):
        spikes = spike_of(volts_ref[:, lanes(b)])
        spikes_ref[:, lanes(b)] = spikes
        rows_ref[b * TRIALS : (b + 1) * TRIALS, :] = spikes
        blocks_ref[b] = spikes.astype(jnp.bfloat16)
    copies[6].wait()
    act_ref[...] = activity_of(population_rows(pops_ref[...]), rows_ref[...])

    copies[4].wait()
    copies[5].wait()
    per_chunk = devs // CHUNKS
    for c in range(CHUNKS):
        chunks[c].wait()
        send_tiles(
            c * per_chunk, (c + 1) * per_chunk, tpt, 0, route_s, src_s, blocks_ref, table_ref, out_ref
        )


def codes_of(tail):
    pick = one_hot(
        lax.broadcasted_iota(jnp.int32, (8, BLOCK), 0),
        lax.broadcasted_iota(jnp.int32, (8, BLOCK), 1),
    )
    blocks = lax.dot_general(
        pick, tail, (((1,), (1,)), ((), ())), preferred_element_type=jnp.float32
    ).astype(jnp.int32)
    trial = lax.broadcasted_iota(jnp.int32, blocks.shape, 1) % TRIALS
    return blocks * TRIALS + trial


def inflow_of(code, arrived, rows):
    row = lax.broadcasted_iota(jnp.int32, (rows, code.shape[1]), 0)
    return jnp.dot(one_hot(row, code), arrived, preferred_element_type=jnp.float32)


def update(b, inflow, volts_ref, cur_ref, ext_ref, spikes_ref, dsyn_ref, dmem_ref):
    at = lanes(b)
    dsyn = dsyn_ref[b : b + 1, :]
    dmem = dmem_ref[b : b + 1, :]
    cur = dsyn * cur_ref[:, at] + inflow[b * TRIALS : (b + 1) * TRIALS, :]
    volts = (
        dmem * volts_ref[:, at]
        + (1.0 - dmem) * (cur + ext_ref[:, at])
        - reset_size * spikes_ref[:, at]
    )
    return volts, cur


def step_kernel(step, *refs):
    (route_ref, src_ref, arrived_ref, codes_ref, volts_ref, cur_ref, ext_ref,
     spikes_ref, dsyn_ref, dmem_ref, pops_ref, table_ref) = refs[:12]
    volts_out, cur_out, spikes_out, out_ref, act_ref = refs[12:17]
    route_s, src_s, blocks_ref, rows_ref, sems = refs[-5:]
    devs = out_ref.shape[0]
    count = blocks_ref.shape[0]
    tpt = table_ref.shape[0] // devs
    to_smem = (
        pltpu.make_async_copy(route_ref.at[step : step + 1], route_s, sems.at[0]),
        pltpu.make_async_copy(src_ref, src_s, sems.at[1]),
    )
    for copy in to_smem:
        copy.start()
    if step == 1:
        codes = codes_of(arrived_ref[:, TRIALS:, :].reshape(devs * TRIALS, BLOCK))
        refs[17][...] = codes
        arrived = arrived_ref[:, :TRIALS, :].reshape(devs * TRIALS, BLOCK)
    else:
        codes = codes_ref[...]
        arrived = arrived_ref[...].reshape(devs * TRIALS, BLOCK)
    inflow = inflow_of(codes[step - 1 : step, :], arrived, count * TRIALS)
    for b in range(count):
        volts, cur = update(
            b, inflow, volts_ref, cur_ref, ext_ref, spikes_ref, dsyn_ref, dmem_ref
        )
        volts_out[:, lanes(b)] = volts
        cur_out[:, lanes(b)] = cur
        spikes = spike_of(volts)
        spikes_out[:, lanes(b)] = spikes
        rows_ref[b * TRIALS : (b + 1) * TRIALS, :] = spikes
        blocks_ref[b] = spikes.astype(jnp.bfloat16)
    act_ref[...] = activity_of(population_rows(pops_ref[...]), rows_ref[...])
    for copy in to_smem:
        copy.wait()
    send_tiles(0, devs, tpt, 0, route_s, src_s, blocks_ref, table_ref, out_ref)


def last_kernel(step, arrived_ref, codes_ref, volts_ref, cur_ref, ext_ref, spikes_ref,
                dsyn_ref, dmem_ref, volts_out, cur_out):
    devs = arrived_ref.shape[0]
    count = dsyn_ref.shape[0]
    arrived = arrived_ref[...].reshape(devs * TRIALS, BLOCK)
    inflow = inflow_of(codes_ref[step - 1 : step, :], arrived, count * TRIALS)
    for b in range(count):
        volts, cur = update(
            b, inflow, volts_ref, cur_ref, ext_ref, spikes_ref, dsyn_ref, dmem_ref
        )
        volts_out[:, lanes(b)] = volts
        cur_out[:, lanes(b)] = cur


def shards(
    potential,
    current,
    ext_drive,
    decay_syn,
    decay_mem,
    weights,
    tile_src,
    tile_dst,
    blk_pop,
    tile_route,
    counts,
):
    devs, tpt = weights.shape[1:3]
    count = blk_pop.shape[0]
    steps = tile_route.shape[0]
    f32, bf16, i32 = jnp.float32, jnp.bfloat16, jnp.int32
    table = weights.reshape(devs * tpt, BLOCK, BLOCK)
    src = tile_src[0].T
    dst = tile_dst[0].T
    route = tile_route.reshape(steps, 1, devs)
    used = counts.reshape(steps, 1, devs)
    dsyn = decay_syn.reshape(count, BLOCK)
    dmem = decay_mem.reshape(count, BLOCK)
    pops = blk_pop.reshape(1, count)
    state = jax.ShapeDtypeStruct((TRIALS, count * BLOCK), f32)
    sent = jax.ShapeDtypeStruct((devs, TRIALS, BLOCK), bf16)
    act = jax.ShapeDtypeStruct((POPS * TRIALS, BLOCK), f32)
    scratch = [
        pltpu.SMEM((1, 1, devs), i32),
        pltpu.SMEM((tpt, devs), i32),
    ]
    blocks = [
        pltpu.VMEM((count, TRIALS, BLOCK), bf16),
        pltpu.VMEM((count * TRIALS, BLOCK), f32),
    ]

    def exchange(out):
        return lax.all_to_all(out, ("area", "local"), 0, 0, tiled=True)

    def in_hbm(array):
        return pltpu.with_memory_space_constraint(array, pltpu.HBM)

    out, spikes, local_table, activity = pl.pallas_call(
        first_kernel,
        out_shape=(
            jax.ShapeDtypeStruct((devs, 2 * TRIALS, BLOCK), bf16),
            state,
            pltpu.VMEM(table.shape, bf16),
            act,
        ),
        in_specs=[HBM] * 7,
        out_specs=(VMEM,) * 4,
        scratch_shapes=scratch
        + [
            pltpu.VMEM((steps, 1, devs), i32),
            pltpu.VMEM((tpt, devs), i32),
            pltpu.VMEM((steps, 1, devs), i32),
            pltpu.VMEM(state.shape, f32),
            pltpu.VMEM((1, count), i32),
        ]
        + blocks
        + [pltpu.SemaphoreType.DMA((7,)), pltpu.SemaphoreType.DMA((CHUNKS,))],
        compiler_params=params(8),
        name="first",
    )(*[in_hbm(a) for a in (route, src, dst, used, potential, pops, table)])
    arrived = exchange(out)
    volts, cur = potential, current
    codes = jnp.zeros((8, devs * TRIALS), i32)
    history = [activity]
    for step in range(1, steps):
        outs = [state, state, state, sent, act]
        if step == 1:
            outs.append(jax.ShapeDtypeStruct((8, devs * TRIALS), i32))
        results = pl.pallas_call(
            functools.partial(step_kernel, step),
            out_shape=tuple(outs),
            in_specs=[VMEM] * 12,
            out_specs=(VMEM,) * len(outs),
            scratch_shapes=scratch + blocks + [pltpu.SemaphoreType.DMA((2,))],
            compiler_params=params(8),
            name=f"step{step}",
        )(route, src, arrived, codes, volts, cur, ext_drive, spikes, dsyn, dmem, pops, local_table)
        volts, cur, spikes, out, activity = results[:5]
        if step == 1:
            codes = results[5]
        history.append(activity)
        if step == steps - 1:
            history, out = lax.optimization_barrier((history, out))
        arrived = exchange(out)
    rates = jnp.stack(history).sum(axis=2).reshape(steps, TRIALS, POPS)
    n_local = lax.axis_size("local")
    parts = [rates] + [
        lax.ppermute(rates, "local", [(i, (i + shift) % n_local) for i in range(n_local)])
        for shift in range(1, n_local)
    ]
    total = (parts[0] + parts[2]) + (parts[1] + parts[3])
    total = total / (BLOCK * count)
    volts, cur = pl.pallas_call(
        functools.partial(last_kernel, steps),
        out_shape=(state, state),
        in_specs=[VMEM] * 8,
        out_specs=(VMEM, VMEM),
        compiler_params=params(8),
        name="last",
    )(arrived, codes, volts, cur, ext_drive, spikes, dsyn, dmem)
    return volts, cur, total[None]


def solution(mesh):
    both = ("area", "local")
    in_specs = (
        P(None, both),
        P(None, both),
        P(None, both),
        P(both),
        P(both),
        P(both, None, None, None, None),
        P(both, None, None),
        P(both, None, None),
        P(both),
        P(None, both, None, None),
        P(None, both, None),
    )
    out_specs = (P(None, both), P(None, both), P("area", None, None, None))
    return jax.shard_map(shards, mesh=mesh, in_specs=in_specs, out_specs=out_specs, check_vma=False)
```

```python
import functools

import jax
import jax.numpy as jnp
from jax import lax
from jax.experimental import pallas as pl
from jax.experimental.pallas import tpu as pltpu
from jax.sharding import PartitionSpec as P

POPS = 8
BLOCK = 128
TRIALS = 8
NO_BLOCK = 64
CHUNKS = 8

spike_gain = 4.0
threshold = 1.0
reset_size = 0.5

VMEM = pl.BlockSpec(memory_space=pltpu.VMEM)
HBM = pl.BlockSpec(memory_space=pltpu.HBM)


def params(mib, **more):
    return pltpu.CompilerParams(vmem_limit_bytes=mib << 20, **more)


def lanes(block):
    return slice(block * BLOCK, (block + 1) * BLOCK)


def spike_of(volts):
    return jax.nn.sigmoid(spike_gain * (volts - threshold))


def send_tiles(first, last, tpt, row, route_ref, src_ref, blocks_ref, table_ref, out_ref):
    for d in range(first, last, 2):
        k, l = route_ref[row, 0, d], route_ref[row, 0, d + 1]
        spikes = jnp.concatenate([blocks_ref[src_ref[k, d]], blocks_ref[src_ref[l, d + 1]]], axis=0)
        tiles = jnp.concatenate([table_ref[d * tpt + k], table_ref[(d + 1) * tpt + l]], axis=1)
        current = jnp.dot(spikes, tiles, preferred_element_type=jnp.float32).astype(jnp.bfloat16)
        out_ref[d, 0:TRIALS, :] = current[:TRIALS, :BLOCK]
        out_ref[d + 1, 0:TRIALS, :] = current[TRIALS:, BLOCK:]


def one_hot(row, col):
    return jnp.where(row == col, 1.0, 0.0).astype(jnp.bfloat16)


def population_rows(pops):
    count = pops.shape[1]
    spread = one_hot(
        lax.broadcasted_iota(jnp.int32, (count, count * TRIALS), 0),
        lax.broadcasted_iota(jnp.int32, (count, count * TRIALS), 1) // TRIALS,
    )
    pops = jnp.broadcast_to(pops.astype(jnp.float32), (TRIALS, count)).astype(jnp.bfloat16)
    pops = jnp.dot(pops, spread, preferred_element_type=jnp.float32)[0:1, :].astype(jnp.int32)
    trial = lax.broadcasted_iota(jnp.int32, pops.shape, 1) % TRIALS
    row = lax.broadcasted_iota(jnp.int32, (TRIALS * POPS, count * TRIALS), 0)
    return one_hot(row, trial * POPS + pops)


def activity_of(member, spikes):
    high = spikes.astype(jnp.bfloat16)
    low = (spikes - high.astype(jnp.float32)).astype(jnp.bfloat16)
    return jnp.dot(member, high, preferred_element_type=jnp.float32) + jnp.dot(
        member, low, preferred_element_type=jnp.float32
    )


def first_kernel(
    route_hbm, src_hbm, dst_hbm, counts_hbm, volts_hbm, pops_hbm, table_hbm,
    out_ref, spikes_ref, table_ref, act_ref,
    route_s, src_s, routes_ref, dst_ref, counts_ref, volts_ref, pops_ref,
    blocks_ref, rows_ref, sems, chunk_sems,
):
    devs = out_ref.shape[0]
    tpt = dst_ref.shape[0]
    steps = routes_ref.shape[0]
    size = table_ref.shape[0] // CHUNKS
    copies = [
        pltpu.make_async_copy(a, b, sems.at[i])
        for i, (a, b) in enumerate(
            (
                (volts_hbm, volts_ref),
                (route_hbm, routes_ref),
                (dst_hbm, dst_ref),
                (counts_hbm, counts_ref),
                (route_hbm.at[0:1], route_s),
                (src_hbm, src_s),
                (pops_hbm, pops_ref),
            )
        )
    ]
    for copy in copies:
        copy.start()

    def chunk(c):
        at = pl.ds(c * size, size)
        return pltpu.make_async_copy(table_hbm.at[at], table_ref.at[at], chunk_sems.at[c])

    def start(c, carry):
        chunk(c).start()
        return carry

    lax.fori_loop(0, CHUNKS, start, 0)
    copies[1].wait()
    copies[2].wait()
    copies[3].wait()

    step = lax.broadcasted_iota(jnp.int32, (BLOCK, devs), 0)
    targets = jnp.zeros((BLOCK, devs), jnp.int32)
    for t in range(steps):
        target = jnp.where(routes_ref[t] == 0, dst_ref[0:1, :], dst_ref[1:2, :])
        target = jnp.where(counts_ref[t] > 0, target, NO_BLOCK)
        targets = jnp.where(step == t, target, targets)
    targets = targets.astype(jnp.float32).astype(jnp.bfloat16)
    rows = lax.broadcasted_iota(jnp.int32, (devs * TRIALS, devs), 0) // TRIALS
    cols = lax.broadcasted_iota(jnp.int32, (devs * TRIALS, devs), 1)
    tails = lax.dot_general(
        one_hot(rows, cols), targets, (((1,), (1,)), ((), ())), preferred_element_type=jnp.float32
    )
    tails = tails.astype(jnp.bfloat16)
    for d in range(devs):
        out_ref[d, TRIALS:, :] = tails[d * TRIALS : (d + 1) * TRIALS, :]

    copies[0].wait()
    for b in range(blocks_ref.shape[0]):
        spikes = spike_of(volts_ref[:, lanes(b)])
        spikes_ref[:, lanes(b)] = spikes
        rows_ref[b * TRIALS : (b + 1) * TRIALS, :] = spikes
        blocks_ref[b] = spikes.astype(jnp.bfloat16)
    copies[6].wait()
    act_ref[...] = activity_of(population_rows(pops_ref[...]), rows_ref[...])

    copies[4].wait()
    copies[5].wait()
    per_chunk = devs // CHUNKS
    for c in range(CHUNKS):
        chunk(c).wait()
        send_tiles(
            c * per_chunk, (c + 1) * per_chunk, tpt, 0, route_s, src_s, blocks_ref, table_ref, out_ref
        )


def codes_of(tail):
    pick = one_hot(
        lax.broadcasted_iota(jnp.int32, (8, BLOCK), 0),
        lax.broadcasted_iota(jnp.int32, (8, BLOCK), 1),
    )
    blocks = lax.dot_general(
        pick, tail, (((1,), (1,)), ((), ())), preferred_element_type=jnp.float32
    ).astype(jnp.int32)
    trial = lax.broadcasted_iota(jnp.int32, blocks.shape, 1) % TRIALS
    return blocks * TRIALS + trial


def inflow_of(code, arrived, rows):
    row = lax.broadcasted_iota(jnp.int32, (rows, code.shape[1]), 0)
    return jnp.dot(one_hot(row, code), arrived, preferred_element_type=jnp.float32)


def update(b, inflow, volts_ref, cur_ref, ext_ref, spikes_ref, dsyn_ref, dmem_ref):
    at = lanes(b)
    dsyn = dsyn_ref[b : b + 1, :]
    dmem = dmem_ref[b : b + 1, :]
    cur = dsyn * cur_ref[:, at] + inflow[b * TRIALS : (b + 1) * TRIALS, :]
    volts = (
        dmem * volts_ref[:, at]
        + (1.0 - dmem) * (cur + ext_ref[:, at])
        - reset_size * spikes_ref[:, at]
    )
    return volts, cur


def step_kernel(step, *refs):
    (route_ref, src_ref, arrived_ref, codes_ref, volts_ref, cur_ref, ext_ref,
     spikes_ref, dsyn_ref, dmem_ref, pops_ref, table_ref) = refs[:12]
    volts_out, cur_out, spikes_out, out_ref, act_ref = refs[12:17]
    route_s, src_s, blocks_ref, rows_ref, sems = refs[-5:]
    devs = out_ref.shape[0]
    count = blocks_ref.shape[0]
    tpt = table_ref.shape[0] // devs
    to_smem = (
        pltpu.make_async_copy(route_ref.at[step : step + 1], route_s, sems.at[0]),
        pltpu.make_async_copy(src_ref, src_s, sems.at[1]),
    )
    for copy in to_smem:
        copy.start()
    if step == 1:
        codes = codes_of(arrived_ref[:, TRIALS:, :].reshape(devs * TRIALS, BLOCK))
        refs[17][...] = codes
        arrived = arrived_ref[:, :TRIALS, :].reshape(devs * TRIALS, BLOCK)
    else:
        codes = codes_ref[...]
        arrived = arrived_ref[...].reshape(devs * TRIALS, BLOCK)
    inflow = inflow_of(codes[step - 1 : step, :], arrived, count * TRIALS)
    for b in range(count):
        volts, cur = update(
            b, inflow, volts_ref, cur_ref, ext_ref, spikes_ref, dsyn_ref, dmem_ref
        )
        volts_out[:, lanes(b)] = volts
        cur_out[:, lanes(b)] = cur
        spikes = spike_of(volts)
        spikes_out[:, lanes(b)] = spikes
        rows_ref[b * TRIALS : (b + 1) * TRIALS, :] = spikes
        blocks_ref[b] = spikes.astype(jnp.bfloat16)
    act_ref[...] = activity_of(population_rows(pops_ref[...]), rows_ref[...])
    for copy in to_smem:
        copy.wait()
    send_tiles(0, devs, tpt, 0, route_s, src_s, blocks_ref, table_ref, out_ref)


def last_kernel(step, arrived_ref, codes_ref, volts_ref, cur_ref, ext_ref, spikes_ref,
                dsyn_ref, dmem_ref, volts_out, cur_out):
    devs = arrived_ref.shape[0]
    count = dsyn_ref.shape[0]
    arrived = arrived_ref[...].reshape(devs * TRIALS, BLOCK)
    inflow = inflow_of(codes_ref[step - 1 : step, :], arrived, count * TRIALS)
    for b in range(count):
        volts, cur = update(
            b, inflow, volts_ref, cur_ref, ext_ref, spikes_ref, dsyn_ref, dmem_ref
        )
        volts_out[:, lanes(b)] = volts
        cur_out[:, lanes(b)] = cur


def shards(
    potential,
    current,
    ext_drive,
    decay_syn,
    decay_mem,
    weights,
    tile_src,
    tile_dst,
    blk_pop,
    tile_route,
    counts,
):
    devs, tpt = weights.shape[1:3]
    count = blk_pop.shape[0]
    steps = tile_route.shape[0]
    f32, bf16, i32 = jnp.float32, jnp.bfloat16, jnp.int32
    table = weights.reshape(devs * tpt, BLOCK, BLOCK)
    src = tile_src[0].T
    dst = tile_dst[0].T
    route = tile_route.reshape(steps, 1, devs)
    used = counts.reshape(steps, 1, devs)
    dsyn = decay_syn.reshape(count, BLOCK)
    dmem = decay_mem.reshape(count, BLOCK)
    pops = blk_pop.reshape(1, count)
    state = jax.ShapeDtypeStruct((TRIALS, count * BLOCK), f32)
    sent = jax.ShapeDtypeStruct((devs, TRIALS, BLOCK), bf16)
    act = jax.ShapeDtypeStruct((POPS * TRIALS, BLOCK), f32)
    scratch = [
        pltpu.SMEM((1, 1, devs), i32),
        pltpu.SMEM((tpt, devs), i32),
    ]
    blocks = [
        pltpu.VMEM((count, TRIALS, BLOCK), bf16),
        pltpu.VMEM((count * TRIALS, BLOCK), f32),
    ]

    def exchange(out):
        return lax.all_to_all(out, ("area", "local"), 0, 0, tiled=True)

    def in_hbm(array):
        return pltpu.with_memory_space_constraint(array, pltpu.HBM)

    out, spikes, local_table, activity = pl.pallas_call(
        first_kernel,
        out_shape=(
            jax.ShapeDtypeStruct((devs, 2 * TRIALS, BLOCK), bf16),
            state,
            pltpu.VMEM(table.shape, bf16),
            act,
        ),
        in_specs=[HBM] * 7,
        out_specs=(VMEM,) * 4,
        scratch_shapes=scratch
        + [
            pltpu.VMEM((steps, 1, devs), i32),
            pltpu.VMEM((tpt, devs), i32),
            pltpu.VMEM((steps, 1, devs), i32),
            pltpu.VMEM(state.shape, f32),
            pltpu.VMEM((1, count), i32),
        ]
        + blocks
        + [pltpu.SemaphoreType.DMA((7,)), pltpu.SemaphoreType.DMA((CHUNKS,))],
        compiler_params=params(8),
        name="first",
    )(*[in_hbm(a) for a in (route, src, dst, used, potential, pops, table)])
    arrived = exchange(out)
    volts, cur = potential, current
    codes = jnp.zeros((8, devs * TRIALS), i32)
    history = [activity]
    for step in range(1, steps):
        outs = [state, state, state, sent, act]
        if step == 1:
            outs.append(jax.ShapeDtypeStruct((8, devs * TRIALS), i32))
        results = pl.pallas_call(
            functools.partial(step_kernel, step),
            out_shape=tuple(outs),
            in_specs=[VMEM] * 12,
            out_specs=(VMEM,) * len(outs),
            scratch_shapes=scratch + blocks + [pltpu.SemaphoreType.DMA((2,))],
            compiler_params=params(8),
            name=f"step{step}",
        )(route, src, arrived, codes, volts, cur, ext_drive, spikes, dsyn, dmem, pops, local_table)
        volts, cur, spikes, out, activity = results[:5]
        if step == 1:
            codes = results[5]
        history.append(activity)
        if step == steps - 1:
            history, out = lax.optimization_barrier((history, out))
        arrived = exchange(out)
    rates = jnp.stack(history).sum(axis=2).reshape(steps, TRIALS, POPS)
    n_local = lax.axis_size("local")
    parts = [rates] + [
        lax.ppermute(rates, "local", [(i, (i + shift) % n_local) for i in range(n_local)])
        for shift in range(1, n_local)
    ]
    total = (parts[0] + parts[2]) + (parts[1] + parts[3])
    total = total / (BLOCK * count)
    volts, cur = pl.pallas_call(
        functools.partial(last_kernel, steps),
        out_shape=(state, state),
        in_specs=[VMEM] * 8,
        out_specs=(VMEM, VMEM),
        compiler_params=params(8),
        name="last",
    )(arrived, codes, volts, cur, ext_drive, spikes, dsyn, dmem)
    return volts, cur, total[None]


def solution(mesh):
    both = ("area", "local")
    in_specs = (
        P(None, both),
        P(None, both),
        P(None, both),
        P(both),
        P(both),
        P(both, None, None, None, None),
        P(both, None, None),
        P(both, None, None),
        P(both),
        P(None, both, None, None),
        P(None, both, None),
    )
    out_specs = (P(None, both), P(None, both), P("area", None, None, None))
    return jax.shard_map(shards, mesh=mesh, in_specs=in_specs, out_specs=out_specs, check_vma=False)
```

```python
import functools

import jax
import jax.numpy as jnp
from jax import lax
from jax.experimental import pallas as pl
from jax.experimental.pallas import tpu as pltpu
from jax.sharding import PartitionSpec as P

POPS = 8
BLOCK = 128
TRIALS = 8
NO_BLOCK = 64
EXTRA = 2
CHUNK = 16
WHOLE = 32

spike_gain = 4.0
threshold = 1.0
reset_size = 0.5

VMEM = pl.BlockSpec(memory_space=pltpu.VMEM)
HBM = pl.BlockSpec(memory_space=pltpu.HBM)


def params(mib, **more):
    return pltpu.CompilerParams(vmem_limit_bytes=mib << 20, **more)


def lanes(block):
    return slice(block * BLOCK, (block + 1) * BLOCK)


def spike_of(volts):
    return jax.nn.sigmoid(spike_gain * (volts - threshold))


def send_tiles(first, last, tile_of, route_ref, src_ref, blocks_ref, tiles_ref, store):
    for d in range(first, last, 2):
        k, l = route_ref[0, 0, d], route_ref[0, 0, d + 1]
        spikes = jnp.concatenate([blocks_ref[src_ref[k, d]], blocks_ref[src_ref[l, d + 1]]], axis=0)
        tiles = jnp.concatenate([tiles_ref[tile_of(d, k)], tiles_ref[tile_of(d + 1, l)]], axis=1)
        current = jnp.dot(spikes, tiles, preferred_element_type=jnp.float32).astype(jnp.bfloat16)
        store(d, current[:TRIALS, :BLOCK])
        store(d + 1, current[TRIALS:, BLOCK:])


def one_hot(row, col):
    return jnp.where(row == col, 1.0, 0.0).astype(jnp.bfloat16)


def population_rows(pops):
    count = pops.shape[1]
    spread = one_hot(
        lax.broadcasted_iota(jnp.int32, (count, count * TRIALS), 0),
        lax.broadcasted_iota(jnp.int32, (count, count * TRIALS), 1) // TRIALS,
    )
    pops = jnp.broadcast_to(pops.astype(jnp.float32), (TRIALS, count)).astype(jnp.bfloat16)
    pops = jnp.dot(pops, spread, preferred_element_type=jnp.float32)[0:1, :].astype(jnp.int32)
    trial = lax.broadcasted_iota(jnp.int32, pops.shape, 1) % TRIALS
    row = lax.broadcasted_iota(jnp.int32, (TRIALS * POPS, count * TRIALS), 0)
    return one_hot(row, trial * POPS + pops)


def activity_of(member, spikes):
    high = spikes.astype(jnp.bfloat16)
    low = (spikes - high.astype(jnp.float32)).astype(jnp.bfloat16)
    return jnp.dot(member, high, preferred_element_type=jnp.float32) + jnp.dot(
        member, low, preferred_element_type=jnp.float32
    )


def first_kernel(
    route_hbm, src_hbm, dst_hbm, counts_hbm, volts_hbm, pops_hbm, table_hbm,
    out_ref, spikes_ref, act_ref,
    route_s, src_s, routes_ref, dst_ref, counts_ref, volts_ref, pops_ref, tiles_ref,
    blocks_ref, rows_ref, sems, whole_sems, routed_sems,
):
    tpt, devs = dst_ref.shape
    steps = routes_ref.shape[0]
    copies = [
        pltpu.make_async_copy(a, b, sems.at[i])
        for i, (a, b) in enumerate(
            (
                (route_hbm.at[0:1], route_s),
                (src_hbm, src_s),
                (volts_hbm, volts_ref),
                (route_hbm, routes_ref),
                (dst_hbm, dst_ref),
                (counts_hbm, counts_ref),
                (pops_hbm, pops_ref),
            )
        )
    ]
    for copy in copies:
        copy.start()

    def whole(c):
        at = pl.ds(c * CHUNK * tpt, CHUNK * tpt)
        return pltpu.make_async_copy(table_hbm.at[at], tiles_ref.at[at], whole_sems.at[c])

    def start_whole(c, carry):
        whole(c).start()
        return carry

    lax.fori_loop(0, WHOLE // CHUNK, start_whole, 0)
    copies[0].wait()

    base = WHOLE * tpt - WHOLE

    def start_routed(c, carry):
        for j in range(CHUNK):
            d = WHOLE + c * CHUNK + j
            pltpu.make_async_copy(
                table_hbm.at[d * tpt + route_s[0, 0, d]], tiles_ref.at[base + d], routed_sems.at[c]
            ).start()
        return carry

    lax.fori_loop(0, (devs - WHOLE) // CHUNK, start_routed, 0)
    for copy in copies[3:6]:
        copy.wait()

    step = lax.broadcasted_iota(jnp.int32, (BLOCK, devs), 0)
    targets = jnp.zeros((BLOCK, devs), jnp.int32)
    for t in range(steps):
        target = jnp.where(routes_ref[t] == 0, dst_ref[0:1, :], dst_ref[1:2, :])
        target = jnp.where(counts_ref[t] > 0, target, NO_BLOCK)
        targets = jnp.where(step == t, target, targets)
    targets = targets.astype(jnp.float32).astype(jnp.bfloat16)
    rows = lax.broadcasted_iota(jnp.int32, (devs * EXTRA, devs), 0) // EXTRA
    cols = lax.broadcasted_iota(jnp.int32, (devs * EXTRA, devs), 1)
    extra = lax.dot_general(
        one_hot(rows, cols), targets, (((1,), (1,)), ((), ())), preferred_element_type=jnp.float32
    )
    extra = extra.astype(jnp.bfloat16)
    long = TRIALS + EXTRA
    for d in range(devs):
        out_ref[d * long + TRIALS : (d + 1) * long, :] = extra[d * EXTRA : (d + 1) * EXTRA, :]

    copies[2].wait()
    for b in range(blocks_ref.shape[0]):
        spikes = spike_of(volts_ref[:, lanes(b)])
        spikes_ref[:, lanes(b)] = spikes
        rows_ref[b * TRIALS : (b + 1) * TRIALS, :] = spikes
        blocks_ref[b] = spikes.astype(jnp.bfloat16)
    copies[6].wait()
    act_ref[...] = activity_of(population_rows(pops_ref[...]), rows_ref[...])
    copies[1].wait()

    def store(d, current):
        out_ref[d * long : d * long + TRIALS, :] = current

    for c in range(WHOLE // CHUNK):
        whole(c).wait()
        send_tiles(
            c * CHUNK, (c + 1) * CHUNK, lambda d, k: d * tpt + k, route_s, src_s, blocks_ref, tiles_ref, store
        )
    for c in range((devs - WHOLE) // CHUNK):
        at = WHOLE + c * CHUNK
        pltpu.make_async_copy(
            table_hbm.at[pl.ds(0, CHUNK)], tiles_ref.at[pl.ds(base + at, CHUNK)], routed_sems.at[c]
        ).wait()
        send_tiles(
            at, at + CHUNK, lambda d, k: base + d, route_s, src_s, blocks_ref, tiles_ref, store
        )


def iotas(shape):
    return lax.broadcasted_iota(jnp.int32, shape, 0), lax.broadcasted_iota(jnp.int32, shape, 1)


def codes_of(message, devs):
    long = TRIALS + EXTRA
    read = lax.dot_general(
        one_hot(*iotas((8, BLOCK))), message, (((1,), (1,)), ((), ())), preferred_element_type=jnp.float32
    )
    place = lax.broadcasted_iota(jnp.int32, read.shape, 1) % long
    blocks = jnp.where(place >= TRIALS, read, 0.0)
    near = blocks
    width = near.shape[1]
    near = pltpu.roll(near, width - 2, 1)
    near = near + pltpu.roll(near, width - 2, 1)
    near = near + pltpu.roll(near, width - 4, 1)
    here = jnp.where(place < TRIALS, near.astype(jnp.int32) * TRIALS + place, -1)
    row, col = iotas((devs * long, devs))
    one = jnp.dot(
        jnp.where(place == TRIALS, blocks, 0.0).astype(jnp.bfloat16),
        one_hot(row // long, col),
        preferred_element_type=jnp.float32,
    ).astype(jnp.bfloat16)
    row, col = iotas((devs, devs * TRIALS))
    later = jnp.dot(one, one_hot(row, col // TRIALS), preferred_element_type=jnp.float32)
    trial = lax.broadcasted_iota(jnp.int32, later.shape, 1) % TRIALS
    return here, later.astype(jnp.int32) * TRIALS + trial


def inflow_of(code, arrived, rows):
    row = lax.broadcasted_iota(jnp.int32, (rows, code.shape[1]), 0)
    return jnp.dot(one_hot(row, code), arrived, preferred_element_type=jnp.float32)


def update(b, inflow, volts_ref, cur_ref, ext_ref, spikes_ref, dsyn_ref, dmem_ref):
    at = lanes(b)
    dsyn = dsyn_ref[b : b + 1, :]
    dmem = dmem_ref[b : b + 1, :]
    cur = dsyn * cur_ref[:, at] + inflow[b * TRIALS : (b + 1) * TRIALS, :]
    volts = (
        dmem * volts_ref[:, at]
        + (1.0 - dmem) * (cur + ext_ref[:, at])
        - reset_size * spikes_ref[:, at]
    )
    return volts, cur


def step_kernel(step, *refs):
    (route_ref, src_ref, arrived_ref, codes_ref, volts_ref, cur_ref, ext_ref,
     spikes_ref, dsyn_ref, dmem_ref, pops_ref, table_ref) = refs[:12]
    volts_out, cur_out, spikes_out, out_ref, act_ref = refs[12:17]
    route_s, src_s, blocks_ref, rows_ref, sems = refs[-5:]
    devs = out_ref.shape[0]
    count = blocks_ref.shape[0]
    tpt = table_ref.shape[0] // devs
    to_smem = (
        pltpu.make_async_copy(route_ref.at[step : step + 1], route_s, sems.at[0]),
        pltpu.make_async_copy(src_ref, src_s, sems.at[1]),
    )
    for copy in to_smem:
        copy.start()
    if step == 1:
        arrived = arrived_ref[...]
        codes, later = codes_of(arrived, devs)
        refs[17][...] = later
    else:
        codes = codes_ref[...]
        arrived = arrived_ref[...].reshape(devs * TRIALS, BLOCK)
    inflow = inflow_of(codes[step - 1 : step, :], arrived, count * TRIALS)
    for b in range(count):
        volts, cur = update(
            b, inflow, volts_ref, cur_ref, ext_ref, spikes_ref, dsyn_ref, dmem_ref
        )
        volts_out[:, lanes(b)] = volts
        cur_out[:, lanes(b)] = cur
        spikes = spike_of(volts)
        spikes_out[:, lanes(b)] = spikes
        rows_ref[b * TRIALS : (b + 1) * TRIALS, :] = spikes
        blocks_ref[b] = spikes.astype(jnp.bfloat16)
    act_ref[...] = activity_of(population_rows(pops_ref[...]), rows_ref[...])
    for copy in to_smem:
        copy.wait()

    def store(d, current):
        out_ref[d] = current

    send_tiles(0, devs, lambda d, k: d * tpt + k, route_s, src_s, blocks_ref, table_ref, store)


def last_kernel(step, arrived_ref, codes_ref, volts_ref, cur_ref, ext_ref, spikes_ref,
                dsyn_ref, dmem_ref, volts_out, cur_out):
    devs = arrived_ref.shape[0]
    count = dsyn_ref.shape[0]
    arrived = arrived_ref[...].reshape(devs * TRIALS, BLOCK)
    inflow = inflow_of(codes_ref[step - 1 : step, :], arrived, count * TRIALS)
    for b in range(count):
        volts, cur = update(
            b, inflow, volts_ref, cur_ref, ext_ref, spikes_ref, dsyn_ref, dmem_ref
        )
        volts_out[:, lanes(b)] = volts
        cur_out[:, lanes(b)] = cur


def shards(
    potential,
    current,
    ext_drive,
    decay_syn,
    decay_mem,
    weights,
    tile_src,
    tile_dst,
    blk_pop,
    tile_route,
    counts,
):
    devs, tpt = weights.shape[1:3]
    count = blk_pop.shape[0]
    steps = tile_route.shape[0]
    f32, bf16, i32 = jnp.float32, jnp.bfloat16, jnp.int32
    table = weights.reshape(devs * tpt, BLOCK, BLOCK)
    src = tile_src[0].T
    dst = tile_dst[0].T
    route = tile_route.reshape(steps, 1, devs)
    used = counts.reshape(steps, 1, devs)
    dsyn = decay_syn.reshape(count, BLOCK)
    dmem = decay_mem.reshape(count, BLOCK)
    pops = blk_pop.reshape(1, count)
    state = jax.ShapeDtypeStruct((TRIALS, count * BLOCK), f32)
    sent = jax.ShapeDtypeStruct((devs, TRIALS, BLOCK), bf16)
    act = jax.ShapeDtypeStruct((POPS * TRIALS, BLOCK), f32)
    scratch = [
        pltpu.SMEM((1, 1, devs), i32),
        pltpu.SMEM((tpt, devs), i32),
    ]
    blocks = [
        pltpu.VMEM((count, TRIALS, BLOCK), bf16),
        pltpu.VMEM((count * TRIALS, BLOCK), f32),
    ]

    def exchange(out):
        return lax.all_to_all(out, ("area", "local"), 0, 0, tiled=True)

    def in_hbm(array):
        return pltpu.with_memory_space_constraint(array, pltpu.HBM)

    long = TRIALS + EXTRA
    out, spikes, activity = pl.pallas_call(
        first_kernel,
        out_shape=(jax.ShapeDtypeStruct((devs * long, BLOCK), bf16), state, act),
        in_specs=[HBM] * 7,
        out_specs=(VMEM,) * 3,
        scratch_shapes=scratch
        + [
            pltpu.VMEM((steps, 1, devs), i32),
            pltpu.VMEM((tpt, devs), i32),
            pltpu.VMEM((steps, 1, devs), i32),
            pltpu.VMEM(state.shape, f32),
            pltpu.VMEM((1, count), i32),
            pltpu.VMEM((devs + WHOLE * (tpt - 1), BLOCK, BLOCK), bf16),
        ]
        + blocks
        + [
            pltpu.SemaphoreType.DMA((7,)),
            pltpu.SemaphoreType.DMA((WHOLE // CHUNK,)),
            pltpu.SemaphoreType.DMA(((devs - WHOLE) // CHUNK,)),
        ],
        compiler_params=params(16),
        name="first",
    )(*[in_hbm(a) for a in (route, src, dst, used, potential, pops, table)])
    arrived = exchange(out.reshape(devs, long // 2, 2, BLOCK)).reshape(devs * long, BLOCK)
    local_table = table
    volts, cur = potential, current
    codes = jnp.zeros((8, devs * TRIALS), i32)
    history = [activity]
    for step in range(1, steps):
        outs = [state, state, state, sent, act]
        if step == steps - 1:
            outs[3] = pltpu.VMEM(sent.shape, bf16)
        if step == 1:
            outs.append(jax.ShapeDtypeStruct((8, devs * TRIALS), i32))
        results = pl.pallas_call(
            functools.partial(step_kernel, step),
            out_shape=tuple(outs),
            in_specs=[VMEM] * 12,
            out_specs=(VMEM,) * len(outs),
            scratch_shapes=scratch + blocks + [pltpu.SemaphoreType.DMA((2,))],
            compiler_params=params(8),
            name=f"step{step}",
        )(route, src, arrived, codes, volts, cur, ext_drive, spikes, dsyn, dmem, pops, local_table)
        volts, cur, spikes, out, activity = results[:5]
        if step == 1:
            codes = results[5]
        history.append(activity)
        if step == steps - 1:
            history, out = lax.optimization_barrier((history, out))
        arrived = exchange(out)
    rates = jnp.stack(history).sum(axis=2).reshape(steps, TRIALS, POPS)
    n_local = lax.axis_size("local")
    parts = [rates] + [
        lax.ppermute(rates, "local", [(i, (i + shift) % n_local) for i in range(n_local)])
        for shift in range(1, n_local)
    ]
    total = (parts[0] + parts[2]) + (parts[1] + parts[3])
    total = total / (BLOCK * count)
    volts, cur = pl.pallas_call(
        functools.partial(last_kernel, steps),
        out_shape=(state, state),
        in_specs=[VMEM] * 8,
        out_specs=(VMEM, VMEM),
        compiler_params=params(8),
        name="last",
    )(arrived, codes, volts, cur, ext_drive, spikes, dsyn, dmem)
    return volts, cur, total[None]


def solution(mesh):
    both = ("area", "local")
    in_specs = (
        P(None, both),
        P(None, both),
        P(None, both),
        P(both),
        P(both),
        P(both, None, None, None, None),
        P(both, None, None),
        P(both, None, None),
        P(both),
        P(None, both, None, None),
        P(None, both, None),
    )
    out_specs = (P(None, both), P(None, both), P("area", None, None, None))
    return jax.shard_map(shards, mesh=mesh, in_specs=in_specs, out_specs=out_specs, check_vma=False)
```

```python
import functools

import jax
import jax.numpy as jnp
from jax import lax
from jax.experimental import pallas as pl
from jax.experimental.pallas import tpu as pltpu
from jax.sharding import PartitionSpec as P

POPS = 8
BLOCK = 128
TRIALS = 8
NO_BLOCK = 64
EXTRA = 2
CHUNK = 16
WHOLE = 32

spike_gain = 4.0
threshold = 1.0
reset_size = 0.5

VMEM = pl.BlockSpec(memory_space=pltpu.VMEM)
ANY = pl.BlockSpec(memory_space=pl.ANY)
HBM = pl.BlockSpec(memory_space=pltpu.HBM)


def params(mib, **more):
    return pltpu.CompilerParams(vmem_limit_bytes=mib << 20, **more)


def lanes(block):
    return slice(block * BLOCK, (block + 1) * BLOCK)


def spike_of(volts):
    return jax.nn.sigmoid(spike_gain * (volts - threshold))


def send_tiles(first, last, tile_of, route_ref, src_ref, blocks_ref, tiles_ref, store):
    for d in range(first, last, 2):
        k, l = route_ref[0, 0, d], route_ref[0, 0, d + 1]
        spikes = jnp.concatenate([blocks_ref[src_ref[k, d]], blocks_ref[src_ref[l, d + 1]]], axis=0)
        tiles = jnp.concatenate([tiles_ref[tile_of(d, k)], tiles_ref[tile_of(d + 1, l)]], axis=1)
        current = jnp.dot(spikes, tiles, preferred_element_type=jnp.float32).astype(jnp.bfloat16)
        store(d, current[:TRIALS, :BLOCK])
        store(d + 1, current[TRIALS:, BLOCK:])


def one_hot(row, col):
    return jnp.where(row == col, 1.0, 0.0).astype(jnp.bfloat16)


def population_rows(pops):
    count = pops.shape[1]
    spread = one_hot(
        lax.broadcasted_iota(jnp.int32, (count, count * TRIALS), 0),
        lax.broadcasted_iota(jnp.int32, (count, count * TRIALS), 1) // TRIALS,
    )
    pops = jnp.broadcast_to(pops.astype(jnp.float32), (TRIALS, count)).astype(jnp.bfloat16)
    pops = jnp.dot(pops, spread, preferred_element_type=jnp.float32)[0:1, :].astype(jnp.int32)
    trial = lax.broadcasted_iota(jnp.int32, pops.shape, 1) % TRIALS
    row = lax.broadcasted_iota(jnp.int32, (TRIALS * POPS, count * TRIALS), 0)
    return one_hot(row, trial * POPS + pops)


def activity_of(member, spikes):
    high = spikes.astype(jnp.bfloat16)
    low = (spikes - high.astype(jnp.float32)).astype(jnp.bfloat16)
    return jnp.dot(member, high, preferred_element_type=jnp.float32) + jnp.dot(
        member, low, preferred_element_type=jnp.float32
    )


def first_kernel(
    route_hbm, src_hbm, dst_hbm, counts_hbm, volts_hbm, pops_hbm, table_hbm,
    out_ref, spikes_ref, act_ref,
    route_s, src_s, routes_ref, dst_ref, counts_ref, volts_ref, pops_ref, tiles_ref,
    blocks_ref, rows_ref, sems, whole_sems, routed_sems,
):
    tpt, devs = dst_ref.shape
    steps = routes_ref.shape[0]
    copies = [
        pltpu.make_async_copy(a, b, sems.at[i])
        for i, (a, b) in enumerate(
            (
                (route_hbm.at[0:1], route_s),
                (src_hbm, src_s),
                (volts_hbm, volts_ref),
                (route_hbm, routes_ref),
                (dst_hbm, dst_ref),
                (counts_hbm, counts_ref),
                (pops_hbm, pops_ref),
            )
        )
    ]
    for copy in copies:
        copy.start()

    def whole(c):
        at = pl.ds(c * CHUNK * tpt, CHUNK * tpt)
        return pltpu.make_async_copy(table_hbm.at[at], tiles_ref.at[at], whole_sems.at[c])

    def start_whole(c, carry):
        whole(c).start()
        return carry

    lax.fori_loop(0, WHOLE // CHUNK, start_whole, 0)
    copies[0].wait()

    base = WHOLE * tpt - WHOLE

    def start_routed(c, carry):
        for j in range(CHUNK):
            d = WHOLE + c * CHUNK + j
            pltpu.make_async_copy(
                table_hbm.at[d * tpt + route_s[0, 0, d]], tiles_ref.at[base + d], routed_sems.at[c]
            ).start()
        return carry

    lax.fori_loop(0, (devs - WHOLE) // CHUNK, start_routed, 0)
    for copy in copies[3:6]:
        copy.wait()

    step = lax.broadcasted_iota(jnp.int32, (BLOCK, devs), 0)
    targets = jnp.zeros((BLOCK, devs), jnp.int32)
    for t in range(steps):
        target = jnp.where(routes_ref[t] == 0, dst_ref[0:1, :], dst_ref[1:2, :])
        target = jnp.where(counts_ref[t] > 0, target, NO_BLOCK)
        targets = jnp.where(step == t, target, targets)
    targets = targets.astype(jnp.float32).astype(jnp.bfloat16)
    rows = lax.broadcasted_iota(jnp.int32, (devs * EXTRA, devs), 0) // EXTRA
    cols = lax.broadcasted_iota(jnp.int32, (devs * EXTRA, devs), 1)
    extra = lax.dot_general(
        one_hot(rows, cols), targets, (((1,), (1,)), ((), ())), preferred_element_type=jnp.float32
    )
    extra = extra.astype(jnp.bfloat16)
    long = TRIALS + EXTRA
    for d in range(devs):
        out_ref[d * long + TRIALS : (d + 1) * long, :] = extra[d * EXTRA : (d + 1) * EXTRA, :]

    copies[2].wait()
    for b in range(blocks_ref.shape[0]):
        spikes = spike_of(volts_ref[:, lanes(b)])
        spikes_ref[:, lanes(b)] = spikes
        rows_ref[b * TRIALS : (b + 1) * TRIALS, :] = spikes
        blocks_ref[b] = spikes.astype(jnp.bfloat16)
    copies[6].wait()
    act_ref[...] = activity_of(population_rows(pops_ref[...]), rows_ref[...])
    copies[1].wait()

    def store(d, current):
        out_ref[d * long : d * long + TRIALS, :] = current

    for c in range(WHOLE // CHUNK):
        whole(c).wait()
        send_tiles(
            c * CHUNK, (c + 1) * CHUNK, lambda d, k: d * tpt + k, route_s, src_s, blocks_ref, tiles_ref, store
        )
    for c in range((devs - WHOLE) // CHUNK):
        at = WHOLE + c * CHUNK
        pltpu.make_async_copy(
            table_hbm.at[pl.ds(0, CHUNK)], tiles_ref.at[pl.ds(base + at, CHUNK)], routed_sems.at[c]
        ).wait()
        send_tiles(
            at, at + CHUNK, lambda d, k: base + d, route_s, src_s, blocks_ref, tiles_ref, store
        )


def gate_kernel(message_ref, out_ref):
    pass


def iotas(shape):
    return lax.broadcasted_iota(jnp.int32, shape, 0), lax.broadcasted_iota(jnp.int32, shape, 1)


def codes_of(message, devs):
    long = TRIALS + EXTRA
    read = lax.dot_general(
        one_hot(*iotas((8, BLOCK))), message, (((1,), (1,)), ((), ())), preferred_element_type=jnp.float32
    )
    place = lax.broadcasted_iota(jnp.int32, read.shape, 1) % long
    blocks = jnp.where(place >= TRIALS, read, 0.0)
    near = blocks
    width = near.shape[1]
    near = pltpu.roll(near, width - 2, 1)
    near = near + pltpu.roll(near, width - 2, 1)
    near = near + pltpu.roll(near, width - 4, 1)
    here = jnp.where(place < TRIALS, near.astype(jnp.int32) * TRIALS + place, -1)
    row, col = iotas((devs * long, devs))
    one = jnp.dot(
        jnp.where(place == TRIALS, blocks, 0.0).astype(jnp.bfloat16),
        one_hot(row // long, col),
        preferred_element_type=jnp.float32,
    ).astype(jnp.bfloat16)
    row, col = iotas((devs, devs * TRIALS))
    later = jnp.dot(one, one_hot(row, col // TRIALS), preferred_element_type=jnp.float32)
    trial = lax.broadcasted_iota(jnp.int32, later.shape, 1) % TRIALS
    return here, later.astype(jnp.int32) * TRIALS + trial


def inflow_of(code, arrived, rows):
    row = lax.broadcasted_iota(jnp.int32, (rows, code.shape[1]), 0)
    return jnp.dot(one_hot(row, code), arrived, preferred_element_type=jnp.float32)


def update(b, inflow, volts_ref, cur_ref, ext_ref, spikes_ref, dsyn_ref, dmem_ref):
    at = lanes(b)
    dsyn = dsyn_ref[b : b + 1, :]
    dmem = dmem_ref[b : b + 1, :]
    cur = dsyn * cur_ref[:, at] + inflow[b * TRIALS : (b + 1) * TRIALS, :]
    volts = (
        dmem * volts_ref[:, at]
        + (1.0 - dmem) * (cur + ext_ref[:, at])
        - reset_size * spikes_ref[:, at]
    )
    return volts, cur


def step_kernel(step, *refs):
    (route_ref, src_ref, arrived_ref, codes_ref, volts_ref, cur_ref, ext_ref,
     spikes_ref, dsyn_ref, dmem_ref, pops_ref, table_ref) = refs[:12]
    volts_out, cur_out, spikes_out, out_ref, act_ref = refs[12:17]
    route_s, src_s, blocks_ref, rows_ref, sems = refs[-5:]
    devs = out_ref.shape[0]
    count = blocks_ref.shape[0]
    tpt = table_ref.shape[0] // devs
    to_smem = (
        pltpu.make_async_copy(route_ref.at[step : step + 1], route_s, sems.at[0]),
        pltpu.make_async_copy(src_ref, src_s, sems.at[1]),
    )
    for copy in to_smem:
        copy.start()
    if step == 1:
        arrived = arrived_ref[...]
        codes, later = codes_of(arrived, devs)
        refs[17][...] = later
    else:
        codes = codes_ref[...]
        arrived = arrived_ref[...].reshape(devs * TRIALS, BLOCK)
    inflow = inflow_of(codes[step - 1 : step, :], arrived, count * TRIALS)
    for b in range(count):
        volts, cur = update(
            b, inflow, volts_ref, cur_ref, ext_ref, spikes_ref, dsyn_ref, dmem_ref
        )
        volts_out[:, lanes(b)] = volts
        cur_out[:, lanes(b)] = cur
        spikes = spike_of(volts)
        spikes_out[:, lanes(b)] = spikes
        rows_ref[b * TRIALS : (b + 1) * TRIALS, :] = spikes
        blocks_ref[b] = spikes.astype(jnp.bfloat16)
    act_ref[...] = activity_of(population_rows(pops_ref[...]), rows_ref[...])
    for copy in to_smem:
        copy.wait()

    def store(d, current):
        out_ref[d] = current

    send_tiles(0, devs, lambda d, k: d * tpt + k, route_s, src_s, blocks_ref, table_ref, store)


def last_kernel(step, arrived_ref, codes_ref, volts_ref, cur_ref, ext_ref, spikes_ref,
                dsyn_ref, dmem_ref, volts_out, cur_out):
    devs = arrived_ref.shape[0]
    count = dsyn_ref.shape[0]
    arrived = arrived_ref[...].reshape(devs * TRIALS, BLOCK)
    inflow = inflow_of(codes_ref[step - 1 : step, :], arrived, count * TRIALS)
    for b in range(count):
        volts, cur = update(
            b, inflow, volts_ref, cur_ref, ext_ref, spikes_ref, dsyn_ref, dmem_ref
        )
        volts_out[:, lanes(b)] = volts
        cur_out[:, lanes(b)] = cur


def shards(
    potential,
    current,
    ext_drive,
    decay_syn,
    decay_mem,
    weights,
    tile_src,
    tile_dst,
    blk_pop,
    tile_route,
    counts,
):
    devs, tpt = weights.shape[1:3]
    count = blk_pop.shape[0]
    steps = tile_route.shape[0]
    f32, bf16, i32 = jnp.float32, jnp.bfloat16, jnp.int32
    table = weights.reshape(devs * tpt, BLOCK, BLOCK)
    src = tile_src[0].T
    dst = tile_dst[0].T
    route = tile_route.reshape(steps, 1, devs)
    used = counts.reshape(steps, 1, devs)
    dsyn = decay_syn.reshape(count, BLOCK)
    dmem = decay_mem.reshape(count, BLOCK)
    pops = blk_pop.reshape(1, count)
    state = jax.ShapeDtypeStruct((TRIALS, count * BLOCK), f32)
    sent = jax.ShapeDtypeStruct((devs, TRIALS, BLOCK), bf16)
    act = jax.ShapeDtypeStruct((POPS * TRIALS, BLOCK), f32)
    scratch = [
        pltpu.SMEM((1, 1, devs), i32),
        pltpu.SMEM((tpt, devs), i32),
    ]
    blocks = [
        pltpu.VMEM((count, TRIALS, BLOCK), bf16),
        pltpu.VMEM((count * TRIALS, BLOCK), f32),
    ]

    def exchange(out):
        return lax.all_to_all(out, ("area", "local"), 0, 0, tiled=True)

    def in_hbm(array):
        return pltpu.with_memory_space_constraint(array, pltpu.HBM)

    long = TRIALS + EXTRA
    out, spikes, activity = pl.pallas_call(
        first_kernel,
        out_shape=(jax.ShapeDtypeStruct((devs * long, BLOCK), bf16), state, act),
        in_specs=[HBM] * 7,
        out_specs=(VMEM,) * 3,
        scratch_shapes=scratch
        + [
            pltpu.VMEM((steps, 1, devs), i32),
            pltpu.VMEM((tpt, devs), i32),
            pltpu.VMEM((steps, 1, devs), i32),
            pltpu.VMEM(state.shape, f32),
            pltpu.VMEM((1, count), i32),
            pltpu.VMEM((devs + WHOLE * (tpt - 1), BLOCK, BLOCK), bf16),
        ]
        + blocks
        + [
            pltpu.SemaphoreType.DMA((7,)),
            pltpu.SemaphoreType.DMA((WHOLE // CHUNK,)),
            pltpu.SemaphoreType.DMA(((devs - WHOLE) // CHUNK,)),
        ],
        compiler_params=params(16),
        name="first",
    )(*[in_hbm(a) for a in (route, src, dst, used, potential, pops, table)])
    for i in range(2):
        out = pl.pallas_call(
            gate_kernel,
            out_shape=jax.ShapeDtypeStruct(out.shape, out.dtype),
            in_specs=[ANY],
            out_specs=ANY,
            input_output_aliases={0: 0},
            cost_estimate=pl.CostEstimate(flops=6_000_000_000, bytes_accessed=0, transcendentals=0),
            compiler_params=params(1),
            name=f"gate{i}",
        )(out)
    arrived = exchange(out.reshape(devs, long // 2, 2, BLOCK)).reshape(devs * long, BLOCK)
    local_table = table
    volts, cur = potential, current
    codes = jnp.zeros((8, devs * TRIALS), i32)
    history = [activity]
    for step in range(1, steps):
        outs = [state, state, state, sent, act]
        if step == steps - 1:
            outs[3] = pltpu.VMEM(sent.shape, bf16)
        if step == 1:
            outs.append(jax.ShapeDtypeStruct((8, devs * TRIALS), i32))
        results = pl.pallas_call(
            functools.partial(step_kernel, step),
            out_shape=tuple(outs),
            in_specs=[VMEM] * 12,
            out_specs=(VMEM,) * len(outs),
            scratch_shapes=scratch + blocks + [pltpu.SemaphoreType.DMA((2,))],
            compiler_params=params(8),
            name=f"step{step}",
        )(route, src, arrived, codes, volts, cur, ext_drive, spikes, dsyn, dmem, pops, local_table)
        volts, cur, spikes, out, activity = results[:5]
        if step == 1:
            codes = results[5]
        history.append(activity)
        if step == steps - 1:
            history, out = lax.optimization_barrier((history, out))
        arrived = exchange(out)
    rates = jnp.stack(history).sum(axis=2).reshape(steps, TRIALS, POPS)
    n_local = lax.axis_size("local")
    parts = [rates] + [
        lax.ppermute(rates, "local", [(i, (i + shift) % n_local) for i in range(n_local)])
        for shift in range(1, n_local)
    ]
    total = (parts[0] + parts[2]) + (parts[1] + parts[3])
    total = total / (BLOCK * count)
    volts, cur = pl.pallas_call(
        functools.partial(last_kernel, steps),
        out_shape=(state, state),
        in_specs=[VMEM] * 8,
        out_specs=(VMEM, VMEM),
        compiler_params=params(8),
        name="last",
    )(arrived, codes, volts, cur, ext_drive, spikes, dsyn, dmem)
    return volts, cur, total[None]


def solution(mesh):
    both = ("area", "local")
    in_specs = (
        P(None, both),
        P(None, both),
        P(None, both),
        P(both),
        P(both),
        P(both, None, None, None, None),
        P(both, None, None),
        P(both, None, None),
        P(both),
        P(None, both, None, None),
        P(None, both, None),
    )
    out_specs = (P(None, both), P(None, both), P("area", None, None, None))
    return jax.shard_map(shards, mesh=mesh, in_specs=in_specs, out_specs=out_specs, check_vma=False)
```

```python
import functools

import jax
import jax.numpy as jnp
from jax import lax
from jax.experimental import pallas as pl
from jax.experimental.pallas import tpu as pltpu
from jax.sharding import PartitionSpec as P

POPS = 8
BLOCK = 128
TRIALS = 8
NO_BLOCK = 64
EXTRA = 2
PIECES = 4
CHUNK = 32
WHOLE = 32

spike_gain = 4.0
threshold = 1.0
reset_size = 0.5

VMEM = pl.BlockSpec(memory_space=pltpu.VMEM)
ANY = pl.BlockSpec(memory_space=pl.ANY)
HBM = pl.BlockSpec(memory_space=pltpu.HBM)


def params(mib, **more):
    return pltpu.CompilerParams(vmem_limit_bytes=mib << 20, **more)


def lanes(block):
    return slice(block * BLOCK, (block + 1) * BLOCK)


def spike_of(volts):
    return jax.nn.sigmoid(spike_gain * (volts - threshold))


def send_tiles(first, last, pick, blocks_ref, tiles_ref, store):
    for d in range(first, last, 2):
        (block, tile), (block_b, tile_b) = pick(d), pick(d + 1)
        spikes = jnp.concatenate([blocks_ref[block], blocks_ref[block_b]], axis=0)
        tiles = jnp.concatenate([tiles_ref[tile], tiles_ref[tile_b]], axis=1)
        current = jnp.dot(spikes, tiles, preferred_element_type=jnp.float32).astype(jnp.bfloat16)
        store(d, current[:TRIALS, :BLOCK])
        store(d + 1, current[TRIALS:, BLOCK:])


def one_hot(row, col):
    return jnp.where(row == col, 1.0, 0.0).astype(jnp.bfloat16)


def population_rows(pops):
    count = pops.shape[1]
    spread = one_hot(
        lax.broadcasted_iota(jnp.int32, (count, count * TRIALS), 0),
        lax.broadcasted_iota(jnp.int32, (count, count * TRIALS), 1) // TRIALS,
    )
    pops = jnp.broadcast_to(pops.astype(jnp.float32), (TRIALS, count)).astype(jnp.bfloat16)
    pops = jnp.dot(pops, spread, preferred_element_type=jnp.float32)[0:1, :].astype(jnp.int32)
    trial = lax.broadcasted_iota(jnp.int32, pops.shape, 1) % TRIALS
    row = lax.broadcasted_iota(jnp.int32, (TRIALS * POPS, count * TRIALS), 0)
    return one_hot(row, trial * POPS + pops)


def activity_of(member, spikes):
    high = spikes.astype(jnp.bfloat16)
    low = (spikes - high.astype(jnp.float32)).astype(jnp.bfloat16)
    return jnp.dot(member, high, preferred_element_type=jnp.float32) + jnp.dot(
        member, low, preferred_element_type=jnp.float32
    )


def first_kernel(
    route_hbm, src_hbm, dst_hbm, counts_hbm, volts_hbm, pops_hbm, table_hbm,
    out_ref, spikes_ref, act_ref, chosen_ref,
    route_s, src_s, routes_ref, from_ref, dst_ref, counts_ref, volts_ref, pops_ref, tiles_ref,
    blocks_ref, rows_ref, sems, whole_sems, routed_sems,
):
    tpt, devs = dst_ref.shape
    steps = routes_ref.shape[0]
    copies = [
        pltpu.make_async_copy(a, b, sems.at[i])
        for i, (a, b) in enumerate(
            (
                (route_hbm.at[0:1], route_s),
                (src_hbm, src_s),
                (volts_hbm, volts_ref),
                (route_hbm, routes_ref),
                (dst_hbm, dst_ref),
                (counts_hbm, counts_ref),
                (src_hbm, from_ref),
                (pops_hbm, pops_ref),
            )
        )
    ]
    for copy in copies:
        copy.start()

    def whole(c):
        at = pl.ds(c * CHUNK * tpt, CHUNK * tpt)
        return pltpu.make_async_copy(table_hbm.at[at], tiles_ref.at[at], whole_sems.at[c])

    def start_whole(c, carry):
        whole(c).start()
        return carry

    lax.fori_loop(0, WHOLE // CHUNK, start_whole, 0)
    copies[0].wait()

    base = WHOLE * tpt - WHOLE

    def start_routed(c, carry):
        for j in range(CHUNK):
            d = WHOLE + c * CHUNK + j
            pltpu.make_async_copy(
                table_hbm.at[d * tpt + route_s[0, 0, d]], tiles_ref.at[base + d], routed_sems.at[c]
            ).start()
        return carry

    lax.fori_loop(0, (devs - WHOLE) // CHUNK, start_routed, 0)
    for copy in copies[3:7]:
        copy.wait()

    step = lax.broadcasted_iota(jnp.int32, (BLOCK, devs), 0)
    targets = jnp.zeros((BLOCK, devs), jnp.int32)
    for t in range(steps):
        target = jnp.where(routes_ref[t] == 0, dst_ref[0:1, :], dst_ref[1:2, :])
        target = jnp.where(counts_ref[t] > 0, target, NO_BLOCK)
        targets = jnp.where(step == t, target, targets)
        device = lax.broadcasted_iota(jnp.int32, (1, devs), 1)
        chosen_ref[t, 0:1, :] = device * tpt + routes_ref[t]
        chosen_ref[t, 1:2, :] = jnp.where(routes_ref[t] == 0, from_ref[0:1, :], from_ref[1:2, :])
    targets = targets.astype(jnp.float32).astype(jnp.bfloat16)
    rows = lax.broadcasted_iota(jnp.int32, (devs * EXTRA, devs), 0) // EXTRA
    cols = lax.broadcasted_iota(jnp.int32, (devs * EXTRA, devs), 1)
    extra = lax.dot_general(
        one_hot(rows, cols), targets, (((1,), (1,)), ((), ())), preferred_element_type=jnp.float32
    )
    extra = extra.astype(jnp.bfloat16)
    long = TRIALS + EXTRA
    for d in range(devs):
        out_ref[d * long + TRIALS : (d + 1) * long, :] = extra[d * EXTRA : (d + 1) * EXTRA, :]

    copies[2].wait()
    for b in range(blocks_ref.shape[0]):
        spikes = spike_of(volts_ref[:, lanes(b)])
        spikes_ref[:, lanes(b)] = spikes
        rows_ref[b * TRIALS : (b + 1) * TRIALS, :] = spikes
        blocks_ref[b] = spikes.astype(jnp.bfloat16)
    copies[7].wait()
    act_ref[...] = activity_of(population_rows(pops_ref[...]), rows_ref[...])
    copies[1].wait()

    def store(d, current):
        out_ref[d * long : d * long + TRIALS, :] = current

    def pick_whole(d):
        k = route_s[0, 0, d]
        return src_s[k, d], d * tpt + k

    def pick_routed(d):
        return src_s[route_s[0, 0, d], d], base + d

    for c in range(WHOLE // CHUNK):
        whole(c).wait()
        send_tiles(c * CHUNK, (c + 1) * CHUNK, pick_whole, blocks_ref, tiles_ref, store)
    for c in range((devs - WHOLE) // CHUNK):
        at = WHOLE + c * CHUNK
        pltpu.make_async_copy(
            table_hbm.at[pl.ds(0, CHUNK)], tiles_ref.at[pl.ds(base + at, CHUNK)], routed_sems.at[c]
        ).wait()
        send_tiles(at, at + CHUNK, pick_routed, blocks_ref, tiles_ref, store)


def gate_kernel(message_ref, out_ref):
    pass


def iotas(shape):
    return lax.broadcasted_iota(jnp.int32, shape, 0), lax.broadcasted_iota(jnp.int32, shape, 1)


def codes_of(message, devs):
    long = TRIALS + EXTRA
    read = lax.dot_general(
        one_hot(*iotas((8, BLOCK))), message, (((1,), (1,)), ((), ())), preferred_element_type=jnp.float32
    )
    place = lax.broadcasted_iota(jnp.int32, read.shape, 1) % long
    blocks = jnp.where(place >= TRIALS, read, 0.0)
    near = blocks
    width = near.shape[1]
    near = pltpu.roll(near, width - 2, 1)
    near = near + pltpu.roll(near, width - 2, 1)
    near = near + pltpu.roll(near, width - 4, 1)
    here = jnp.where(place < TRIALS, near.astype(jnp.int32) * TRIALS + place, -1)
    row, col = iotas((devs * long, devs))
    one = jnp.dot(
        jnp.where(place == TRIALS, blocks, 0.0).astype(jnp.bfloat16),
        one_hot(row // long, col),
        preferred_element_type=jnp.float32,
    ).astype(jnp.bfloat16)
    row, col = iotas((devs, devs * TRIALS))
    later = jnp.dot(one, one_hot(row, col // TRIALS), preferred_element_type=jnp.float32)
    trial = lax.broadcasted_iota(jnp.int32, later.shape, 1) % TRIALS
    return here, later.astype(jnp.int32) * TRIALS + trial


def inflow_of(code, arrived, rows):
    row = lax.broadcasted_iota(jnp.int32, (rows, code.shape[1]), 0)
    return jnp.dot(one_hot(row, code), arrived, preferred_element_type=jnp.float32)


def update(b, inflow, volts_ref, cur_ref, ext_ref, spikes_ref, dsyn_ref, dmem_ref):
    at = lanes(b)
    dsyn = dsyn_ref[b : b + 1, :]
    dmem = dmem_ref[b : b + 1, :]
    cur = dsyn * cur_ref[:, at] + inflow[b * TRIALS : (b + 1) * TRIALS, :]
    volts = (
        dmem * volts_ref[:, at]
        + (1.0 - dmem) * (cur + ext_ref[:, at])
        - reset_size * spikes_ref[:, at]
    )
    return volts, cur


def step_kernel(step, last, *refs):
    (chosen_ref, arrived_ref, codes_ref, volts_ref, cur_ref, ext_ref,
     spikes_ref, dsyn_ref, dmem_ref, pops_ref, table_ref) = refs[:11]
    volts_out, cur_out, spikes_out, out_ref, act_ref = refs[11:16]
    chosen_s, blocks_ref, rows_ref, sems = refs[-5:-1]
    sent_ref = refs[-1]
    devs = out_ref.shape[0]
    count = blocks_ref.shape[0]
    to_smem = pltpu.make_async_copy(chosen_ref.at[step], chosen_s, sems.at[0])
    to_smem.start()
    if step == 1:
        arrived = arrived_ref[...]
        codes, later = codes_of(arrived, devs)
        refs[16][...] = later
    else:
        codes = codes_ref[...]
        arrived = arrived_ref[...].reshape(devs * TRIALS, BLOCK)
    inflow = inflow_of(codes[step - 1 : step, :], arrived, count * TRIALS)
    for b in range(count):
        volts, cur = update(
            b, inflow, volts_ref, cur_ref, ext_ref, spikes_ref, dsyn_ref, dmem_ref
        )
        volts_out[:, lanes(b)] = volts
        cur_out[:, lanes(b)] = cur
        spikes = spike_of(volts)
        spikes_out[:, lanes(b)] = spikes
        rows_ref[b * TRIALS : (b + 1) * TRIALS, :] = spikes
        blocks_ref[b] = spikes.astype(jnp.bfloat16)
    act_ref[...] = activity_of(population_rows(pops_ref[...]), rows_ref[...])
    to_smem.wait()

    def pick(d):
        return chosen_s[1, d], chosen_s[0, d]

    if not last:

        def store(d, current):
            out_ref[d] = current

        send_tiles(0, devs, pick, blocks_ref, table_ref, store)
        return

    def store_sent(d, current):
        sent_ref[d] = current

    size = devs // PIECES
    pieces = []
    for c in range(PIECES):
        send_tiles(c * size, (c + 1) * size, pick, blocks_ref, table_ref, store_sent)
        at = pl.ds(c * size, size)
        pieces.append(pltpu.make_async_copy(sent_ref.at[at], out_ref.at[at], sems.at[1 + c]))
        pieces[-1].start()
    for piece in pieces:
        piece.wait()


def last_kernel(step, arrived_ref, codes_ref, volts_ref, cur_ref, ext_ref, spikes_ref,
                dsyn_ref, dmem_ref, volts_out, cur_out):
    devs = arrived_ref.shape[0]
    count = dsyn_ref.shape[0]
    arrived = arrived_ref[...].reshape(devs * TRIALS, BLOCK)
    inflow = inflow_of(codes_ref[step - 1 : step, :], arrived, count * TRIALS)
    for b in range(count):
        volts, cur = update(
            b, inflow, volts_ref, cur_ref, ext_ref, spikes_ref, dsyn_ref, dmem_ref
        )
        volts_out[:, lanes(b)] = volts
        cur_out[:, lanes(b)] = cur


def shards(
    potential,
    current,
    ext_drive,
    decay_syn,
    decay_mem,
    weights,
    tile_src,
    tile_dst,
    blk_pop,
    tile_route,
    counts,
):
    devs, tpt = weights.shape[1:3]
    count = blk_pop.shape[0]
    steps = tile_route.shape[0]
    f32, bf16, i32 = jnp.float32, jnp.bfloat16, jnp.int32
    table = weights.reshape(devs * tpt, BLOCK, BLOCK)
    src = tile_src[0].T
    dst = tile_dst[0].T
    route = tile_route.reshape(steps, 1, devs)
    used = counts.reshape(steps, 1, devs)
    dsyn = decay_syn.reshape(count, BLOCK)
    dmem = decay_mem.reshape(count, BLOCK)
    pops = blk_pop.reshape(1, count)
    state = jax.ShapeDtypeStruct((TRIALS, count * BLOCK), f32)
    sent = jax.ShapeDtypeStruct((devs, TRIALS, BLOCK), bf16)
    act = jax.ShapeDtypeStruct((POPS * TRIALS, BLOCK), f32)
    scratch = [
        pltpu.SMEM((1, 1, devs), i32),
        pltpu.SMEM((tpt, devs), i32),
    ]
    blocks = [
        pltpu.VMEM((count, TRIALS, BLOCK), bf16),
        pltpu.VMEM((count * TRIALS, BLOCK), f32),
    ]

    def exchange(out):
        return lax.all_to_all(out, ("area", "local"), 0, 0, tiled=True)

    def in_hbm(array):
        return pltpu.with_memory_space_constraint(array, pltpu.HBM)

    long = TRIALS + EXTRA
    out, spikes, activity, chosen = pl.pallas_call(
        first_kernel,
        out_shape=(
            jax.ShapeDtypeStruct((devs * long, BLOCK), bf16),
            state,
            act,
            jax.ShapeDtypeStruct((steps, 2, devs), i32),
        ),
        in_specs=[HBM] * 7,
        out_specs=(VMEM,) * 4,
        scratch_shapes=scratch
        + [
            pltpu.VMEM((steps, 1, devs), i32),
            pltpu.VMEM((tpt, devs), i32),
            pltpu.VMEM((tpt, devs), i32),
            pltpu.VMEM((steps, 1, devs), i32),
            pltpu.VMEM(state.shape, f32),
            pltpu.VMEM((1, count), i32),
            pltpu.VMEM((devs + WHOLE * (tpt - 1), BLOCK, BLOCK), bf16),
        ]
        + blocks
        + [
            pltpu.SemaphoreType.DMA((8,)),
            pltpu.SemaphoreType.DMA((WHOLE // CHUNK,)),
            pltpu.SemaphoreType.DMA(((devs - WHOLE) // CHUNK,)),
        ],
        compiler_params=params(16),
        name="first",
    )(*[in_hbm(a) for a in (route, src, dst, used, potential, pops, table)])
    for i in range(2):
        out = pl.pallas_call(
            gate_kernel,
            out_shape=jax.ShapeDtypeStruct(out.shape, out.dtype),
            in_specs=[ANY],
            out_specs=ANY,
            input_output_aliases={0: 0},
            cost_estimate=pl.CostEstimate(flops=6_000_000_000, bytes_accessed=0, transcendentals=0),
            compiler_params=params(1),
            name=f"gate{i}",
        )(out)
    arrived = exchange(out.reshape(devs, long // 2, 2, BLOCK)).reshape(devs * long, BLOCK)
    local_table = table
    volts, cur = potential, current
    codes = jnp.zeros((8, devs * TRIALS), i32)
    history = [activity]
    for step in range(1, steps):
        outs = [state, state, state, sent, act]
        last = step == steps - 1
        out_specs = [VMEM] * len(outs)
        if step == 1:
            outs.append(jax.ShapeDtypeStruct((8, devs * TRIALS), i32))
            out_specs.append(VMEM)
        if last:
            out_specs[3] = HBM
        results = pl.pallas_call(
            functools.partial(step_kernel, step, last),
            out_shape=tuple(outs),
            in_specs=[VMEM] * 11,
            out_specs=tuple(out_specs),
            scratch_shapes=[pltpu.SMEM((2, devs), i32)]
            + blocks
            + [
                pltpu.SemaphoreType.DMA((1 + PIECES,)),
                pltpu.VMEM(sent.shape if last else (8, BLOCK), bf16),
            ],
            compiler_params=params(8),
            name=f"step{step}",
        )(chosen, arrived, codes, volts, cur, ext_drive, spikes, dsyn, dmem, pops, local_table)
        volts, cur, spikes, out, activity = results[:5]
        if step == 1:
            codes = results[5]
        history.append(activity)
        if last:
            history, out = lax.optimization_barrier((history, out))
        arrived = exchange(out)
    rates = jnp.stack(history).sum(axis=2).reshape(steps, TRIALS, POPS)
    n_local = lax.axis_size("local")
    parts = [rates] + [
        lax.ppermute(rates, "local", [(i, (i + shift) % n_local) for i in range(n_local)])
        for shift in range(1, n_local)
    ]
    total = (parts[0] + parts[2]) + (parts[1] + parts[3])
    total = total / (BLOCK * count)
    volts, cur = pl.pallas_call(
        functools.partial(last_kernel, steps),
        out_shape=(state, state),
        in_specs=[VMEM] * 8,
        out_specs=(VMEM, VMEM),
        compiler_params=params(8),
        name="last",
    )(arrived, codes, volts, cur, ext_drive, spikes, dsyn, dmem)
    return volts, cur, total[None]


def solution(mesh):
    both = ("area", "local")
    in_specs = (
        P(None, both),
        P(None, both),
        P(None, both),
        P(both),
        P(both),
        P(both, None, None, None, None),
        P(both, None, None),
        P(both, None, None),
        P(both),
        P(None, both, None, None),
        P(None, both, None),
    )
    out_specs = (P(None, both), P(None, both), P("area", None, None, None))
    return jax.shard_map(shards, mesh=mesh, in_specs=in_specs, out_specs=out_specs, check_vma=False)
```

```python
import functools

import jax
import jax.numpy as jnp
from jax import lax
from jax.experimental import pallas as pl
from jax.experimental.pallas import tpu as pltpu
from jax.sharding import PartitionSpec as P

POPS = 8
BLOCK = 128
TRIALS = 8
NO_BLOCK = 64
EXTRA = 2
PIECES = 4
CHUNK = 32
WHOLE = 32

spike_gain = 4.0
threshold = 1.0
reset_size = 0.5

VMEM = pl.BlockSpec(memory_space=pltpu.VMEM)
ANY = pl.BlockSpec(memory_space=pl.ANY)
HBM = pl.BlockSpec(memory_space=pltpu.HBM)


def params(mib, **more):
    return pltpu.CompilerParams(vmem_limit_bytes=mib << 20, **more)


def lanes(block):
    return slice(block * BLOCK, (block + 1) * BLOCK)


def spike_of(volts):
    return jax.nn.sigmoid(spike_gain * (volts - threshold))


def send_tiles(first, last, pick, blocks_ref, tiles_ref, store):
    for d in range(first, last, 2):
        (block, tile), (block_b, tile_b) = pick(d), pick(d + 1)
        spikes = jnp.concatenate([blocks_ref[block], blocks_ref[block_b]], axis=0)
        tiles = jnp.concatenate([tiles_ref[tile], tiles_ref[tile_b]], axis=1)
        current = jnp.dot(spikes, tiles, preferred_element_type=jnp.float32).astype(jnp.bfloat16)
        store(d, current[:TRIALS, :BLOCK])
        store(d + 1, current[TRIALS:, BLOCK:])


def one_hot(row, col):
    return jnp.where(row == col, 1.0, 0.0).astype(jnp.bfloat16)


def population_rows(pops):
    count = pops.shape[1]
    spread = one_hot(
        lax.broadcasted_iota(jnp.int32, (count, count * TRIALS), 0),
        lax.broadcasted_iota(jnp.int32, (count, count * TRIALS), 1) // TRIALS,
    )
    pops = jnp.broadcast_to(pops.astype(jnp.float32), (TRIALS, count)).astype(jnp.bfloat16)
    pops = jnp.dot(pops, spread, preferred_element_type=jnp.float32)[0:1, :].astype(jnp.int32)
    trial = lax.broadcasted_iota(jnp.int32, pops.shape, 1) % TRIALS
    row = lax.broadcasted_iota(jnp.int32, (TRIALS * POPS, count * TRIALS), 0)
    return one_hot(row, trial * POPS + pops)


def activity_of(member, spikes):
    high = spikes.astype(jnp.bfloat16)
    low = (spikes - high.astype(jnp.float32)).astype(jnp.bfloat16)
    return jnp.dot(member, high, preferred_element_type=jnp.float32) + jnp.dot(
        member, low, preferred_element_type=jnp.float32
    )


def first_kernel(
    route_hbm, src_hbm, dst_hbm, counts_hbm, volts_hbm, table_hbm,
    out_ref, spikes_ref, chosen_ref,
    route_s, src_s, routes_ref, from_ref, dst_ref, counts_ref, volts_ref, tiles_ref,
    blocks_ref, sems, whole_sems, routed_sems,
):
    tpt, devs = dst_ref.shape
    steps = routes_ref.shape[0]
    copies = [
        pltpu.make_async_copy(a, b, sems.at[i])
        for i, (a, b) in enumerate(
            (
                (route_hbm.at[0:1], route_s),
                (src_hbm, src_s),
                (volts_hbm, volts_ref),
                (route_hbm, routes_ref),
                (dst_hbm, dst_ref),
                (counts_hbm, counts_ref),
                (src_hbm, from_ref),
            )
        )
    ]
    for copy in copies:
        copy.start()

    def whole(c):
        at = pl.ds(c * CHUNK * tpt, CHUNK * tpt)
        return pltpu.make_async_copy(table_hbm.at[at], tiles_ref.at[at], whole_sems.at[c])

    def start_whole(c, carry):
        whole(c).start()
        return carry

    lax.fori_loop(0, WHOLE // CHUNK, start_whole, 0)
    copies[0].wait()

    base = WHOLE * tpt - WHOLE

    def start_routed(c, carry):
        for j in range(CHUNK):
            d = WHOLE + c * CHUNK + j
            pltpu.make_async_copy(
                table_hbm.at[d * tpt + route_s[0, 0, d]], tiles_ref.at[base + d], routed_sems.at[c]
            ).start()
        return carry

    lax.fori_loop(0, (devs - WHOLE) // CHUNK, start_routed, 0)
    for copy in copies[3:7]:
        copy.wait()

    step = lax.broadcasted_iota(jnp.int32, (BLOCK, devs), 0)
    targets = jnp.zeros((BLOCK, devs), jnp.int32)
    for t in range(steps):
        target = jnp.where(routes_ref[t] == 0, dst_ref[0:1, :], dst_ref[1:2, :])
        target = jnp.where(counts_ref[t] > 0, target, NO_BLOCK)
        targets = jnp.where(step == t, target, targets)
        device = lax.broadcasted_iota(jnp.int32, (1, devs), 1)
        chosen_ref[t, 0] = device * tpt + routes_ref[t]
        chosen_ref[t, 1] = jnp.where(routes_ref[t] == 0, from_ref[0:1, :], from_ref[1:2, :])
    targets = targets.astype(jnp.float32).astype(jnp.bfloat16)
    rows = lax.broadcasted_iota(jnp.int32, (devs * EXTRA, devs), 0) // EXTRA
    cols = lax.broadcasted_iota(jnp.int32, (devs * EXTRA, devs), 1)
    extra = lax.dot_general(
        one_hot(rows, cols), targets, (((1,), (1,)), ((), ())), preferred_element_type=jnp.float32
    )
    extra = extra.astype(jnp.bfloat16)
    long = TRIALS + EXTRA
    for d in range(devs):
        out_ref[d * long + TRIALS : (d + 1) * long, :] = extra[d * EXTRA : (d + 1) * EXTRA, :]

    copies[2].wait()
    for b in range(blocks_ref.shape[0]):
        spikes = spike_of(volts_ref[:, lanes(b)])
        spikes_ref[:, lanes(b)] = spikes
        blocks_ref[b] = spikes.astype(jnp.bfloat16)
    copies[1].wait()

    def store(d, current):
        out_ref[d * long : d * long + TRIALS, :] = current

    def pick_whole(d):
        k = route_s[0, 0, d]
        return src_s[k, d], d * tpt + k

    def pick_routed(d):
        return src_s[route_s[0, 0, d], d], base + d

    for c in range(WHOLE // CHUNK):
        whole(c).wait()
        send_tiles(c * CHUNK, (c + 1) * CHUNK, pick_whole, blocks_ref, tiles_ref, store)
    for c in range((devs - WHOLE) // CHUNK):
        at = WHOLE + c * CHUNK
        pltpu.make_async_copy(
            table_hbm.at[pl.ds(0, CHUNK)], tiles_ref.at[pl.ds(base + at, CHUNK)], routed_sems.at[c]
        ).wait()
        send_tiles(at, at + CHUNK, pick_routed, blocks_ref, tiles_ref, store)


def gate_kernel(message_ref, out_ref):
    pass


def iotas(shape):
    return lax.broadcasted_iota(jnp.int32, shape, 0), lax.broadcasted_iota(jnp.int32, shape, 1)


def codes_of(message, devs):
    long = TRIALS + EXTRA
    read = lax.dot_general(
        one_hot(*iotas((8, BLOCK))), message, (((1,), (1,)), ((), ())), preferred_element_type=jnp.float32
    )
    place = lax.broadcasted_iota(jnp.int32, read.shape, 1) % long
    blocks = jnp.where(place >= TRIALS, read, 0.0)
    near = blocks
    width = near.shape[1]
    near = pltpu.roll(near, width - 2, 1)
    near = near + pltpu.roll(near, width - 2, 1)
    near = near + pltpu.roll(near, width - 4, 1)
    here = jnp.where(place < TRIALS, near.astype(jnp.int32) * TRIALS + place, -1)
    row, col = iotas((devs * long, devs))
    one = jnp.dot(
        jnp.where(place == TRIALS, blocks, 0.0).astype(jnp.bfloat16),
        one_hot(row // long, col),
        preferred_element_type=jnp.float32,
    ).astype(jnp.bfloat16)
    row, col = iotas((devs, devs * TRIALS))
    later = jnp.dot(one, one_hot(row, col // TRIALS), preferred_element_type=jnp.float32)
    trial = lax.broadcasted_iota(jnp.int32, later.shape, 1) % TRIALS
    return here, later.astype(jnp.int32) * TRIALS + trial


def inflow_of(code, arrived, rows):
    row = lax.broadcasted_iota(jnp.int32, (rows, code.shape[1]), 0)
    return jnp.dot(one_hot(row, code), arrived, preferred_element_type=jnp.float32)


def update(b, inflow, volts_ref, cur_ref, ext_ref, spikes_ref, dsyn_ref, dmem_ref):
    at = lanes(b)
    dsyn = dsyn_ref[b : b + 1, :]
    dmem = dmem_ref[b : b + 1, :]
    cur = dsyn * cur_ref[:, at] + inflow[b * TRIALS : (b + 1) * TRIALS, :]
    volts = (
        dmem * volts_ref[:, at]
        + (1.0 - dmem) * (cur + ext_ref[:, at])
        - reset_size * spikes_ref[:, at]
    )
    return volts, cur


def step_kernel(step, last, *refs):
    (chosen_ref, arrived_ref, codes_ref, volts_ref, cur_ref, ext_ref,
     spikes_ref, dsyn_ref, dmem_ref, table_ref) = refs[:10]
    volts_out, cur_out, spikes_out, out_ref = refs[10:14]
    chosen_s, blocks_ref, sems = refs[-4:-1]
    sent_ref = refs[-1]
    devs = out_ref.shape[0]
    count = blocks_ref.shape[0]

    def to_smem(row):
        return pltpu.make_async_copy(chosen_ref.at[step, row], chosen_s.at[row], sems.at[row])

    def start(row, carry):
        to_smem(row).start()
        return carry

    lax.fori_loop(0, 2, start, 0)
    if step == 1:
        arrived = arrived_ref[...]
        codes, later = codes_of(arrived, devs)
        refs[14][...] = later
    else:
        codes = codes_ref[...]
        arrived = arrived_ref[...].reshape(devs * TRIALS, BLOCK)
    inflow = inflow_of(codes[step - 1 : step, :], arrived, count * TRIALS)
    for b in range(count):
        volts, cur = update(
            b, inflow, volts_ref, cur_ref, ext_ref, spikes_ref, dsyn_ref, dmem_ref
        )
        volts_out[:, lanes(b)] = volts
        cur_out[:, lanes(b)] = cur
        spikes = spike_of(volts)
        spikes_out[:, lanes(b)] = spikes
        blocks_ref[b] = spikes.astype(jnp.bfloat16)
    to_smem(0).wait()
    to_smem(1).wait()

    def pick(d):
        return chosen_s[1, 0, d], chosen_s[0, 0, d]

    if not last:

        def store(d, current):
            out_ref[d] = current

        send_tiles(0, devs, pick, blocks_ref, table_ref, store)
        return

    def store_sent(d, current):
        sent_ref[d] = current

    size = devs // PIECES
    pieces = []
    for c in range(PIECES):
        send_tiles(c * size, (c + 1) * size, pick, blocks_ref, table_ref, store_sent)
        at = pl.ds(c * size, size)
        pieces.append(pltpu.make_async_copy(sent_ref.at[at], out_ref.at[at], sems.at[2 + c]))
        pieces[-1].start()
    for piece in pieces:
        piece.wait()


def activity_kernel(pops_ref, *refs):
    spikes_refs, act_ref, rows_ref = refs[:-2], refs[-2], refs[-1]
    member = population_rows(pops_ref[...])
    for t, spikes_ref in enumerate(spikes_refs):
        for b in range(spikes_ref.shape[1] // BLOCK):
            rows_ref[t, b * TRIALS : (b + 1) * TRIALS, :] = spikes_ref[:, lanes(b)]
        act_ref[t] = activity_of(member, rows_ref[t])


def last_kernel(step, arrived_ref, codes_ref, volts_ref, cur_ref, ext_ref, spikes_ref,
                dsyn_ref, dmem_ref, volts_out, cur_out):
    devs = arrived_ref.shape[0]
    count = dsyn_ref.shape[0]
    arrived = arrived_ref[...].reshape(devs * TRIALS, BLOCK)
    inflow = inflow_of(codes_ref[step - 1 : step, :], arrived, count * TRIALS)
    for b in range(count):
        volts, cur = update(
            b, inflow, volts_ref, cur_ref, ext_ref, spikes_ref, dsyn_ref, dmem_ref
        )
        volts_out[:, lanes(b)] = volts
        cur_out[:, lanes(b)] = cur


def shards(
    potential,
    current,
    ext_drive,
    decay_syn,
    decay_mem,
    weights,
    tile_src,
    tile_dst,
    blk_pop,
    tile_route,
    counts,
):
    devs, tpt = weights.shape[1:3]
    count = blk_pop.shape[0]
    steps = tile_route.shape[0]
    f32, bf16, i32 = jnp.float32, jnp.bfloat16, jnp.int32
    table = weights.reshape(devs * tpt, BLOCK, BLOCK)
    src = tile_src[0].T
    dst = tile_dst[0].T
    route = tile_route.reshape(steps, 1, devs)
    used = counts.reshape(steps, 1, devs)
    dsyn = decay_syn.reshape(count, BLOCK)
    dmem = decay_mem.reshape(count, BLOCK)
    pops = blk_pop.reshape(1, count)
    state = jax.ShapeDtypeStruct((TRIALS, count * BLOCK), f32)
    sent = jax.ShapeDtypeStruct((devs, TRIALS, BLOCK), bf16)
    scratch = [
        pltpu.SMEM((1, 1, devs), i32),
        pltpu.SMEM((tpt, devs), i32),
    ]
    blocks = [pltpu.VMEM((count, TRIALS, BLOCK), bf16)]

    def exchange(out):
        return lax.all_to_all(out, ("area", "local"), 0, 0, tiled=True)

    def in_hbm(array):
        return pltpu.with_memory_space_constraint(array, pltpu.HBM)

    long = TRIALS + EXTRA
    out, spikes, chosen = pl.pallas_call(
        first_kernel,
        out_shape=(
            jax.ShapeDtypeStruct((devs * long, BLOCK), bf16),
            state,
            jax.ShapeDtypeStruct((steps, 2, 1, devs), i32),
        ),
        in_specs=[HBM] * 6,
        out_specs=(VMEM,) * 3,
        scratch_shapes=scratch
        + [
            pltpu.VMEM((steps, 1, devs), i32),
            pltpu.VMEM((tpt, devs), i32),
            pltpu.VMEM((tpt, devs), i32),
            pltpu.VMEM((steps, 1, devs), i32),
            pltpu.VMEM(state.shape, f32),
            pltpu.VMEM((devs + WHOLE * (tpt - 1), BLOCK, BLOCK), bf16),
        ]
        + blocks
        + [
            pltpu.SemaphoreType.DMA((7,)),
            pltpu.SemaphoreType.DMA((WHOLE // CHUNK,)),
            pltpu.SemaphoreType.DMA(((devs - WHOLE) // CHUNK,)),
        ],
        compiler_params=params(16),
        name="first",
    )(*[in_hbm(a) for a in (route, src, dst, used, potential, table)])
    for i in range(2):
        out = pl.pallas_call(
            gate_kernel,
            out_shape=jax.ShapeDtypeStruct(out.shape, out.dtype),
            in_specs=[ANY],
            out_specs=ANY,
            input_output_aliases={0: 0},
            cost_estimate=pl.CostEstimate(flops=6_000_000_000, bytes_accessed=0, transcendentals=0),
            compiler_params=params(1),
            name=f"gate{i}",
        )(out)
    arrived = exchange(out.reshape(devs, long // 2, 2, BLOCK)).reshape(devs * long, BLOCK)
    local_table = table
    volts, cur = potential, current
    codes = jnp.zeros((8, devs * TRIALS), i32)
    history = [spikes]
    for step in range(1, steps):
        outs = [state, state, state, sent]
        last = step == steps - 1
        out_specs = [VMEM] * len(outs)
        if step == 1:
            outs.append(jax.ShapeDtypeStruct((8, devs * TRIALS), i32))
            out_specs.append(VMEM)
        if last:
            out_specs[3] = HBM
        results = pl.pallas_call(
            functools.partial(step_kernel, step, last),
            out_shape=tuple(outs),
            in_specs=[VMEM] * 10,
            out_specs=tuple(out_specs),
            scratch_shapes=[pltpu.SMEM((2, 1, devs), i32)]
            + blocks
            + [
                pltpu.SemaphoreType.DMA((2 + PIECES,)),
                pltpu.VMEM(sent.shape if last else (8, BLOCK), bf16),
            ],
            compiler_params=params(8),
            name=f"step{step}",
        )(chosen, arrived, codes, volts, cur, ext_drive, spikes, dsyn, dmem, local_table)
        volts, cur, spikes, out = results[:4]
        if step == 1:
            codes = results[4]
        history.append(spikes)
        if last:
            history, out = lax.optimization_barrier((history, out))
        arrived = exchange(out)
    activity = pl.pallas_call(
        activity_kernel,
        out_shape=jax.ShapeDtypeStruct((steps, TRIALS * POPS, BLOCK), f32),
        in_specs=[VMEM] * (1 + steps),
        out_specs=VMEM,
        scratch_shapes=[pltpu.VMEM((steps, count * TRIALS, BLOCK), f32)],
        compiler_params=params(8),
        name="activity",
    )(pops, *history)
    rates = activity.sum(axis=2).reshape(steps, TRIALS, POPS)
    n_local = lax.axis_size("local")
    parts = [rates] + [
        lax.ppermute(rates, "local", [(i, (i + shift) % n_local) for i in range(n_local)])
        for shift in range(1, n_local)
    ]
    total = (parts[0] + parts[2]) + (parts[1] + parts[3])
    total = total / (BLOCK * count)
    volts, cur = pl.pallas_call(
        functools.partial(last_kernel, steps),
        out_shape=(state, state),
        in_specs=[VMEM] * 8,
        out_specs=(VMEM, VMEM),
        compiler_params=params(8),
        name="last",
    )(arrived, codes, volts, cur, ext_drive, spikes, dsyn, dmem)
    return volts, cur, total[None]


def solution(mesh):
    both = ("area", "local")
    in_specs = (
        P(None, both),
        P(None, both),
        P(None, both),
        P(both),
        P(both),
        P(both, None, None, None, None),
        P(both, None, None),
        P(both, None, None),
        P(both),
        P(None, both, None, None),
        P(None, both, None),
    )
    out_specs = (P(None, both), P(None, both), P("area", None, None, None))
    return jax.shard_map(shards, mesh=mesh, in_specs=in_specs, out_specs=out_specs, check_vma=False)
```

```python
import functools

import jax
import jax.numpy as jnp
from jax import lax
from jax.experimental import pallas as pl
from jax.experimental.pallas import tpu as pltpu
from jax.sharding import PartitionSpec as P

POPS = 8
BLOCK = 128
TRIALS = 8
NO_BLOCK = 64
EXTRA = 2
PIECES = 4
CHUNK = 32
WHOLE = 32

spike_gain = 4.0
threshold = 1.0
reset_size = 0.5

VMEM = pl.BlockSpec(memory_space=pltpu.VMEM)
ANY = pl.BlockSpec(memory_space=pl.ANY)
HBM = pl.BlockSpec(memory_space=pltpu.HBM)


def params(mib, **more):
    return pltpu.CompilerParams(vmem_limit_bytes=mib << 20, **more)


def lanes(block):
    return slice(block * BLOCK, (block + 1) * BLOCK)


def spike_of(volts):
    return jax.nn.sigmoid(spike_gain * (volts - threshold))


def send_tiles(first, last, pick, blocks_ref, tiles_ref, store):
    for d in range(first, last, 2):
        (block, tile), (block_b, tile_b) = pick(d), pick(d + 1)
        spikes = jnp.concatenate([blocks_ref[block], blocks_ref[block_b]], axis=0)
        tiles = jnp.concatenate([tiles_ref[tile], tiles_ref[tile_b]], axis=1)
        current = jnp.dot(spikes, tiles, preferred_element_type=jnp.float32).astype(jnp.bfloat16)
        store(d, current[:TRIALS, :BLOCK])
        store(d + 1, current[TRIALS:, BLOCK:])


def one_hot(row, col):
    return jnp.where(row == col, 1.0, 0.0).astype(jnp.bfloat16)


def population_rows(pops):
    count = pops.shape[1]
    spread = one_hot(
        lax.broadcasted_iota(jnp.int32, (count, count * TRIALS), 0),
        lax.broadcasted_iota(jnp.int32, (count, count * TRIALS), 1) // TRIALS,
    )
    pops = jnp.broadcast_to(pops.astype(jnp.float32), (TRIALS, count)).astype(jnp.bfloat16)
    pops = jnp.dot(pops, spread, preferred_element_type=jnp.float32)[0:1, :].astype(jnp.int32)
    trial = lax.broadcasted_iota(jnp.int32, pops.shape, 1) % TRIALS
    row = lax.broadcasted_iota(jnp.int32, (TRIALS * POPS, count * TRIALS), 0)
    return one_hot(row, trial * POPS + pops)


def activity_of(member, spikes):
    high = spikes.astype(jnp.bfloat16)
    low = (spikes - high.astype(jnp.float32)).astype(jnp.bfloat16)
    return jnp.dot(member, high, preferred_element_type=jnp.float32) + jnp.dot(
        member, low, preferred_element_type=jnp.float32
    )


def first_kernel(
    route_hbm, src_hbm, dst_hbm, counts_hbm, volts_hbm, table_hbm,
    out_ref, spikes_ref, chosen_ref, gather_ref, spread_ref,
    route_s, src_s, routes_ref, from_ref, dst_ref, counts_ref, volts_ref, tiles_ref,
    blocks_ref, sems, whole_sems, routed_sems,
):
    tpt, devs = dst_ref.shape
    steps = routes_ref.shape[0]
    copies = [
        pltpu.make_async_copy(a, b, sems.at[i])
        for i, (a, b) in enumerate(
            (
                (route_hbm.at[0:1], route_s),
                (src_hbm, src_s),
                (volts_hbm, volts_ref),
                (route_hbm, routes_ref),
                (dst_hbm, dst_ref),
                (counts_hbm, counts_ref),
                (src_hbm, from_ref),
            )
        )
    ]
    for copy in copies:
        copy.start()

    def whole(c):
        at = pl.ds(c * CHUNK * tpt, CHUNK * tpt)
        return pltpu.make_async_copy(table_hbm.at[at], tiles_ref.at[at], whole_sems.at[c])

    def start_whole(c, carry):
        whole(c).start()
        return carry

    lax.fori_loop(0, WHOLE // CHUNK, start_whole, 0)
    copies[0].wait()

    base = WHOLE * tpt - WHOLE

    def start_routed(c, carry):
        for j in range(CHUNK):
            d = WHOLE + c * CHUNK + j
            pltpu.make_async_copy(
                table_hbm.at[d * tpt + route_s[0, 0, d]], tiles_ref.at[base + d], routed_sems.at[c]
            ).start()
        return carry

    lax.fori_loop(0, (devs - WHOLE) // CHUNK, start_routed, 0)
    for copy in copies[3:7]:
        copy.wait()

    step = lax.broadcasted_iota(jnp.int32, (BLOCK, devs), 0)
    targets = jnp.zeros((BLOCK, devs), jnp.int32)
    for t in range(steps):
        target = jnp.where(routes_ref[t] == 0, dst_ref[0:1, :], dst_ref[1:2, :])
        target = jnp.where(counts_ref[t] > 0, target, NO_BLOCK)
        targets = jnp.where(step == t, target, targets)
        device = lax.broadcasted_iota(jnp.int32, (1, devs), 1)
        chosen_ref[t, 0] = device * tpt + routes_ref[t]
        chosen_ref[t, 1] = jnp.where(routes_ref[t] == 0, from_ref[0:1, :], from_ref[1:2, :])
    targets = targets.astype(jnp.float32).astype(jnp.bfloat16)
    rows = lax.broadcasted_iota(jnp.int32, (devs * EXTRA, devs), 0) // EXTRA
    cols = lax.broadcasted_iota(jnp.int32, (devs * EXTRA, devs), 1)
    extra = lax.dot_general(
        one_hot(rows, cols), targets, (((1,), (1,)), ((), ())), preferred_element_type=jnp.float32
    )
    extra = extra.astype(jnp.bfloat16)
    long = TRIALS + EXTRA
    for d in range(devs):
        out_ref[d * long + TRIALS : (d + 1) * long, :] = extra[d * EXTRA : (d + 1) * EXTRA, :]

    row, col = iotas(gather_ref.shape)
    gather_ref[...] = one_hot(row // long, col)
    row, col = iotas(spread_ref.shape)
    spread_ref[...] = one_hot(row, col // TRIALS)

    copies[2].wait()
    for b in range(blocks_ref.shape[0]):
        spikes = spike_of(volts_ref[:, lanes(b)])
        spikes_ref[:, lanes(b)] = spikes
        blocks_ref[b] = spikes.astype(jnp.bfloat16)
    copies[1].wait()

    def store(d, current):
        out_ref[d * long : d * long + TRIALS, :] = current

    def pick_whole(d):
        k = route_s[0, 0, d]
        return src_s[k, d], d * tpt + k

    def pick_routed(d):
        return src_s[route_s[0, 0, d], d], base + d

    for c in range(WHOLE // CHUNK):
        whole(c).wait()
        send_tiles(c * CHUNK, (c + 1) * CHUNK, pick_whole, blocks_ref, tiles_ref, store)
    for c in range((devs - WHOLE) // CHUNK):
        at = WHOLE + c * CHUNK
        pltpu.make_async_copy(
            table_hbm.at[pl.ds(0, CHUNK)], tiles_ref.at[pl.ds(base + at, CHUNK)], routed_sems.at[c]
        ).wait()
        send_tiles(at, at + CHUNK, pick_routed, blocks_ref, tiles_ref, store)


def gate_kernel(message_ref, out_ref):
    pass


def iotas(shape):
    return lax.broadcasted_iota(jnp.int32, shape, 0), lax.broadcasted_iota(jnp.int32, shape, 1)


def codes_of(message, gather, spread):
    long = TRIALS + EXTRA
    read = lax.dot_general(
        one_hot(*iotas((8, BLOCK))), message, (((1,), (1,)), ((), ())), preferred_element_type=jnp.float32
    )
    place = lax.broadcasted_iota(jnp.int32, read.shape, 1) % long
    blocks = jnp.where(place >= TRIALS, read, 0.0)
    near = blocks
    width = near.shape[1]
    near = pltpu.roll(near, width - 2, 1)
    near = near + pltpu.roll(near, width - 2, 1)
    near = near + pltpu.roll(near, width - 4, 1)
    here = jnp.where(place < TRIALS, near.astype(jnp.int32) * TRIALS + place, -1)
    one = jnp.dot(
        jnp.where(place == TRIALS, blocks, 0.0).astype(jnp.bfloat16), gather, preferred_element_type=jnp.float32
    ).astype(jnp.bfloat16)
    later = jnp.dot(one, spread, preferred_element_type=jnp.float32)
    trial = lax.broadcasted_iota(jnp.int32, later.shape, 1) % TRIALS
    return here, later.astype(jnp.int32) * TRIALS + trial


def inflow_of(code, arrived, rows):
    row = lax.broadcasted_iota(jnp.int32, (rows, BLOCK), 0).astype(jnp.float32).astype(jnp.bfloat16)
    code = jnp.broadcast_to(code.astype(jnp.float32), (16, code.shape[1])).astype(jnp.bfloat16)
    one, zero = jnp.ones((), jnp.bfloat16), jnp.zeros((), jnp.bfloat16)
    deliver = jnp.concatenate(
        [
            jnp.where(row == jnp.concatenate([code[:, lanes(c)]] * (rows // 16), axis=0), one, zero)
            for c in range(code.shape[1] // BLOCK)
        ],
        axis=1,
    )
    return jnp.dot(deliver, arrived, preferred_element_type=jnp.float32)


def update(b, inflow, volts_ref, cur_ref, ext_ref, spikes_ref, dsyn_ref, dmem_ref):
    at = lanes(b)
    dsyn = dsyn_ref[b : b + 1, :]
    dmem = dmem_ref[b : b + 1, :]
    cur = dsyn * cur_ref[:, at] + inflow[b * TRIALS : (b + 1) * TRIALS, :]
    volts = (
        dmem * volts_ref[:, at]
        + (1.0 - dmem) * (cur + ext_ref[:, at])
        - reset_size * spikes_ref[:, at]
    )
    return volts, cur


def step_kernel(step, last, *refs):
    (chosen_ref, arrived_ref, codes_ref, volts_ref, cur_ref, ext_ref,
     spikes_ref, dsyn_ref, dmem_ref, table_ref) = refs[:10]
    if step == 1:
        gather_ref, spread_ref = refs[10:12]
        refs = refs[2:]
    volts_out, cur_out, spikes_out, out_ref = refs[10:14]
    chosen_s, blocks_ref, sems = refs[-4:-1]
    sent_ref = refs[-1]
    devs = out_ref.shape[0]
    count = blocks_ref.shape[0]

    def to_smem(row):
        return pltpu.make_async_copy(chosen_ref.at[step, row], chosen_s.at[row], sems.at[row])

    def start(row, carry):
        to_smem(row).start()
        return carry

    lax.fori_loop(0, 2, start, 0)
    if step == 1:
        arrived = arrived_ref[...]
        codes, later = codes_of(arrived, gather_ref[...], spread_ref[...])
        refs[14][...] = later
    else:
        codes = codes_ref[...]
        arrived = arrived_ref[...].reshape(devs * TRIALS, BLOCK)
    inflow = inflow_of(codes[step - 1 : step, :], arrived, count * TRIALS)
    for b in range(count):
        volts, cur = update(
            b, inflow, volts_ref, cur_ref, ext_ref, spikes_ref, dsyn_ref, dmem_ref
        )
        volts_out[:, lanes(b)] = volts
        cur_out[:, lanes(b)] = cur
        spikes = spike_of(volts)
        spikes_out[:, lanes(b)] = spikes
        blocks_ref[b] = spikes.astype(jnp.bfloat16)
    to_smem(0).wait()
    to_smem(1).wait()

    def pick(d):
        return chosen_s[1, 0, d], chosen_s[0, 0, d]

    if not last:

        def store(d, current):
            out_ref[d] = current

        send_tiles(0, devs, pick, blocks_ref, table_ref, store)
        return

    def store_sent(d, current):
        sent_ref[d] = current

    size = devs // PIECES
    pieces = []
    for c in range(PIECES):
        send_tiles(c * size, (c + 1) * size, pick, blocks_ref, table_ref, store_sent)
        at = pl.ds(c * size, size)
        pieces.append(pltpu.make_async_copy(sent_ref.at[at], out_ref.at[at], sems.at[2 + c]))
        pieces[-1].start()
    for piece in pieces:
        piece.wait()


def activity_kernel(pops_ref, *refs):
    spikes_refs, act_ref, rows_ref = refs[:-2], refs[-2], refs[-1]
    member = population_rows(pops_ref[...])
    for t, spikes_ref in enumerate(spikes_refs):
        for b in range(spikes_ref.shape[1] // BLOCK):
            rows_ref[t, b * TRIALS : (b + 1) * TRIALS, :] = spikes_ref[:, lanes(b)]
        act_ref[t] = activity_of(member, rows_ref[t])


def last_kernel(step, arrived_ref, codes_ref, volts_ref, cur_ref, ext_ref, spikes_ref,
                dsyn_ref, dmem_ref, volts_out, cur_out):
    devs = arrived_ref.shape[0]
    count = dsyn_ref.shape[0]
    arrived = arrived_ref[...].reshape(devs * TRIALS, BLOCK)
    inflow = inflow_of(codes_ref[step - 1 : step, :], arrived, count * TRIALS)
    for b in range(count):
        volts, cur = update(
            b, inflow, volts_ref, cur_ref, ext_ref, spikes_ref, dsyn_ref, dmem_ref
        )
        volts_out[:, lanes(b)] = volts
        cur_out[:, lanes(b)] = cur


def shards(
    potential,
    current,
    ext_drive,
    decay_syn,
    decay_mem,
    weights,
    tile_src,
    tile_dst,
    blk_pop,
    tile_route,
    counts,
):
    devs, tpt = weights.shape[1:3]
    count = blk_pop.shape[0]
    steps = tile_route.shape[0]
    f32, bf16, i32 = jnp.float32, jnp.bfloat16, jnp.int32
    table = weights.reshape(devs * tpt, BLOCK, BLOCK)
    src = tile_src[0].T
    dst = tile_dst[0].T
    route = tile_route.reshape(steps, 1, devs)
    used = counts.reshape(steps, 1, devs)
    dsyn = decay_syn.reshape(count, BLOCK)
    dmem = decay_mem.reshape(count, BLOCK)
    pops = blk_pop.reshape(1, count)
    state = jax.ShapeDtypeStruct((TRIALS, count * BLOCK), f32)
    sent = jax.ShapeDtypeStruct((devs, TRIALS, BLOCK), bf16)
    scratch = [
        pltpu.SMEM((1, 1, devs), i32),
        pltpu.SMEM((tpt, devs), i32),
    ]
    blocks = [pltpu.VMEM((count, TRIALS, BLOCK), bf16)]

    def exchange(out):
        return lax.all_to_all(out, ("area", "local"), 0, 0, tiled=True)

    def in_hbm(array):
        return pltpu.with_memory_space_constraint(array, pltpu.HBM)

    long = TRIALS + EXTRA
    out, spikes, chosen, *constants = pl.pallas_call(
        first_kernel,
        out_shape=(
            jax.ShapeDtypeStruct((devs * long, BLOCK), bf16),
            state,
            jax.ShapeDtypeStruct((steps, 2, 1, devs), i32),
            jax.ShapeDtypeStruct((devs * long, devs), bf16),
            jax.ShapeDtypeStruct((devs, devs * TRIALS), bf16),
        ),
        in_specs=[HBM] * 6,
        out_specs=(VMEM,) * 5,
        scratch_shapes=scratch
        + [
            pltpu.VMEM((steps, 1, devs), i32),
            pltpu.VMEM((tpt, devs), i32),
            pltpu.VMEM((tpt, devs), i32),
            pltpu.VMEM((steps, 1, devs), i32),
            pltpu.VMEM(state.shape, f32),
            pltpu.VMEM((devs + WHOLE * (tpt - 1), BLOCK, BLOCK), bf16),
        ]
        + blocks
        + [
            pltpu.SemaphoreType.DMA((7,)),
            pltpu.SemaphoreType.DMA((WHOLE // CHUNK,)),
            pltpu.SemaphoreType.DMA(((devs - WHOLE) // CHUNK,)),
        ],
        compiler_params=params(16),
        name="first",
    )(*[in_hbm(a) for a in (route, src, dst, used, potential, table)])
    for i in range(2):
        out = pl.pallas_call(
            gate_kernel,
            out_shape=jax.ShapeDtypeStruct(out.shape, out.dtype),
            in_specs=[ANY],
            out_specs=ANY,
            input_output_aliases={0: 0},
            cost_estimate=pl.CostEstimate(flops=6_000_000_000, bytes_accessed=0, transcendentals=0),
            compiler_params=params(1),
            name=f"gate{i}",
        )(out)
    arrived = exchange(out.reshape(devs, long // 2, 2, BLOCK)).reshape(devs * long, BLOCK)
    local_table = table
    volts, cur = potential, current
    codes = jnp.zeros((8, devs * TRIALS), i32)
    history = [spikes]
    for step in range(1, steps):
        outs = [state, state, state, sent]
        last = step == steps - 1
        out_specs = [VMEM] * len(outs)
        if step == 1:
            outs.append(jax.ShapeDtypeStruct((8, devs * TRIALS), i32))
            out_specs.append(VMEM)
        else:
            constants = []
        if last:
            out_specs[3] = HBM
        results = pl.pallas_call(
            functools.partial(step_kernel, step, last),
            out_shape=tuple(outs),
            in_specs=[VMEM] * (10 + len(constants)),
            out_specs=tuple(out_specs),
            scratch_shapes=[pltpu.SMEM((2, 1, devs), i32)]
            + blocks
            + [
                pltpu.SemaphoreType.DMA((2 + PIECES,)),
                pltpu.VMEM(sent.shape if last else (8, BLOCK), bf16),
            ],
            compiler_params=params(8),
            name=f"step{step}",
        )(chosen, arrived, codes, volts, cur, ext_drive, spikes, dsyn, dmem, local_table, *constants)
        volts, cur, spikes, out = results[:4]
        if step == 1:
            codes = results[4]
        history.append(spikes)
        if last:
            history, out = lax.optimization_barrier((history, out))
        arrived = exchange(out)
    activity = pl.pallas_call(
        activity_kernel,
        out_shape=jax.ShapeDtypeStruct((steps, TRIALS * POPS, BLOCK), f32),
        in_specs=[VMEM] * (1 + steps),
        out_specs=VMEM,
        scratch_shapes=[pltpu.VMEM((steps, count * TRIALS, BLOCK), f32)],
        compiler_params=params(8),
        name="activity",
    )(pops, *history)
    rates = activity.sum(axis=2).reshape(steps, TRIALS, POPS)
    n_local = lax.axis_size("local")
    parts = [rates] + [
        lax.ppermute(rates, "local", [(i, (i + shift) % n_local) for i in range(n_local)])
        for shift in range(1, n_local)
    ]
    total = (parts[0] + parts[2]) + (parts[1] + parts[3])
    total = total / (BLOCK * count)
    volts, cur = pl.pallas_call(
        functools.partial(last_kernel, steps),
        out_shape=(state, state),
        in_specs=[VMEM] * 8,
        out_specs=(VMEM, VMEM),
        compiler_params=params(8),
        name="last",
    )(arrived, codes, volts, cur, ext_drive, spikes, dsyn, dmem)
    return volts, cur, total[None]


def solution(mesh):
    both = ("area", "local")
    in_specs = (
        P(None, both),
        P(None, both),
        P(None, both),
        P(both),
        P(both),
        P(both, None, None, None, None),
        P(both, None, None),
        P(both, None, None),
        P(both),
        P(None, both, None, None),
        P(None, both, None),
    )
    out_specs = (P(None, both), P(None, both), P("area", None, None, None))
    return jax.shard_map(shards, mesh=mesh, in_specs=in_specs, out_specs=out_specs, check_vma=False)
```

```python
import functools

import jax
import jax.numpy as jnp
from jax import lax
from jax.experimental import pallas as pl
from jax.experimental.pallas import tpu as pltpu
from jax.sharding import PartitionSpec as P

POPS = 8
BLOCK = 128
TRIALS = 8
NO_BLOCK = 64
EXTRA = 2
EARLY = 32
HALVES = 2
PIECES = 4
CHUNK = 32
WHOLE = 32

spike_gain = 4.0
threshold = 1.0
reset_size = 0.5

VMEM = pl.BlockSpec(memory_space=pltpu.VMEM)
ANY = pl.BlockSpec(memory_space=pl.ANY)
HBM = pl.BlockSpec(memory_space=pltpu.HBM)


def params(mib, **more):
    return pltpu.CompilerParams(vmem_limit_bytes=mib << 20, **more)


def lanes(block):
    return slice(block * BLOCK, (block + 1) * BLOCK)


def spike_of(volts):
    return jax.nn.sigmoid(spike_gain * (volts - threshold))


def send_tiles(first, last, pick, blocks_ref, tiles_ref, store):
    for d in range(first, last, 2):
        (block, tile), (block_b, tile_b) = pick(d), pick(d + 1)
        spikes = jnp.concatenate([blocks_ref[block], blocks_ref[block_b]], axis=0)
        tiles = jnp.concatenate([tiles_ref[tile], tiles_ref[tile_b]], axis=1)
        current = jnp.dot(spikes, tiles, preferred_element_type=jnp.float32).astype(jnp.bfloat16)
        store(d, current[:TRIALS, :BLOCK])
        store(d + 1, current[TRIALS:, BLOCK:])


def one_hot(row, col):
    return jnp.where(row == col, 1.0, 0.0).astype(jnp.bfloat16)


def population_rows(pops):
    count = pops.shape[1]
    spread = one_hot(
        lax.broadcasted_iota(jnp.int32, (count, count * TRIALS), 0),
        lax.broadcasted_iota(jnp.int32, (count, count * TRIALS), 1) // TRIALS,
    )
    pops = jnp.broadcast_to(pops.astype(jnp.float32), (TRIALS, count)).astype(jnp.bfloat16)
    pops = jnp.dot(pops, spread, preferred_element_type=jnp.float32)[0:1, :].astype(jnp.int32)
    trial = lax.broadcasted_iota(jnp.int32, pops.shape, 1) % TRIALS
    row = lax.broadcasted_iota(jnp.int32, (TRIALS * POPS, count * TRIALS), 0)
    return one_hot(row, trial * POPS + pops)


def activity_of(member, spikes):
    high = spikes.astype(jnp.bfloat16)
    low = (spikes - high.astype(jnp.float32)).astype(jnp.bfloat16)
    return jnp.dot(member, high, preferred_element_type=jnp.float32) + jnp.dot(
        member, low, preferred_element_type=jnp.float32
    )


def first_kernel(
    route_hbm, src_hbm, dst_hbm, counts_hbm, volts_hbm, table_hbm,
    out_ref, spikes_ref, chosen_ref, gather_ref, spread_ref,
    route_s, src_s, routes_ref, from_ref, dst_ref, counts_ref, volts_ref, tiles_ref,
    blocks_ref, sems, whole_sems, routed_sems,
):
    tpt, devs = dst_ref.shape
    steps = routes_ref.shape[0]
    copies = [
        pltpu.make_async_copy(a, b, sems.at[i])
        for i, (a, b) in enumerate(
            (
                (route_hbm.at[0:1], route_s),
                (src_hbm, src_s),
                (volts_hbm, volts_ref),
                (route_hbm, routes_ref),
                (dst_hbm, dst_ref),
                (counts_hbm, counts_ref),
                (src_hbm, from_ref),
            )
        )
    ]
    for copy in copies:
        copy.start()

    def whole(c):
        at = pl.ds(c * CHUNK * tpt, CHUNK * tpt)
        return pltpu.make_async_copy(table_hbm.at[at], tiles_ref.at[at], whole_sems.at[c])

    def start_whole(c, carry):
        whole(c).start()
        return carry

    lax.fori_loop(0, WHOLE // CHUNK, start_whole, 0)
    copies[0].wait()

    base = WHOLE * tpt - WHOLE

    def start_routed(c, carry):
        for j in range(CHUNK):
            d = WHOLE + c * CHUNK + j
            pltpu.make_async_copy(
                table_hbm.at[d * tpt + route_s[0, 0, d]], tiles_ref.at[base + d], routed_sems.at[c]
            ).start()
        return carry

    lax.fori_loop(0, (devs - WHOLE) // CHUNK, start_routed, 0)
    for copy in copies[3:7]:
        copy.wait()

    step = lax.broadcasted_iota(jnp.int32, (BLOCK, devs), 0)
    targets = jnp.zeros((BLOCK, devs), jnp.int32)
    for t in range(steps):
        target = jnp.where(routes_ref[t] == 0, dst_ref[0:1, :], dst_ref[1:2, :])
        target = jnp.where(counts_ref[t] > 0, target, NO_BLOCK)
        targets = jnp.where(step == t, target, targets)
        device = lax.broadcasted_iota(jnp.int32, (1, devs), 1)
        chosen_ref[t, 0] = device * tpt + routes_ref[t]
        chosen_ref[t, 1] = jnp.where(routes_ref[t] == 0, from_ref[0:1, :], from_ref[1:2, :])
    targets = targets.astype(jnp.float32).astype(jnp.bfloat16)
    rows = lax.broadcasted_iota(jnp.int32, (devs * EXTRA, devs), 0) // EXTRA
    cols = lax.broadcasted_iota(jnp.int32, (devs * EXTRA, devs), 1)
    extra = lax.dot_general(
        one_hot(rows, cols), targets, (((1,), (1,)), ((), ())), preferred_element_type=jnp.float32
    )
    extra = extra.astype(jnp.bfloat16)
    long = TRIALS + EXTRA
    for d in range(devs):
        out_ref[d * long + TRIALS : (d + 1) * long, :] = extra[d * EXTRA : (d + 1) * EXTRA, :]

    row, col = iotas(gather_ref.shape)
    gather_ref[...] = one_hot(row // long, col)
    row, col = iotas(spread_ref.shape)
    spread_ref[...] = one_hot(row, col // TRIALS)

    copies[2].wait()
    for b in range(blocks_ref.shape[0]):
        spikes = spike_of(volts_ref[:, lanes(b)])
        spikes_ref[:, lanes(b)] = spikes
        blocks_ref[b] = spikes.astype(jnp.bfloat16)
    copies[1].wait()

    def store(d, current):
        out_ref[d * long : d * long + TRIALS, :] = current

    def pick_whole(d):
        k = route_s[0, 0, d]
        return src_s[k, d], d * tpt + k

    def pick_routed(d):
        return src_s[route_s[0, 0, d], d], base + d

    for c in range(WHOLE // CHUNK):
        whole(c).wait()
        send_tiles(c * CHUNK, (c + 1) * CHUNK, pick_whole, blocks_ref, tiles_ref, store)
    for c in range((devs - WHOLE) // CHUNK):
        at = WHOLE + c * CHUNK
        pltpu.make_async_copy(
            table_hbm.at[pl.ds(0, CHUNK)], tiles_ref.at[pl.ds(base + at, CHUNK)], routed_sems.at[c]
        ).wait()
        send_tiles(at, at + CHUNK, pick_routed, blocks_ref, tiles_ref, store)


def gate_kernel(message_ref, out_ref):
    pass


def iotas(shape):
    return lax.broadcasted_iota(jnp.int32, shape, 0), lax.broadcasted_iota(jnp.int32, shape, 1)


def codes_of(message, gather, spread):
    long = TRIALS + EXTRA
    read = lax.dot_general(
        one_hot(*iotas((8, BLOCK))), message, (((1,), (1,)), ((), ())), preferred_element_type=jnp.float32
    )
    place = lax.broadcasted_iota(jnp.int32, read.shape, 1) % long
    blocks = jnp.where(place >= TRIALS, read, 0.0)
    near = blocks
    width = near.shape[1]
    near = pltpu.roll(near, width - 2, 1)
    near = near + pltpu.roll(near, width - 2, 1)
    near = near + pltpu.roll(near, width - 4, 1)
    here = jnp.where(place < TRIALS, near.astype(jnp.int32) * TRIALS + place, -1)
    one = jnp.dot(
        jnp.where(place == TRIALS, blocks, 0.0).astype(jnp.bfloat16), gather, preferred_element_type=jnp.float32
    ).astype(jnp.bfloat16)
    later = jnp.dot(one, spread, preferred_element_type=jnp.float32)
    trial = lax.broadcasted_iota(jnp.int32, later.shape, 1) % TRIALS
    return here, later.astype(jnp.int32) * TRIALS + trial


def inflow_of(code, arrived, rows):
    row = lax.broadcasted_iota(jnp.int32, (rows, BLOCK), 0).astype(jnp.float32).astype(jnp.bfloat16)
    code = jnp.broadcast_to(code.astype(jnp.float32), (16, code.shape[1])).astype(jnp.bfloat16)
    one, zero = jnp.ones((), jnp.bfloat16), jnp.zeros((), jnp.bfloat16)
    deliver = jnp.concatenate(
        [
            jnp.where(row == jnp.concatenate([code[:, lanes(c)]] * (rows // 16), axis=0), one, zero)
            for c in range(code.shape[1] // BLOCK)
        ],
        axis=1,
    )
    return jnp.dot(deliver, arrived, preferred_element_type=jnp.float32)


def update(b, inflow, volts_ref, cur_ref, ext_ref, spikes_ref, dsyn_ref, dmem_ref):
    at = lanes(b)
    dsyn = dsyn_ref[b : b + 1, :]
    dmem = dmem_ref[b : b + 1, :]
    cur = dsyn * cur_ref[:, at] + inflow[b * TRIALS : (b + 1) * TRIALS, :]
    volts = (
        dmem * volts_ref[:, at]
        + (1.0 - dmem) * (cur + ext_ref[:, at])
        - reset_size * spikes_ref[:, at]
    )
    return volts, cur


def step_kernel(step, last, *refs):
    (chosen_ref, arrived_ref, codes_ref, volts_ref, cur_ref, ext_ref,
     spikes_ref, dsyn_ref, dmem_ref, table_ref) = refs[:10]
    if step == 1:
        gather_ref, spread_ref = refs[10:12]
        refs = refs[2:]
    volts_out, cur_out, spikes_out, out_ref = refs[10:14]
    chosen_s, blocks_ref, sems = refs[-4:-1]
    sent_ref = refs[-1]
    devs = out_ref.shape[0]
    count = blocks_ref.shape[0]

    def to_smem(row):
        return pltpu.make_async_copy(chosen_ref.at[step, row], chosen_s.at[row], sems.at[row])

    def start(row, carry):
        to_smem(row).start()
        return carry

    lax.fori_loop(0, 2, start, 0)
    if step == 1:
        arrived = arrived_ref[...]
        codes, later = codes_of(arrived, gather_ref[...], spread_ref[...])
        refs[14][...] = later
    else:
        codes = codes_ref[...]
        arrived = arrived_ref[...].reshape(devs * TRIALS, BLOCK)
    inflow = inflow_of(codes[step - 1 : step, :], arrived, count * TRIALS)
    for b in range(count):
        volts, cur = update(
            b, inflow, volts_ref, cur_ref, ext_ref, spikes_ref, dsyn_ref, dmem_ref
        )
        volts_out[:, lanes(b)] = volts
        cur_out[:, lanes(b)] = cur
        spikes = spike_of(volts)
        spikes_out[:, lanes(b)] = spikes
        blocks_ref[b] = spikes.astype(jnp.bfloat16)
    tile_row, block_row = chosen_ref[step, 0], chosen_ref[step, 1]

    def pick(d):
        if d < EARLY:
            return block_row[0, d], tile_row[0, d]
        if d == EARLY:
            to_smem(0).wait()
            to_smem(1).wait()
        return chosen_s[1, 0, d], chosen_s[0, 0, d]

    if not last:

        def store(d, current):
            out_ref[d] = current

        send_tiles(0, devs, pick, blocks_ref, table_ref, store)
        return

    def store_sent(d, current):
        sent_ref[d] = current

    size = devs // PIECES
    pieces = []
    for c in range(PIECES):
        send_tiles(c * size, (c + 1) * size, pick, blocks_ref, table_ref, store_sent)
        at = pl.ds(c * size, size)
        pieces.append(pltpu.make_async_copy(sent_ref.at[at], out_ref.at[at], sems.at[2 + c]))
        pieces[-1].start()
    for piece in pieces:
        piece.wait()


def activity_kernel(pops_ref, *refs):
    spikes_refs, act_ref, rows_ref = refs[:-2], refs[-2], refs[-1]
    member = population_rows(pops_ref[...])
    for t, spikes_ref in enumerate(spikes_refs):
        for b in range(spikes_ref.shape[1] // BLOCK):
            rows_ref[t, b * TRIALS : (b + 1) * TRIALS, :] = spikes_ref[:, lanes(b)]
        act_ref[t] = activity_of(member, rows_ref[t])


def last_kernel(step, arrived_ref, codes_ref, volts_ref, cur_ref, ext_ref, spikes_ref,
                dsyn_ref, dmem_ref, volts_hbm, cur_hbm, volts_out, cur_out, sems):
    devs = arrived_ref.shape[0]
    count = dsyn_ref.shape[0]
    arrived = arrived_ref[...].reshape(devs * TRIALS, BLOCK)
    inflow = inflow_of(codes_ref[step - 1 : step, :], arrived, count * TRIALS)
    size = count // HALVES
    copies = []
    for c in range(HALVES):
        for b in range(c * size, (c + 1) * size):
            volts, cur = update(
                b, inflow, volts_ref, cur_ref, ext_ref, spikes_ref, dsyn_ref, dmem_ref
            )
            volts_out[:, lanes(b)] = volts
            cur_out[:, lanes(b)] = cur
        at = pl.ds(c * size * BLOCK, size * BLOCK)
        for i, (here, there) in enumerate(((volts_out, volts_hbm), (cur_out, cur_hbm))):
            copies.append(pltpu.make_async_copy(here.at[:, at], there.at[:, at], sems.at[2 * c + i]))
            copies[-1].start()
    for copy in copies:
        copy.wait()


def shards(
    potential,
    current,
    ext_drive,
    decay_syn,
    decay_mem,
    weights,
    tile_src,
    tile_dst,
    blk_pop,
    tile_route,
    counts,
):
    devs, tpt = weights.shape[1:3]
    count = blk_pop.shape[0]
    steps = tile_route.shape[0]
    f32, bf16, i32 = jnp.float32, jnp.bfloat16, jnp.int32
    table = weights.reshape(devs * tpt, BLOCK, BLOCK)
    src = tile_src[0].T
    dst = tile_dst[0].T
    route = tile_route.reshape(steps, 1, devs)
    used = counts.reshape(steps, 1, devs)
    dsyn = decay_syn.reshape(count, BLOCK)
    dmem = decay_mem.reshape(count, BLOCK)
    pops = blk_pop.reshape(1, count)
    state = jax.ShapeDtypeStruct((TRIALS, count * BLOCK), f32)
    sent = jax.ShapeDtypeStruct((devs, TRIALS, BLOCK), bf16)
    scratch = [
        pltpu.SMEM((1, 1, devs), i32),
        pltpu.SMEM((tpt, devs), i32),
    ]
    blocks = [pltpu.VMEM((count, TRIALS, BLOCK), bf16)]

    def exchange(out):
        return lax.all_to_all(out, ("area", "local"), 0, 0, tiled=True)

    def in_hbm(array):
        return pltpu.with_memory_space_constraint(array, pltpu.HBM)

    long = TRIALS + EXTRA
    out, spikes, chosen, *constants = pl.pallas_call(
        first_kernel,
        out_shape=(
            jax.ShapeDtypeStruct((devs * long, BLOCK), bf16),
            state,
            jax.ShapeDtypeStruct((steps, 2, 1, devs), i32),
            jax.ShapeDtypeStruct((devs * long, devs), bf16),
            jax.ShapeDtypeStruct((devs, devs * TRIALS), bf16),
        ),
        in_specs=[HBM] * 6,
        out_specs=(VMEM,) * 5,
        scratch_shapes=scratch
        + [
            pltpu.VMEM((steps, 1, devs), i32),
            pltpu.VMEM((tpt, devs), i32),
            pltpu.VMEM((tpt, devs), i32),
            pltpu.VMEM((steps, 1, devs), i32),
            pltpu.VMEM(state.shape, f32),
            pltpu.VMEM((devs + WHOLE * (tpt - 1), BLOCK, BLOCK), bf16),
        ]
        + blocks
        + [
            pltpu.SemaphoreType.DMA((7,)),
            pltpu.SemaphoreType.DMA((WHOLE // CHUNK,)),
            pltpu.SemaphoreType.DMA(((devs - WHOLE) // CHUNK,)),
        ],
        compiler_params=params(16),
        name="first",
    )(*[in_hbm(a) for a in (route, src, dst, used, potential, table)])
    for i in range(2):
        out = pl.pallas_call(
            gate_kernel,
            out_shape=jax.ShapeDtypeStruct(out.shape, out.dtype),
            in_specs=[ANY],
            out_specs=ANY,
            input_output_aliases={0: 0},
            cost_estimate=pl.CostEstimate(flops=6_000_000_000, bytes_accessed=0, transcendentals=0),
            compiler_params=params(1),
            name=f"gate{i}",
        )(out)
    arrived = exchange(out.reshape(devs, long // 2, 2, BLOCK)).reshape(devs * long, BLOCK)
    local_table = table
    volts, cur = potential, current
    codes = jnp.zeros((8, devs * TRIALS), i32)
    history = [spikes]
    for step in range(1, steps):
        outs = [state, state, state, sent]
        last = step == steps - 1
        out_specs = [VMEM] * len(outs)
        if step == 1:
            outs.append(jax.ShapeDtypeStruct((8, devs * TRIALS), i32))
            out_specs.append(VMEM)
        else:
            constants = []
        if last:
            out_specs[3] = HBM
        results = pl.pallas_call(
            functools.partial(step_kernel, step, last),
            out_shape=tuple(outs),
            in_specs=[VMEM] * (10 + len(constants)),
            out_specs=tuple(out_specs),
            scratch_shapes=[pltpu.SMEM((2, 1, devs), i32)]
            + blocks
            + [
                pltpu.SemaphoreType.DMA((2 + PIECES,)),
                pltpu.VMEM(sent.shape if last else (8, BLOCK), bf16),
            ],
            compiler_params=params(8),
            name=f"step{step}",
        )(chosen, arrived, codes, volts, cur, ext_drive, spikes, dsyn, dmem, local_table, *constants)
        volts, cur, spikes, out = results[:4]
        if step == 1:
            codes = results[4]
        history.append(spikes)
        if last:
            history, out = lax.optimization_barrier((history, out))
        arrived = exchange(out)
    activity = pl.pallas_call(
        activity_kernel,
        out_shape=jax.ShapeDtypeStruct((steps, TRIALS * POPS, BLOCK), f32),
        in_specs=[VMEM] * (1 + steps),
        out_specs=VMEM,
        scratch_shapes=[pltpu.VMEM((steps, count * TRIALS, BLOCK), f32)],
        compiler_params=params(8),
        name="activity",
    )(pops, *history)
    rates = activity.sum(axis=2).reshape(steps, TRIALS, POPS)
    n_local = lax.axis_size("local")
    parts = [rates] + [
        lax.ppermute(rates, "local", [(i, (i + shift) % n_local) for i in range(n_local)])
        for shift in range(1, n_local)
    ]
    total = (parts[0] + parts[2]) + (parts[1] + parts[3])
    total = total / (BLOCK * count)
    volts, cur = pl.pallas_call(
        functools.partial(last_kernel, steps),
        out_shape=(state, state),
        in_specs=[VMEM] * 8,
        out_specs=(HBM, HBM),
        scratch_shapes=[
            pltpu.VMEM(state.shape, f32),
            pltpu.VMEM(state.shape, f32),
            pltpu.SemaphoreType.DMA((2 * HALVES,)),
        ],
        compiler_params=params(8),
        name="last",
    )(arrived, codes, volts, cur, ext_drive, spikes, dsyn, dmem)
    return volts, cur, total[None]


def solution(mesh):
    both = ("area", "local")
    in_specs = (
        P(None, both),
        P(None, both),
        P(None, both),
        P(both),
        P(both),
        P(both, None, None, None, None),
        P(both, None, None),
        P(both, None, None),
        P(both),
        P(None, both, None, None),
        P(None, both, None),
    )
    out_specs = (P(None, both), P(None, both), P("area", None, None, None))
    return jax.shard_map(shards, mesh=mesh, in_specs=in_specs, out_specs=out_specs, check_vma=False)
```

```python
import functools

import jax
import jax.numpy as jnp
from jax import lax
from jax.experimental import pallas as pl
from jax.experimental.pallas import tpu as pltpu
from jax.sharding import PartitionSpec as P

POPS = 8
BLOCK = 128
TRIALS = 8
NO_BLOCK = 64
EXTRA = 2
EARLY = 32
HALVES = 2
PIECES = 4
PART = 16
CHUNK = 32
WHOLE = 32

spike_gain = 4.0
threshold = 1.0
reset_size = 0.5

VMEM = pl.BlockSpec(memory_space=pltpu.VMEM)
ANY = pl.BlockSpec(memory_space=pl.ANY)
HBM = pl.BlockSpec(memory_space=pltpu.HBM)


def params(mib, **more):
    return pltpu.CompilerParams(vmem_limit_bytes=mib << 20, **more)


def lanes(block):
    return slice(block * BLOCK, (block + 1) * BLOCK)


def spike_of(volts):
    return jax.nn.sigmoid(spike_gain * (volts - threshold))


def send_tiles(first, last, pick, blocks_ref, tiles_ref, store):
    for d in range(first, last, 2):
        (block, tile), (block_b, tile_b) = pick(d), pick(d + 1)
        spikes = jnp.concatenate([blocks_ref[block], blocks_ref[block_b]], axis=0)
        tiles = jnp.concatenate([tiles_ref[tile], tiles_ref[tile_b]], axis=1)
        current = jnp.dot(spikes, tiles, preferred_element_type=jnp.float32).astype(jnp.bfloat16)
        store(d, current[:TRIALS, :BLOCK])
        store(d + 1, current[TRIALS:, BLOCK:])


def one_hot(row, col):
    return jnp.where(row == col, 1.0, 0.0).astype(jnp.bfloat16)


def population_rows(pops):
    count = pops.shape[1]
    spread = one_hot(
        lax.broadcasted_iota(jnp.int32, (count, count * TRIALS), 0),
        lax.broadcasted_iota(jnp.int32, (count, count * TRIALS), 1) // TRIALS,
    )
    pops = jnp.broadcast_to(pops.astype(jnp.float32), (TRIALS, count)).astype(jnp.bfloat16)
    pops = jnp.dot(pops, spread, preferred_element_type=jnp.float32)[0:1, :].astype(jnp.int32)
    trial = lax.broadcasted_iota(jnp.int32, pops.shape, 1) % TRIALS
    row = lax.broadcasted_iota(jnp.int32, (TRIALS * POPS, count * TRIALS), 0)
    return one_hot(row, trial * POPS + pops)


def activity_of(member, spikes):
    high = spikes.astype(jnp.bfloat16)
    low = (spikes - high.astype(jnp.float32)).astype(jnp.bfloat16)
    return jnp.dot(member, high, preferred_element_type=jnp.float32) + jnp.dot(
        member, low, preferred_element_type=jnp.float32
    )


def first_kernel(
    route_hbm, src_hbm, dst_hbm, counts_hbm, volts_hbm, table_hbm,
    out_ref, spikes_ref, chosen_ref, gather_ref, spread_ref,
    route_s, src_s, routes_ref, from_ref, dst_ref, counts_ref, volts_ref, tiles_ref,
    blocks_ref, sems, whole_sems, routed_sems,
):
    tpt, devs = dst_ref.shape
    steps = routes_ref.shape[0]
    copies = [
        pltpu.make_async_copy(a, b, sems.at[i])
        for i, (a, b) in enumerate(
            (
                (route_hbm.at[0:1], route_s),
                (src_hbm, src_s),
                (volts_hbm, volts_ref),
                (route_hbm, routes_ref),
                (dst_hbm, dst_ref),
                (counts_hbm, counts_ref),
                (src_hbm, from_ref),
            )
        )
    ]
    for copy in copies:
        copy.start()

    def whole(c):
        at = pl.ds(c * CHUNK * tpt, CHUNK * tpt)
        return pltpu.make_async_copy(table_hbm.at[at], tiles_ref.at[at], whole_sems.at[c])

    def start_whole(c, carry):
        whole(c).start()
        return carry

    lax.fori_loop(0, WHOLE // CHUNK, start_whole, 0)
    copies[0].wait()

    base = WHOLE * tpt - WHOLE

    def start_routed(c, carry):
        for j in range(PART):
            d = WHOLE + c * PART + j
            pltpu.make_async_copy(
                table_hbm.at[d * tpt + route_s[0, 0, d]], tiles_ref.at[base + d], routed_sems.at[c]
            ).start()
        return carry

    lax.fori_loop(0, (devs - WHOLE) // PART, start_routed, 0)
    for copy in copies[3:7]:
        copy.wait()

    step = lax.broadcasted_iota(jnp.int32, (BLOCK, devs), 0)
    targets = jnp.zeros((BLOCK, devs), jnp.int32)
    for t in range(steps):
        target = jnp.where(routes_ref[t] == 0, dst_ref[0:1, :], dst_ref[1:2, :])
        target = jnp.where(counts_ref[t] > 0, target, NO_BLOCK)
        targets = jnp.where(step == t, target, targets)
        device = lax.broadcasted_iota(jnp.int32, (1, devs), 1)
        chosen_ref[t, 0] = device * tpt + routes_ref[t]
        chosen_ref[t, 1] = jnp.where(routes_ref[t] == 0, from_ref[0:1, :], from_ref[1:2, :])
    targets = targets.astype(jnp.float32).astype(jnp.bfloat16)
    rows = lax.broadcasted_iota(jnp.int32, (devs * EXTRA, devs), 0) // EXTRA
    cols = lax.broadcasted_iota(jnp.int32, (devs * EXTRA, devs), 1)
    extra = lax.dot_general(
        one_hot(rows, cols), targets, (((1,), (1,)), ((), ())), preferred_element_type=jnp.float32
    )
    extra = extra.astype(jnp.bfloat16)
    long = TRIALS + EXTRA
    for d in range(devs):
        out_ref[d * long + TRIALS : (d + 1) * long, :] = extra[d * EXTRA : (d + 1) * EXTRA, :]

    row, col = iotas(gather_ref.shape)
    gather_ref[...] = one_hot(row // long, col)
    row, col = iotas(spread_ref.shape)
    spread_ref[...] = one_hot(row, col // TRIALS)

    copies[2].wait()
    for b in range(blocks_ref.shape[0]):
        spikes = spike_of(volts_ref[:, lanes(b)])
        spikes_ref[:, lanes(b)] = spikes
        blocks_ref[b] = spikes.astype(jnp.bfloat16)
    copies[1].wait()

    def store(d, current):
        out_ref[d * long : d * long + TRIALS, :] = current

    def pick_whole(d):
        k = route_s[0, 0, d]
        return src_s[k, d], d * tpt + k

    def pick_routed(d):
        return src_s[route_s[0, 0, d], d], base + d

    for c in range(WHOLE // CHUNK):
        whole(c).wait()
        send_tiles(c * CHUNK, (c + 1) * CHUNK, pick_whole, blocks_ref, tiles_ref, store)
    at = WHOLE
    while at < devs:
        size = CHUNK if at + CHUNK < devs else PART
        for c in range((at - WHOLE) // PART, (at - WHOLE + size) // PART):
            pltpu.make_async_copy(
                table_hbm.at[pl.ds(0, PART)], tiles_ref.at[pl.ds(base + WHOLE + c * PART, PART)], routed_sems.at[c]
            ).wait()
        send_tiles(at, at + size, pick_routed, blocks_ref, tiles_ref, store)
        at += size


def gate_kernel(message_ref, out_ref):
    pass


def iotas(shape):
    return lax.broadcasted_iota(jnp.int32, shape, 0), lax.broadcasted_iota(jnp.int32, shape, 1)


def codes_of(message, gather, spread):
    long = TRIALS + EXTRA
    read = lax.dot_general(
        one_hot(*iotas((8, BLOCK))), message, (((1,), (1,)), ((), ())), preferred_element_type=jnp.float32
    )
    place = lax.broadcasted_iota(jnp.int32, read.shape, 1) % long
    blocks = jnp.where(place >= TRIALS, read, 0.0)
    near = blocks
    width = near.shape[1]
    near = pltpu.roll(near, width - 2, 1)
    near = near + pltpu.roll(near, width - 2, 1)
    near = near + pltpu.roll(near, width - 4, 1)
    here = jnp.where(place < TRIALS, near.astype(jnp.int32) * TRIALS + place, -1)
    one = jnp.dot(
        jnp.where(place == TRIALS, blocks, 0.0).astype(jnp.bfloat16), gather, preferred_element_type=jnp.float32
    ).astype(jnp.bfloat16)
    later = jnp.dot(one, spread, preferred_element_type=jnp.float32)
    trial = lax.broadcasted_iota(jnp.int32, later.shape, 1) % TRIALS
    return here, later.astype(jnp.int32) * TRIALS + trial


def inflow_of(code, arrived, rows):
    row = lax.broadcasted_iota(jnp.int32, (rows, BLOCK), 0).astype(jnp.float32).astype(jnp.bfloat16)
    code = jnp.broadcast_to(code.astype(jnp.float32), (16, code.shape[1])).astype(jnp.bfloat16)
    one, zero = jnp.ones((), jnp.bfloat16), jnp.zeros((), jnp.bfloat16)
    deliver = jnp.concatenate(
        [
            jnp.where(row == jnp.concatenate([code[:, lanes(c)]] * (rows // 16), axis=0), one, zero)
            for c in range(code.shape[1] // BLOCK)
        ],
        axis=1,
    )
    return jnp.dot(deliver, arrived, preferred_element_type=jnp.float32)


def update(b, inflow, volts_ref, cur_ref, ext_ref, spikes_ref, dsyn_ref, dmem_ref):
    at = lanes(b)
    dsyn = dsyn_ref[b : b + 1, :]
    dmem = dmem_ref[b : b + 1, :]
    cur = dsyn * cur_ref[:, at] + inflow[b * TRIALS : (b + 1) * TRIALS, :]
    volts = (
        dmem * volts_ref[:, at]
        + (1.0 - dmem) * (cur + ext_ref[:, at])
        - reset_size * spikes_ref[:, at]
    )
    return volts, cur


def step_kernel(step, last, *refs):
    (chosen_ref, arrived_ref, codes_ref, volts_ref, cur_ref, ext_ref,
     spikes_ref, dsyn_ref, dmem_ref, table_ref) = refs[:10]
    if step == 1:
        gather_ref, spread_ref = refs[10:12]
        refs = refs[2:]
    volts_out, cur_out, spikes_out, out_ref = refs[10:14]
    chosen_s, blocks_ref, sems = refs[-4:-1]
    sent_ref = refs[-1]
    devs = out_ref.shape[0]
    count = blocks_ref.shape[0]

    def to_smem(row):
        return pltpu.make_async_copy(chosen_ref.at[step, row], chosen_s.at[row], sems.at[row])

    def start(row, carry):
        to_smem(row).start()
        return carry

    lax.fori_loop(0, 2, start, 0)
    if step == 1:
        arrived = arrived_ref[...]
        codes, later = codes_of(arrived, gather_ref[...], spread_ref[...])
        refs[14][...] = later
    else:
        codes = codes_ref[...]
        arrived = arrived_ref[...].reshape(devs * TRIALS, BLOCK)
    inflow = inflow_of(codes[step - 1 : step, :], arrived, count * TRIALS)
    for b in range(count):
        volts, cur = update(
            b, inflow, volts_ref, cur_ref, ext_ref, spikes_ref, dsyn_ref, dmem_ref
        )
        volts_out[:, lanes(b)] = volts
        cur_out[:, lanes(b)] = cur
        spikes = spike_of(volts)
        spikes_out[:, lanes(b)] = spikes
        blocks_ref[b] = spikes.astype(jnp.bfloat16)
    tile_row, block_row = chosen_ref[step, 0], chosen_ref[step, 1]
    early = EARLY if step > 1 else 0

    def pick(d):
        if d < early:
            return block_row[0, d], tile_row[0, d]
        if d == early:
            to_smem(0).wait()
            to_smem(1).wait()
        return chosen_s[1, 0, d], chosen_s[0, 0, d]

    if not last:

        def store(d, current):
            out_ref[d] = current

        send_tiles(0, devs, pick, blocks_ref, table_ref, store)
        return

    def store_sent(d, current):
        sent_ref[d] = current

    size = devs // PIECES
    pieces = []
    for c in range(PIECES):
        send_tiles(c * size, (c + 1) * size, pick, blocks_ref, table_ref, store_sent)
        at = pl.ds(c * size, size)
        pieces.append(pltpu.make_async_copy(sent_ref.at[at], out_ref.at[at], sems.at[2 + c]))
        pieces[-1].start()
    for piece in pieces:
        piece.wait()


def activity_kernel(pops_ref, *refs):
    spikes_refs, act_ref, rows_ref = refs[:-2], refs[-2], refs[-1]
    member = population_rows(pops_ref[...])
    for t, spikes_ref in enumerate(spikes_refs):
        for b in range(spikes_ref.shape[1] // BLOCK):
            rows_ref[t, b * TRIALS : (b + 1) * TRIALS, :] = spikes_ref[:, lanes(b)]
        act_ref[t] = activity_of(member, rows_ref[t])


def last_kernel(step, arrived_ref, codes_ref, volts_ref, cur_ref, ext_ref, spikes_ref,
                dsyn_ref, dmem_ref, volts_hbm, cur_hbm, volts_out, cur_out, sems):
    devs = arrived_ref.shape[0]
    count = dsyn_ref.shape[0]
    arrived = arrived_ref[...].reshape(devs * TRIALS, BLOCK)
    inflow = inflow_of(codes_ref[step - 1 : step, :], arrived, count * TRIALS)
    size = count // HALVES
    copies = []
    for c in range(HALVES):
        for b in range(c * size, (c + 1) * size):
            volts, cur = update(
                b, inflow, volts_ref, cur_ref, ext_ref, spikes_ref, dsyn_ref, dmem_ref
            )
            volts_out[:, lanes(b)] = volts
            cur_out[:, lanes(b)] = cur
        at = pl.ds(c * size * BLOCK, size * BLOCK)
        for i, (here, there) in enumerate(((volts_out, volts_hbm), (cur_out, cur_hbm))):
            copies.append(pltpu.make_async_copy(here.at[:, at], there.at[:, at], sems.at[2 * c + i]))
            copies[-1].start()
    for copy in copies:
        copy.wait()


def shards(
    potential,
    current,
    ext_drive,
    decay_syn,
    decay_mem,
    weights,
    tile_src,
    tile_dst,
    blk_pop,
    tile_route,
    counts,
):
    devs, tpt = weights.shape[1:3]
    count = blk_pop.shape[0]
    steps = tile_route.shape[0]
    f32, bf16, i32 = jnp.float32, jnp.bfloat16, jnp.int32
    table = weights.reshape(devs * tpt, BLOCK, BLOCK)
    src = tile_src[0].T
    dst = tile_dst[0].T
    route = tile_route.reshape(steps, 1, devs)
    used = counts.reshape(steps, 1, devs)
    dsyn = decay_syn.reshape(count, BLOCK)
    dmem = decay_mem.reshape(count, BLOCK)
    pops = blk_pop.reshape(1, count)
    state = jax.ShapeDtypeStruct((TRIALS, count * BLOCK), f32)
    sent = jax.ShapeDtypeStruct((devs, TRIALS, BLOCK), bf16)
    scratch = [
        pltpu.SMEM((1, 1, devs), i32),
        pltpu.SMEM((tpt, devs), i32),
    ]
    blocks = [pltpu.VMEM((count, TRIALS, BLOCK), bf16)]

    def exchange(out):
        return lax.all_to_all(out, ("area", "local"), 0, 0, tiled=True)

    def in_hbm(array):
        return pltpu.with_memory_space_constraint(array, pltpu.HBM)

    long = TRIALS + EXTRA
    out, spikes, chosen, *constants = pl.pallas_call(
        first_kernel,
        out_shape=(
            jax.ShapeDtypeStruct((devs * long, BLOCK), bf16),
            state,
            jax.ShapeDtypeStruct((steps, 2, 1, devs), i32),
            jax.ShapeDtypeStruct((devs * long, devs), bf16),
            jax.ShapeDtypeStruct((devs, devs * TRIALS), bf16),
        ),
        in_specs=[HBM] * 6,
        out_specs=(VMEM,) * 5,
        scratch_shapes=scratch
        + [
            pltpu.VMEM((steps, 1, devs), i32),
            pltpu.VMEM((tpt, devs), i32),
            pltpu.VMEM((tpt, devs), i32),
            pltpu.VMEM((steps, 1, devs), i32),
            pltpu.VMEM(state.shape, f32),
            pltpu.VMEM((devs + WHOLE * (tpt - 1), BLOCK, BLOCK), bf16),
        ]
        + blocks
        + [
            pltpu.SemaphoreType.DMA((7,)),
            pltpu.SemaphoreType.DMA((WHOLE // CHUNK,)),
            pltpu.SemaphoreType.DMA(((devs - WHOLE) // PART,)),
        ],
        compiler_params=params(16),
        name="first",
    )(*[in_hbm(a) for a in (route, src, dst, used, potential, table)])
    for i in range(2):
        out = pl.pallas_call(
            gate_kernel,
            out_shape=jax.ShapeDtypeStruct(out.shape, out.dtype),
            in_specs=[ANY],
            out_specs=ANY,
            input_output_aliases={0: 0},
            cost_estimate=pl.CostEstimate(flops=6_000_000_000, bytes_accessed=0, transcendentals=0),
            compiler_params=params(1),
            name=f"gate{i}",
        )(out)
    arrived = exchange(out.reshape(devs, long // 2, 2, BLOCK)).reshape(devs * long, BLOCK)
    local_table = table
    volts, cur = potential, current
    codes = jnp.zeros((8, devs * TRIALS), i32)
    history = [spikes]
    for step in range(1, steps):
        outs = [state, state, state, sent]
        last = step == steps - 1
        out_specs = [VMEM] * len(outs)
        if step == 1:
            outs.append(jax.ShapeDtypeStruct((8, devs * TRIALS), i32))
            out_specs.append(VMEM)
        else:
            constants = []
        if last:
            out_specs[3] = HBM
        results = pl.pallas_call(
            functools.partial(step_kernel, step, last),
            out_shape=tuple(outs),
            in_specs=[VMEM] * (10 + len(constants)),
            out_specs=tuple(out_specs),
            scratch_shapes=[pltpu.SMEM((2, 1, devs), i32)]
            + blocks
            + [
                pltpu.SemaphoreType.DMA((2 + PIECES,)),
                pltpu.VMEM(sent.shape if last else (8, BLOCK), bf16),
            ],
            compiler_params=params(8),
            name=f"step{step}",
        )(chosen, arrived, codes, volts, cur, ext_drive, spikes, dsyn, dmem, local_table, *constants)
        volts, cur, spikes, out = results[:4]
        if step == 1:
            codes = results[4]
        history.append(spikes)
        if last:
            history, out = lax.optimization_barrier((history, out))
        arrived = exchange(out)
    activity = pl.pallas_call(
        activity_kernel,
        out_shape=jax.ShapeDtypeStruct((steps, TRIALS * POPS, BLOCK), f32),
        in_specs=[VMEM] * (1 + steps),
        out_specs=VMEM,
        scratch_shapes=[pltpu.VMEM((steps, count * TRIALS, BLOCK), f32)],
        compiler_params=params(8),
        name="activity",
    )(pops, *history)
    rates = activity.sum(axis=2).reshape(steps, TRIALS, POPS)
    n_local = lax.axis_size("local")
    parts = [rates] + [
        lax.ppermute(rates, "local", [(i, (i + shift) % n_local) for i in range(n_local)])
        for shift in range(1, n_local)
    ]
    total = (parts[0] + parts[2]) + (parts[1] + parts[3])
    total = total / (BLOCK * count)
    volts, cur = pl.pallas_call(
        functools.partial(last_kernel, steps),
        out_shape=(state, state),
        in_specs=[VMEM] * 8,
        out_specs=(HBM, HBM),
        scratch_shapes=[
            pltpu.VMEM(state.shape, f32),
            pltpu.VMEM(state.shape, f32),
            pltpu.SemaphoreType.DMA((2 * HALVES,)),
        ],
        compiler_params=params(8),
        name="last",
    )(arrived, codes, volts, cur, ext_drive, spikes, dsyn, dmem)
    return volts, cur, total[None]


def solution(mesh):
    both = ("area", "local")
    in_specs = (
        P(None, both),
        P(None, both),
        P(None, both),
        P(both),
        P(both),
        P(both, None, None, None, None),
        P(both, None, None),
        P(both, None, None),
        P(both),
        P(None, both, None, None),
        P(None, both, None),
    )
    out_specs = (P(None, both), P(None, both), P("area", None, None, None))
    return jax.shard_map(shards, mesh=mesh, in_specs=in_specs, out_specs=out_specs, check_vma=False)
```

```python
import functools

import jax
import jax.numpy as jnp
from jax import lax
from jax.experimental import pallas as pl
from jax.experimental.pallas import tpu as pltpu
from jax.sharding import PartitionSpec as P

POPS = 8
BLOCK = 128
TRIALS = 8
NO_BLOCK = 64
EXTRA = 2
EARLY = 32
HALVES = 2
PIECES = 4
CHUNK = 32
WHOLE = 32

spike_gain = 4.0
threshold = 1.0
reset_size = 0.5

VMEM = pl.BlockSpec(memory_space=pltpu.VMEM)
ANY = pl.BlockSpec(memory_space=pl.ANY)
HBM = pl.BlockSpec(memory_space=pltpu.HBM)


def params(mib, **more):
    return pltpu.CompilerParams(vmem_limit_bytes=mib << 20, **more)


def lanes(block):
    return slice(block * BLOCK, (block + 1) * BLOCK)


def spike_of(volts):
    return jax.nn.sigmoid(spike_gain * (volts - threshold))


def send_tiles(first, last, pick, blocks_ref, tiles_ref, store):
    for d in range(first, last, 2):
        (block, tile), (block_b, tile_b) = pick(d), pick(d + 1)
        spikes = jnp.concatenate([blocks_ref[block], blocks_ref[block_b]], axis=0)
        tiles = jnp.concatenate([tiles_ref[tile], tiles_ref[tile_b]], axis=1)
        current = jnp.dot(spikes, tiles, preferred_element_type=jnp.float32).astype(jnp.bfloat16)
        store(d, current[:TRIALS, :BLOCK])
        store(d + 1, current[TRIALS:, BLOCK:])


def one_hot(row, col):
    return jnp.where(row == col, 1.0, 0.0).astype(jnp.bfloat16)


def population_rows(pops):
    count = pops.shape[1]
    spread = one_hot(
        lax.broadcasted_iota(jnp.int32, (count, count * TRIALS), 0),
        lax.broadcasted_iota(jnp.int32, (count, count * TRIALS), 1) // TRIALS,
    )
    pops = jnp.broadcast_to(pops.astype(jnp.float32), (TRIALS, count)).astype(jnp.bfloat16)
    pops = jnp.dot(pops, spread, preferred_element_type=jnp.float32)[0:1, :].astype(jnp.int32)
    trial = lax.broadcasted_iota(jnp.int32, pops.shape, 1) % TRIALS
    row = lax.broadcasted_iota(jnp.int32, (TRIALS * POPS, count * TRIALS), 0)
    return one_hot(row, trial * POPS + pops)


def activity_of(member, spikes):
    high = spikes.astype(jnp.bfloat16)
    low = (spikes - high.astype(jnp.float32)).astype(jnp.bfloat16)
    return jnp.dot(member, high, preferred_element_type=jnp.float32) + jnp.dot(
        member, low, preferred_element_type=jnp.float32
    )


def first_kernel(
    route_hbm, src_hbm, dst_hbm, counts_hbm, volts_hbm, table_hbm,
    out_ref, spikes_ref, chosen_ref, gather_ref, spread_ref,
    route_s, src_s, routes_ref, from_ref, dst_ref, counts_ref, volts_ref, tiles_ref,
    blocks_ref, sems, whole_sems, routed_sems,
):
    tpt, devs = dst_ref.shape
    steps = routes_ref.shape[0]
    copies = [
        pltpu.make_async_copy(a, b, sems.at[i])
        for i, (a, b) in enumerate(
            (
                (route_hbm.at[0:1], route_s),
                (src_hbm, src_s),
                (volts_hbm, volts_ref),
                (route_hbm, routes_ref),
                (dst_hbm, dst_ref),
                (counts_hbm, counts_ref),
                (src_hbm, from_ref),
            )
        )
    ]
    for copy in copies:
        copy.start()

    def whole(c):
        at = pl.ds(c * CHUNK * tpt, CHUNK * tpt)
        return pltpu.make_async_copy(table_hbm.at[at], tiles_ref.at[at], whole_sems.at[c])

    def start_whole(c, carry):
        whole(c).start()
        return carry

    lax.fori_loop(0, WHOLE // CHUNK, start_whole, 0)
    copies[0].wait()

    base = WHOLE * tpt - WHOLE

    def start_routed(c, carry):
        for j in range(CHUNK):
            d = WHOLE + c * CHUNK + j
            pltpu.make_async_copy(
                table_hbm.at[d * tpt + route_s[0, 0, d]], tiles_ref.at[base + d], routed_sems.at[c]
            ).start()
        return carry

    lax.fori_loop(0, (devs - WHOLE) // CHUNK, start_routed, 0)
    for copy in copies[3:7]:
        copy.wait()

    step = lax.broadcasted_iota(jnp.int32, (BLOCK, devs), 0)
    targets = jnp.zeros((BLOCK, devs), jnp.int32)
    for t in range(steps):
        target = jnp.where(routes_ref[t] == 0, dst_ref[0:1, :], dst_ref[1:2, :])
        target = jnp.where(counts_ref[t] > 0, target, NO_BLOCK)
        targets = jnp.where(step == t, target, targets)
        device = lax.broadcasted_iota(jnp.int32, (1, devs), 1)
        chosen_ref[t, 0] = device * tpt + routes_ref[t]
        chosen_ref[t, 1] = jnp.where(routes_ref[t] == 0, from_ref[0:1, :], from_ref[1:2, :])
    targets = targets.astype(jnp.float32).astype(jnp.bfloat16)
    rows = lax.broadcasted_iota(jnp.int32, (devs * EXTRA, devs), 0) // EXTRA
    cols = lax.broadcasted_iota(jnp.int32, (devs * EXTRA, devs), 1)
    extra = lax.dot_general(
        one_hot(rows, cols), targets, (((1,), (1,)), ((), ())), preferred_element_type=jnp.float32
    )
    extra = extra.astype(jnp.bfloat16)
    long = TRIALS + EXTRA
    for d in range(devs):
        out_ref[d * long + TRIALS : (d + 1) * long, :] = extra[d * EXTRA : (d + 1) * EXTRA, :]

    row, col = iotas(gather_ref.shape)
    gather_ref[...] = one_hot(row // long, col)
    row, col = iotas(spread_ref.shape)
    spread_ref[...] = one_hot(row, col // TRIALS)

    copies[2].wait()
    for b in range(blocks_ref.shape[0]):
        spikes = spike_of(volts_ref[:, lanes(b)])
        spikes_ref[:, lanes(b)] = spikes
        blocks_ref[b] = spikes.astype(jnp.bfloat16)
    copies[1].wait()

    def store(d, current):
        out_ref[d * long : d * long + TRIALS, :] = current

    def pick_whole(d):
        k = route_s[0, 0, d]
        return src_s[k, d], d * tpt + k

    def pick_routed(d):
        return src_s[route_s[0, 0, d], d], base + d

    for c in range(WHOLE // CHUNK):
        whole(c).wait()
        send_tiles(c * CHUNK, (c + 1) * CHUNK, pick_whole, blocks_ref, tiles_ref, store)
    for c in range((devs - WHOLE) // CHUNK):
        at = WHOLE + c * CHUNK
        pltpu.make_async_copy(
            table_hbm.at[pl.ds(0, CHUNK)], tiles_ref.at[pl.ds(base + at, CHUNK)], routed_sems.at[c]
        ).wait()
        send_tiles(at, at + CHUNK, pick_routed, blocks_ref, tiles_ref, store)


def gate_kernel(message_ref, out_ref):
    pass


def iotas(shape):
    return lax.broadcasted_iota(jnp.int32, shape, 0), lax.broadcasted_iota(jnp.int32, shape, 1)


def codes_of(message, gather, spread):
    long = TRIALS + EXTRA
    read = lax.dot_general(
        one_hot(*iotas((8, BLOCK))), message, (((1,), (1,)), ((), ())), preferred_element_type=jnp.float32
    )
    place = lax.broadcasted_iota(jnp.int32, read.shape, 1) % long
    blocks = jnp.where(place >= TRIALS, read, 0.0)
    near = blocks
    width = near.shape[1]
    near = pltpu.roll(near, width - 2, 1)
    near = near + pltpu.roll(near, width - 2, 1)
    near = near + pltpu.roll(near, width - 4, 1)
    here = jnp.where(place < TRIALS, near.astype(jnp.int32) * TRIALS + place, -1)
    one = jnp.dot(
        jnp.where(place == TRIALS, blocks, 0.0).astype(jnp.bfloat16), gather, preferred_element_type=jnp.float32
    ).astype(jnp.bfloat16)
    later = jnp.dot(one, spread, preferred_element_type=jnp.float32)
    trial = lax.broadcasted_iota(jnp.int32, later.shape, 1) % TRIALS
    return here, later.astype(jnp.int32) * TRIALS + trial


def inflow_of(code, arrived, rows):
    row = lax.broadcasted_iota(jnp.int32, (rows, BLOCK), 0).astype(jnp.float32).astype(jnp.bfloat16)
    code = jnp.broadcast_to(code.astype(jnp.float32), (16, code.shape[1])).astype(jnp.bfloat16)
    one, zero = jnp.ones((), jnp.bfloat16), jnp.zeros((), jnp.bfloat16)
    deliver = jnp.concatenate(
        [
            jnp.where(row == jnp.concatenate([code[:, lanes(c)]] * (rows // 16), axis=0), one, zero)
            for c in range(code.shape[1] // BLOCK)
        ],
        axis=1,
    )
    return jnp.dot(deliver, arrived, preferred_element_type=jnp.float32)


def update(b, inflow, volts_ref, cur_ref, ext_ref, spikes_ref, dsyn_ref, dmem_ref):
    at = lanes(b)
    dsyn = dsyn_ref[b : b + 1, :]
    dmem = dmem_ref[b : b + 1, :]
    cur = dsyn * cur_ref[:, at] + inflow[b * TRIALS : (b + 1) * TRIALS, :]
    volts = (
        dmem * volts_ref[:, at]
        + (1.0 - dmem) * (cur + ext_ref[:, at])
        - reset_size * spikes_ref[:, at]
    )
    return volts, cur


def step_kernel(step, last, *refs):
    (chosen_ref, arrived_ref, codes_ref, volts_ref, cur_ref, ext_ref,
     spikes_ref, dsyn_ref, dmem_ref, table_ref) = refs[:10]
    if step == 1:
        gather_ref, spread_ref = refs[10:12]
        refs = refs[2:]
    volts_out, cur_out, spikes_out, out_ref = refs[10:14]
    chosen_s, blocks_ref, sems = refs[-4:-1]
    sent_ref = refs[-1]
    devs = out_ref.shape[0]
    count = blocks_ref.shape[0]

    def to_smem(row):
        return pltpu.make_async_copy(chosen_ref.at[step, row], chosen_s.at[row], sems.at[row])

    def start(row, carry):
        to_smem(row).start()
        return carry

    lax.fori_loop(0, 2, start, 0)
    if step == 1:
        arrived = arrived_ref[...]
        codes, later = codes_of(arrived, gather_ref[...], spread_ref[...])
        refs[14][...] = later
    else:
        codes = codes_ref[...]
        arrived = arrived_ref[...].reshape(devs * TRIALS, BLOCK)
    inflow = inflow_of(codes[step - 1 : step, :], arrived, count * TRIALS)
    for b in range(count):
        volts, cur = update(
            b, inflow, volts_ref, cur_ref, ext_ref, spikes_ref, dsyn_ref, dmem_ref
        )
        volts_out[:, lanes(b)] = volts
        cur_out[:, lanes(b)] = cur
        spikes = spike_of(volts)
        spikes_out[:, lanes(b)] = spikes
        blocks_ref[b] = spikes.astype(jnp.bfloat16)
    tile_row, block_row = chosen_ref[step, 0], chosen_ref[step, 1]
    early = EARLY if step > 1 else 0

    def pick(d):
        if d < early:
            return block_row[0, d], tile_row[0, d]
        if d == early:
            to_smem(0).wait()
            to_smem(1).wait()
        return chosen_s[1, 0, d], chosen_s[0, 0, d]

    if not last:

        def store(d, current):
            out_ref[d] = current

        send_tiles(0, devs, pick, blocks_ref, table_ref, store)
        return

    def store_sent(d, current):
        sent_ref[d] = current

    size = devs // PIECES
    pieces = []
    for c in range(PIECES):
        send_tiles(c * size, (c + 1) * size, pick, blocks_ref, table_ref, store_sent)
        at = pl.ds(c * size, size)
        pieces.append(pltpu.make_async_copy(sent_ref.at[at], out_ref.at[at], sems.at[2 + c]))
        pieces[-1].start()
    for piece in pieces:
        piece.wait()


def activity_kernel(pops_ref, *refs):
    spikes_refs, act_ref, rows_ref = refs[:-2], refs[-2], refs[-1]
    member = population_rows(pops_ref[...])
    for t, spikes_ref in enumerate(spikes_refs):
        for b in range(spikes_ref.shape[1] // BLOCK):
            rows_ref[t, b * TRIALS : (b + 1) * TRIALS, :] = spikes_ref[:, lanes(b)]
        act_ref[t] = activity_of(member, rows_ref[t])


def last_kernel(step, arrived_ref, codes_ref, volts_ref, cur_ref, ext_ref, spikes_ref,
                dsyn_ref, dmem_ref, volts_hbm, cur_hbm, volts_out, cur_out, sems):
    devs = arrived_ref.shape[0]
    count = dsyn_ref.shape[0]
    arrived = arrived_ref[...].reshape(devs * TRIALS, BLOCK)
    inflow = inflow_of(codes_ref[step - 1 : step, :], arrived, count * TRIALS)
    size = count // HALVES
    copies = []
    for c in range(HALVES):
        for b in range(c * size, (c + 1) * size):
            volts, cur = update(
                b, inflow, volts_ref, cur_ref, ext_ref, spikes_ref, dsyn_ref, dmem_ref
            )
            volts_out[:, lanes(b)] = volts
            cur_out[:, lanes(b)] = cur
        at = pl.ds(c * size * BLOCK, size * BLOCK)
        for i, (here, there) in enumerate(((volts_out, volts_hbm), (cur_out, cur_hbm))):
            copies.append(pltpu.make_async_copy(here.at[:, at], there.at[:, at], sems.at[2 * c + i]))
            copies[-1].start()
    for copy in copies:
        copy.wait()


def shards(
    potential,
    current,
    ext_drive,
    decay_syn,
    decay_mem,
    weights,
    tile_src,
    tile_dst,
    blk_pop,
    tile_route,
    counts,
):
    devs, tpt = weights.shape[1:3]
    count = blk_pop.shape[0]
    steps = tile_route.shape[0]
    f32, bf16, i32 = jnp.float32, jnp.bfloat16, jnp.int32
    table = weights.reshape(devs * tpt, BLOCK, BLOCK)
    src = tile_src[0].T
    dst = tile_dst[0].T
    route = tile_route.reshape(steps, 1, devs)
    used = counts.reshape(steps, 1, devs)
    dsyn = decay_syn.reshape(count, BLOCK)
    dmem = decay_mem.reshape(count, BLOCK)
    pops = blk_pop.reshape(1, count)
    state = jax.ShapeDtypeStruct((TRIALS, count * BLOCK), f32)
    sent = jax.ShapeDtypeStruct((devs, TRIALS, BLOCK), bf16)
    scratch = [
        pltpu.SMEM((1, 1, devs), i32),
        pltpu.SMEM((tpt, devs), i32),
    ]
    blocks = [pltpu.VMEM((count, TRIALS, BLOCK), bf16)]

    def exchange(out):
        return lax.all_to_all(out, ("area", "local"), 0, 0, tiled=True)

    def in_hbm(array):
        return pltpu.with_memory_space_constraint(array, pltpu.HBM)

    long = TRIALS + EXTRA
    out, spikes, chosen, *constants = pl.pallas_call(
        first_kernel,
        out_shape=(
            jax.ShapeDtypeStruct((devs * long, BLOCK), bf16),
            state,
            jax.ShapeDtypeStruct((steps, 2, 1, devs), i32),
            jax.ShapeDtypeStruct((devs * long, devs), bf16),
            jax.ShapeDtypeStruct((devs, devs * TRIALS), bf16),
        ),
        in_specs=[HBM] * 6,
        out_specs=(VMEM,) * 5,
        scratch_shapes=scratch
        + [
            pltpu.VMEM((steps, 1, devs), i32),
            pltpu.VMEM((tpt, devs), i32),
            pltpu.VMEM((tpt, devs), i32),
            pltpu.VMEM((steps, 1, devs), i32),
            pltpu.VMEM(state.shape, f32),
            pltpu.VMEM((devs + WHOLE * (tpt - 1), BLOCK, BLOCK), bf16),
        ]
        + blocks
        + [
            pltpu.SemaphoreType.DMA((7,)),
            pltpu.SemaphoreType.DMA((WHOLE // CHUNK,)),
            pltpu.SemaphoreType.DMA(((devs - WHOLE) // CHUNK,)),
        ],
        compiler_params=params(16),
        name="first",
    )(*[in_hbm(a) for a in (route, src, dst, used, potential, table)])
    for i in range(2):
        out = pl.pallas_call(
            gate_kernel,
            out_shape=jax.ShapeDtypeStruct(out.shape, out.dtype),
            in_specs=[ANY],
            out_specs=ANY,
            input_output_aliases={0: 0},
            cost_estimate=pl.CostEstimate(flops=6_000_000_000, bytes_accessed=0, transcendentals=0),
            compiler_params=params(1),
            name=f"gate{i}",
        )(out)
    arrived = exchange(out.reshape(devs, long // 2, 2, BLOCK)).reshape(devs * long, BLOCK)
    local_table = table
    volts, cur = potential, current
    codes = jnp.zeros((8, devs * TRIALS), i32)
    history = [spikes]
    for step in range(1, steps):
        outs = [state, state, state, sent]
        last = step == steps - 1
        out_specs = [VMEM] * len(outs)
        if step == 1:
            outs.append(jax.ShapeDtypeStruct((8, devs * TRIALS), i32))
            out_specs.append(VMEM)
        else:
            constants = []
        if last:
            out_specs[3] = HBM
        results = pl.pallas_call(
            functools.partial(step_kernel, step, last),
            out_shape=tuple(outs),
            in_specs=[VMEM] * (10 + len(constants)),
            out_specs=tuple(out_specs),
            scratch_shapes=[pltpu.SMEM((2, 1, devs), i32)]
            + blocks
            + [
                pltpu.SemaphoreType.DMA((2 + PIECES,)),
                pltpu.VMEM(sent.shape if last else (8, BLOCK), bf16),
            ],
            compiler_params=params(8),
            name=f"step{step}",
        )(chosen, arrived, codes, volts, cur, ext_drive, spikes, dsyn, dmem, local_table, *constants)
        volts, cur, spikes, out = results[:4]
        if step == 1:
            codes = results[4]
        history.append(spikes)
        if last:
            history, out = lax.optimization_barrier((history, out))
        arrived = exchange(out)
    activity = pl.pallas_call(
        activity_kernel,
        out_shape=jax.ShapeDtypeStruct((steps, TRIALS * POPS, BLOCK), f32),
        in_specs=[VMEM] * (1 + steps),
        out_specs=VMEM,
        scratch_shapes=[pltpu.VMEM((steps, count * TRIALS, BLOCK), f32)],
        compiler_params=params(8),
        name="activity",
    )(pops, *history)
    rates = activity.sum(axis=2).reshape(steps, TRIALS, POPS)
    n_local = lax.axis_size("local")
    parts = [rates] + [
        lax.ppermute(rates, "local", [(i, (i + shift) % n_local) for i in range(n_local)])
        for shift in range(1, n_local)
    ]
    total = (parts[0] + parts[2]) + (parts[1] + parts[3])
    total = total / (BLOCK * count)
    volts, cur = pl.pallas_call(
        functools.partial(last_kernel, steps),
        out_shape=(state, state),
        in_specs=[VMEM] * 8,
        out_specs=(HBM, HBM),
        scratch_shapes=[
            pltpu.VMEM(state.shape, f32),
            pltpu.VMEM(state.shape, f32),
            pltpu.SemaphoreType.DMA((2 * HALVES,)),
        ],
        compiler_params=params(8),
        name="last",
    )(arrived, codes, volts, cur, ext_drive, spikes, dsyn, dmem)
    return volts, cur, total[None]


def solution(mesh):
    both = ("area", "local")
    in_specs = (
        P(None, both),
        P(None, both),
        P(None, both),
        P(both),
        P(both),
        P(both, None, None, None, None),
        P(both, None, None),
        P(both, None, None),
        P(both),
        P(None, both, None, None),
        P(None, both, None),
    )
    out_specs = (P(None, both), P(None, both), P("area", None, None, None))
    return jax.shard_map(shards, mesh=mesh, in_specs=in_specs, out_specs=out_specs, check_vma=False)
```

```python
import functools

import jax
import jax.numpy as jnp
from jax import lax
from jax.experimental import pallas as pl
from jax.experimental.pallas import tpu as pltpu
from jax.sharding import PartitionSpec as P

POPS = 8
BLOCK = 128
TRIALS = 8
NO_BLOCK = 64
EXTRA = 2
EARLY = 32
HALVES = 2
PIECES = 2
CHUNK = 32
WHOLE = 32

spike_gain = 4.0
threshold = 1.0
reset_size = 0.5

VMEM = pl.BlockSpec(memory_space=pltpu.VMEM)
ANY = pl.BlockSpec(memory_space=pl.ANY)
HBM = pl.BlockSpec(memory_space=pltpu.HBM)


def params(mib, **more):
    return pltpu.CompilerParams(vmem_limit_bytes=mib << 20, **more)


def lanes(block):
    return slice(block * BLOCK, (block + 1) * BLOCK)


def spike_of(volts):
    return jax.nn.sigmoid(spike_gain * (volts - threshold))


def send_tiles(first, last, pick, blocks_ref, tiles_ref, store):
    for d in range(first, last, 2):
        (block, tile), (block_b, tile_b) = pick(d), pick(d + 1)
        spikes = jnp.concatenate([blocks_ref[block], blocks_ref[block_b]], axis=0)
        tiles = jnp.concatenate([tiles_ref[tile], tiles_ref[tile_b]], axis=1)
        current = jnp.dot(spikes, tiles, preferred_element_type=jnp.float32).astype(jnp.bfloat16)
        store(d, current[:TRIALS, :BLOCK])
        store(d + 1, current[TRIALS:, BLOCK:])


def one_hot(row, col):
    return jnp.where(row == col, 1.0, 0.0).astype(jnp.bfloat16)


def population_rows(pops):
    count = pops.shape[1]
    spread = one_hot(
        lax.broadcasted_iota(jnp.int32, (count, count * TRIALS), 0),
        lax.broadcasted_iota(jnp.int32, (count, count * TRIALS), 1) // TRIALS,
    )
    pops = jnp.broadcast_to(pops.astype(jnp.float32), (TRIALS, count)).astype(jnp.bfloat16)
    pops = jnp.dot(pops, spread, preferred_element_type=jnp.float32)[0:1, :].astype(jnp.int32)
    trial = lax.broadcasted_iota(jnp.int32, pops.shape, 1) % TRIALS
    row = lax.broadcasted_iota(jnp.int32, (TRIALS * POPS, count * TRIALS), 0)
    return one_hot(row, trial * POPS + pops)


def activity_of(member, spikes):
    high = spikes.astype(jnp.bfloat16)
    low = (spikes - high.astype(jnp.float32)).astype(jnp.bfloat16)
    return jnp.dot(member, high, preferred_element_type=jnp.float32) + jnp.dot(
        member, low, preferred_element_type=jnp.float32
    )


def first_kernel(
    route_hbm, src_hbm, dst_hbm, counts_hbm, volts_hbm, table_hbm,
    out_ref, spikes_ref, chosen_ref, gather_ref, spread_ref,
    route_s, src_s, routes_ref, from_ref, dst_ref, counts_ref, volts_ref, tiles_ref,
    blocks_ref, sems, whole_sems, routed_sems,
):
    tpt, devs = dst_ref.shape
    steps = routes_ref.shape[0]
    copies = [
        pltpu.make_async_copy(a, b, sems.at[i])
        for i, (a, b) in enumerate(
            (
                (route_hbm.at[0:1], route_s),
                (src_hbm, src_s),
                (volts_hbm, volts_ref),
                (route_hbm, routes_ref),
                (dst_hbm, dst_ref),
                (counts_hbm, counts_ref),
                (src_hbm, from_ref),
            )
        )
    ]
    for copy in copies:
        copy.start()

    def whole(c):
        at = pl.ds(c * CHUNK * tpt, CHUNK * tpt)
        return pltpu.make_async_copy(table_hbm.at[at], tiles_ref.at[at], whole_sems.at[c])

    def start_whole(c, carry):
        whole(c).start()
        return carry

    lax.fori_loop(0, WHOLE // CHUNK, start_whole, 0)
    copies[0].wait()

    base = WHOLE * tpt - WHOLE

    def start_routed(c, carry):
        for j in range(CHUNK):
            d = WHOLE + c * CHUNK + j
            pltpu.make_async_copy(
                table_hbm.at[d * tpt + route_s[0, 0, d]], tiles_ref.at[base + d], routed_sems.at[c]
            ).start()
        return carry

    lax.fori_loop(0, (devs - WHOLE) // CHUNK, start_routed, 0)
    for copy in copies[3:7]:
        copy.wait()

    step = lax.broadcasted_iota(jnp.int32, (BLOCK, devs), 0)
    targets = jnp.zeros((BLOCK, devs), jnp.int32)
    for t in range(steps):
        target = jnp.where(routes_ref[t] == 0, dst_ref[0:1, :], dst_ref[1:2, :])
        target = jnp.where(counts_ref[t] > 0, target, NO_BLOCK)
        targets = jnp.where(step == t, target, targets)
        device = lax.broadcasted_iota(jnp.int32, (1, devs), 1)
        chosen_ref[t, 0] = device * tpt + routes_ref[t]
        chosen_ref[t, 1] = jnp.where(routes_ref[t] == 0, from_ref[0:1, :], from_ref[1:2, :])
    targets = targets.astype(jnp.float32).astype(jnp.bfloat16)
    rows = lax.broadcasted_iota(jnp.int32, (devs * EXTRA, devs), 0) // EXTRA
    cols = lax.broadcasted_iota(jnp.int32, (devs * EXTRA, devs), 1)
    extra = lax.dot_general(
        one_hot(rows, cols), targets, (((1,), (1,)), ((), ())), preferred_element_type=jnp.float32
    )
    extra = extra.astype(jnp.bfloat16)
    long = TRIALS + EXTRA
    for d in range(devs):
        out_ref[d * long + TRIALS : (d + 1) * long, :] = extra[d * EXTRA : (d + 1) * EXTRA, :]

    row, col = iotas(gather_ref.shape)
    gather_ref[...] = one_hot(row // long, col)
    row, col = iotas(spread_ref.shape)
    spread_ref[...] = one_hot(row, col // TRIALS)

    copies[2].wait()
    for b in range(blocks_ref.shape[0]):
        spikes = spike_of(volts_ref[:, lanes(b)])
        spikes_ref[:, lanes(b)] = spikes
        blocks_ref[b] = spikes.astype(jnp.bfloat16)
    copies[1].wait()

    def store(d, current):
        out_ref[d * long : d * long + TRIALS, :] = current

    def pick_whole(d):
        k = route_s[0, 0, d]
        return src_s[k, d], d * tpt + k

    def pick_routed(d):
        return src_s[route_s[0, 0, d], d], base + d

    for c in range(WHOLE // CHUNK):
        whole(c).wait()
        send_tiles(c * CHUNK, (c + 1) * CHUNK, pick_whole, blocks_ref, tiles_ref, store)
    for c in range((devs - WHOLE) // CHUNK):
        at = WHOLE + c * CHUNK
        pltpu.make_async_copy(
            table_hbm.at[pl.ds(0, CHUNK)], tiles_ref.at[pl.ds(base + at, CHUNK)], routed_sems.at[c]
        ).wait()
        send_tiles(at, at + CHUNK, pick_routed, blocks_ref, tiles_ref, store)


def gate_kernel(message_ref, out_ref):
    pass


def iotas(shape):
    return lax.broadcasted_iota(jnp.int32, shape, 0), lax.broadcasted_iota(jnp.int32, shape, 1)


def codes_of(message, gather, spread):
    long = TRIALS + EXTRA
    read = lax.dot_general(
        one_hot(*iotas((8, BLOCK))), message, (((1,), (1,)), ((), ())), preferred_element_type=jnp.float32
    )
    place = lax.broadcasted_iota(jnp.int32, read.shape, 1) % long
    blocks = jnp.where(place >= TRIALS, read, 0.0)
    near = blocks
    width = near.shape[1]
    near = pltpu.roll(near, width - 2, 1)
    near = near + pltpu.roll(near, width - 2, 1)
    near = near + pltpu.roll(near, width - 4, 1)
    here = jnp.where(place < TRIALS, near.astype(jnp.int32) * TRIALS + place, -1)
    one = jnp.dot(
        jnp.where(place == TRIALS, blocks, 0.0).astype(jnp.bfloat16), gather, preferred_element_type=jnp.float32
    ).astype(jnp.bfloat16)
    later = jnp.dot(one, spread, preferred_element_type=jnp.float32)
    trial = lax.broadcasted_iota(jnp.int32, later.shape, 1) % TRIALS
    return here, later.astype(jnp.int32) * TRIALS + trial


def inflow_of(code, arrived, rows):
    row = lax.broadcasted_iota(jnp.int32, (rows, BLOCK), 0).astype(jnp.float32).astype(jnp.bfloat16)
    code = jnp.broadcast_to(code.astype(jnp.float32), (16, code.shape[1])).astype(jnp.bfloat16)
    one, zero = jnp.ones((), jnp.bfloat16), jnp.zeros((), jnp.bfloat16)
    deliver = jnp.concatenate(
        [
            jnp.where(row == jnp.concatenate([code[:, lanes(c)]] * (rows // 16), axis=0), one, zero)
            for c in range(code.shape[1] // BLOCK)
        ],
        axis=1,
    )
    return jnp.dot(deliver, arrived, preferred_element_type=jnp.float32)


def update(b, inflow, volts_ref, cur_ref, ext_ref, spikes_ref, dsyn_ref, dmem_ref):
    at = lanes(b)
    dsyn = dsyn_ref[b : b + 1, :]
    dmem = dmem_ref[b : b + 1, :]
    cur = dsyn * cur_ref[:, at] + inflow[b * TRIALS : (b + 1) * TRIALS, :]
    volts = (
        dmem * volts_ref[:, at]
        + (1.0 - dmem) * (cur + ext_ref[:, at])
        - reset_size * spikes_ref[:, at]
    )
    return volts, cur


def step_kernel(step, last, *refs):
    (chosen_ref, arrived_ref, codes_ref, volts_ref, cur_ref, ext_ref,
     spikes_ref, dsyn_ref, dmem_ref, table_ref) = refs[:10]
    if step == 1:
        gather_ref, spread_ref = refs[10:12]
        refs = refs[2:]
    volts_out, cur_out, spikes_out, out_ref = refs[10:14]
    chosen_s, blocks_ref, sems = refs[-4:-1]
    sent_ref = refs[-1]
    devs = out_ref.shape[0]
    count = blocks_ref.shape[0]

    def to_smem(row):
        return pltpu.make_async_copy(chosen_ref.at[step, row], chosen_s.at[row], sems.at[row])

    def start(row, carry):
        to_smem(row).start()
        return carry

    lax.fori_loop(0, 2, start, 0)
    if step == 1:
        arrived = arrived_ref[...]
        codes, later = codes_of(arrived, gather_ref[...], spread_ref[...])
        refs[14][...] = later
    else:
        codes = codes_ref[...]
        arrived = arrived_ref[...].reshape(devs * TRIALS, BLOCK)
    inflow = inflow_of(codes[step - 1 : step, :], arrived, count * TRIALS)
    for b in range(count):
        volts, cur = update(
            b, inflow, volts_ref, cur_ref, ext_ref, spikes_ref, dsyn_ref, dmem_ref
        )
        volts_out[:, lanes(b)] = volts
        cur_out[:, lanes(b)] = cur
        spikes = spike_of(volts)
        spikes_out[:, lanes(b)] = spikes
        blocks_ref[b] = spikes.astype(jnp.bfloat16)
    tile_row, block_row = chosen_ref[step, 0], chosen_ref[step, 1]
    early = EARLY if step > 1 else 0

    def pick(d):
        if d < early:
            return block_row[0, d], tile_row[0, d]
        if d == early:
            to_smem(0).wait()
            to_smem(1).wait()
        return chosen_s[1, 0, d], chosen_s[0, 0, d]

    if not last:

        def store(d, current):
            out_ref[d] = current

        send_tiles(0, devs, pick, blocks_ref, table_ref, store)
        return

    def store_sent(d, current):
        sent_ref[d] = current

    size = devs // PIECES
    pieces = []
    for c in range(PIECES):
        send_tiles(c * size, (c + 1) * size, pick, blocks_ref, table_ref, store_sent)
        at = pl.ds(c * size, size)
        pieces.append(pltpu.make_async_copy(sent_ref.at[at], out_ref.at[at], sems.at[2 + c]))
        pieces[-1].start()
    for piece in pieces:
        piece.wait()


def activity_kernel(pops_ref, *refs):
    spikes_refs, act_ref, rows_ref = refs[:-2], refs[-2], refs[-1]
    member = population_rows(pops_ref[...])
    for t, spikes_ref in enumerate(spikes_refs):
        for b in range(spikes_ref.shape[1] // BLOCK):
            rows_ref[t, b * TRIALS : (b + 1) * TRIALS, :] = spikes_ref[:, lanes(b)]
        act_ref[t] = activity_of(member, rows_ref[t])


def last_kernel(step, arrived_ref, codes_ref, volts_ref, cur_ref, ext_ref, spikes_ref,
                dsyn_ref, dmem_ref, volts_hbm, cur_hbm, volts_out, cur_out, sems):
    devs = arrived_ref.shape[0]
    count = dsyn_ref.shape[0]
    arrived = arrived_ref[...].reshape(devs * TRIALS, BLOCK)
    inflow = inflow_of(codes_ref[step - 1 : step, :], arrived, count * TRIALS)
    size = count // HALVES
    copies = []
    for c in range(HALVES):
        for b in range(c * size, (c + 1) * size):
            volts, cur = update(
                b, inflow, volts_ref, cur_ref, ext_ref, spikes_ref, dsyn_ref, dmem_ref
            )
            volts_out[:, lanes(b)] = volts
            cur_out[:, lanes(b)] = cur
        at = pl.ds(c * size * BLOCK, size * BLOCK)
        for i, (here, there) in enumerate(((volts_out, volts_hbm), (cur_out, cur_hbm))):
            copies.append(pltpu.make_async_copy(here.at[:, at], there.at[:, at], sems.at[2 * c + i]))
            copies[-1].start()
    for copy in copies:
        copy.wait()


def shards(
    potential,
    current,
    ext_drive,
    decay_syn,
    decay_mem,
    weights,
    tile_src,
    tile_dst,
    blk_pop,
    tile_route,
    counts,
):
    devs, tpt = weights.shape[1:3]
    count = blk_pop.shape[0]
    steps = tile_route.shape[0]
    f32, bf16, i32 = jnp.float32, jnp.bfloat16, jnp.int32
    table = weights.reshape(devs * tpt, BLOCK, BLOCK)
    src = tile_src[0].T
    dst = tile_dst[0].T
    route = tile_route.reshape(steps, 1, devs)
    used = counts.reshape(steps, 1, devs)
    dsyn = decay_syn.reshape(count, BLOCK)
    dmem = decay_mem.reshape(count, BLOCK)
    pops = blk_pop.reshape(1, count)
    state = jax.ShapeDtypeStruct((TRIALS, count * BLOCK), f32)
    sent = jax.ShapeDtypeStruct((devs, TRIALS, BLOCK), bf16)
    scratch = [
        pltpu.SMEM((1, 1, devs), i32),
        pltpu.SMEM((tpt, devs), i32),
    ]
    blocks = [pltpu.VMEM((count, TRIALS, BLOCK), bf16)]

    def exchange(out):
        return lax.all_to_all(out, ("area", "local"), 0, 0, tiled=True)

    def in_hbm(array):
        return pltpu.with_memory_space_constraint(array, pltpu.HBM)

    long = TRIALS + EXTRA
    out, spikes, chosen, *constants = pl.pallas_call(
        first_kernel,
        out_shape=(
            jax.ShapeDtypeStruct((devs * long, BLOCK), bf16),
            state,
            jax.ShapeDtypeStruct((steps, 2, 1, devs), i32),
            jax.ShapeDtypeStruct((devs * long, devs), bf16),
            jax.ShapeDtypeStruct((devs, devs * TRIALS), bf16),
        ),
        in_specs=[HBM] * 6,
        out_specs=(VMEM,) * 5,
        scratch_shapes=scratch
        + [
            pltpu.VMEM((steps, 1, devs), i32),
            pltpu.VMEM((tpt, devs), i32),
            pltpu.VMEM((tpt, devs), i32),
            pltpu.VMEM((steps, 1, devs), i32),
            pltpu.VMEM(state.shape, f32),
            pltpu.VMEM((devs + WHOLE * (tpt - 1), BLOCK, BLOCK), bf16),
        ]
        + blocks
        + [
            pltpu.SemaphoreType.DMA((7,)),
            pltpu.SemaphoreType.DMA((WHOLE // CHUNK,)),
            pltpu.SemaphoreType.DMA(((devs - WHOLE) // CHUNK,)),
        ],
        compiler_params=params(16),
        name="first",
    )(*[in_hbm(a) for a in (route, src, dst, used, potential, table)])
    for i in range(2):
        out = pl.pallas_call(
            gate_kernel,
            out_shape=jax.ShapeDtypeStruct(out.shape, out.dtype),
            in_specs=[ANY],
            out_specs=ANY,
            input_output_aliases={0: 0},
            cost_estimate=pl.CostEstimate(flops=6_000_000_000, bytes_accessed=0, transcendentals=0),
            compiler_params=params(1),
            name=f"gate{i}",
        )(out)
    arrived = exchange(out.reshape(devs, long // 2, 2, BLOCK)).reshape(devs * long, BLOCK)
    local_table = table
    volts, cur = potential, current
    codes = jnp.zeros((8, devs * TRIALS), i32)
    history = [spikes]
    for step in range(1, steps):
        outs = [state, state, state, sent]
        last = step == steps - 1
        out_specs = [VMEM] * len(outs)
        if step == 1:
            outs.append(jax.ShapeDtypeStruct((8, devs * TRIALS), i32))
            out_specs.append(VMEM)
        else:
            constants = []
        if last:
            out_specs[3] = HBM
        results = pl.pallas_call(
            functools.partial(step_kernel, step, last),
            out_shape=tuple(outs),
            in_specs=[VMEM] * (10 + len(constants)),
            out_specs=tuple(out_specs),
            scratch_shapes=[pltpu.SMEM((2, 1, devs), i32)]
            + blocks
            + [
                pltpu.SemaphoreType.DMA((2 + PIECES,)),
                pltpu.VMEM(sent.shape if last else (8, BLOCK), bf16),
            ],
            compiler_params=params(8),
            name=f"step{step}",
        )(chosen, arrived, codes, volts, cur, ext_drive, spikes, dsyn, dmem, local_table, *constants)
        volts, cur, spikes, out = results[:4]
        if step == 1:
            codes = results[4]
        history.append(spikes)
        if last:
            history, out = lax.optimization_barrier((history, out))
        arrived = exchange(out)
    activity = pl.pallas_call(
        activity_kernel,
        out_shape=jax.ShapeDtypeStruct((steps, TRIALS * POPS, BLOCK), f32),
        in_specs=[VMEM] * (1 + steps),
        out_specs=VMEM,
        scratch_shapes=[pltpu.VMEM((steps, count * TRIALS, BLOCK), f32)],
        compiler_params=params(8),
        name="activity",
    )(pops, *history)
    rates = activity.sum(axis=2).reshape(steps, TRIALS, POPS)
    n_local = lax.axis_size("local")
    parts = [rates] + [
        lax.ppermute(rates, "local", [(i, (i + shift) % n_local) for i in range(n_local)])
        for shift in range(1, n_local)
    ]
    total = (parts[0] + parts[2]) + (parts[1] + parts[3])
    total = total / (BLOCK * count)
    volts, cur = pl.pallas_call(
        functools.partial(last_kernel, steps),
        out_shape=(state, state),
        in_specs=[VMEM] * 8,
        out_specs=(HBM, HBM),
        scratch_shapes=[
            pltpu.VMEM(state.shape, f32),
            pltpu.VMEM(state.shape, f32),
            pltpu.SemaphoreType.DMA((2 * HALVES,)),
        ],
        compiler_params=params(8),
        name="last",
    )(arrived, codes, volts, cur, ext_drive, spikes, dsyn, dmem)
    return volts, cur, total[None]


def solution(mesh):
    both = ("area", "local")
    in_specs = (
        P(None, both),
        P(None, both),
        P(None, both),
        P(both),
        P(both),
        P(both, None, None, None, None),
        P(both, None, None),
        P(both, None, None),
        P(both),
        P(None, both, None, None),
        P(None, both, None),
    )
    out_specs = (P(None, both), P(None, both), P("area", None, None, None))
    return jax.shard_map(shards, mesh=mesh, in_specs=in_specs, out_specs=out_specs, check_vma=False)
```
